512 devices in a mesh: row: 16 (over x_hi, y), col: 32 (over x_lo, z, core).
Axes of the slice: x: 4 (x_hi: 2, x_lo: 2; x = x_hi * 2 + x_lo), y: 8, z: 8, core: 2. Of those that a mesh axis runs over, the one named last changes fastest.
Arguments:
- fact_block: int32 [1572864, 1], P(('row', 'col')), may hold values from 0 to 511; in each aligned block of 3072 rows (0 to 3071, 3072 to 6143, ...) at most 12 rows name the same one
- fact_offset: int32 [1572864], P(('row', 'col')), may hold values from 0 to 2047
- fact_date: int32 [1572864], P(('row', 'col')), may hold values from 0 to 2555
- revenue: bfloat16 [1572864], P(('row', 'col')), may hold values from 0.5 to 4
- supplier_words: int32 [35328], P('col'), may hold values from 0 to 1073741823
- date_words: int32 [96], P('col'), may hold values from 0 to 1073741823
- candidates: int32 [1024], replicated, may hold values from 0 to 1048575
Outputs:
- supplier_revenue: float32 [1048576], P(('row', 'col'))
- candidate_revenue: float32 [1024], replicated
- candidate_total: float32 [], replicated
The draws below stay inside these ranges and needn't reach their ends.
Inputs may be any that keep to these rules, and one draw needn't show every extreme that they name: `fact_block`: each device's rows name no owner block more than 12 times. `candidates`: ids may repeat.
All inputs are finite; a program needn't handle non-finite values.
Results may differ from the reference program's by a relative error of at most 0.0003.
Values sent between devices are 32-bit elements; how exact they have to be, the bound alone decides.
No kernel may reach another device: no remote copies, remote signals or barrier semaphores. Data moves between devices by JAX's collectives and lax.ppermute only.
A program may use at most 64 MiB of HBM per device.

```python
import math
import jax
import jax.numpy as jnp
import numpy as np

ROWS_DEV = 3072
SUP_DEV = 2048
DATES = 2556
CANDS = 1024
ROWS = 1572864
SUPPLIERS = 1048576
MASK_WORDS = 69
DATE_WORDS = 96
CAP = 12
DEVICES = 512


def with_ends(entries, stream_key, least, largest):
    spot = [jax.random.randint(jax.random.fold_in(stream_key, axis), (), 0, length) for axis, length in enumerate(entries.shape)]
    main_axis = entries.shape.index(max(entries.shape))
    beside = spot[:main_axis] + [(spot[main_axis] + 1) % entries.shape[main_axis]] + spot[main_axis + 1:]
    return entries.at[tuple(spot)].set(least).at[tuple(beside)].set(largest)


def shard_levels(rng, extent, pieces, least, top_value):
    gain, own = 1.0, jax.random.fold_in(rng, 6)
    for position, parts in pieces:
        draws = jnp.exp(jax.random.uniform(jax.random.fold_in(own, position), (parts,), jnp.float32, least / len(pieces), top_value / len(pieces)))
        gain = gain * jnp.repeat(draws, extent[position] // parts).reshape([-1 if axis == position else 1 for axis in range(len(extent))])
    return gain


def routed_block(stream_key, own, number, rows, amount, top, limit, skew):
    sequence = jax.random.permutation(stream_key, amount)
    heavy_load, usual = load_shares(amount, rows * top, limit, skew, True), load_shares(amount, rows * top, limit, skew, False)
    places = jnp.arange(amount)

    def named(lengths, offset_by):
        used = int((lengths > 0).sum())
        fixed = max(1, used // 4)
        moved = fixed + (places - fixed + offset_by * (used - fixed)) % max(1, amount - fixed)
        return jnp.zeros((amount,), jnp.int32).at[sequence[jnp.where(places < fixed, places, moved)]].set(jnp.asarray(lengths, jnp.int32))

    lengths = jnp.where(number % 4 == 0, named(heavy_load, number // 4), named(usual, number - number // 4 - 1))
    mixed = jax.random.permutation(jax.random.fold_in(own, 3), amount)
    giver, sink = mixed[0:amount // 2 * 2:2], mixed[1:amount // 2 * 2:2]
    margin = jnp.minimum(lengths[giver] - 1, limit - lengths[sink]) // 2
    margin = jnp.where((giver == sequence[0]) | (sink == sequence[0]) | (lengths[sink] == 0), 0, jnp.maximum(margin, 0))
    moved = jax.random.randint(jax.random.fold_in(own, 4), (amount // 2,), 0, 1 << 20) % (margin + 1)
    lengths = lengths.at[giver].add(-moved).at[sink].add(moved)
    items = jnp.searchsorted(jnp.cumsum(lengths), jnp.arange(rows * top), side="right").astype(jnp.int32)
    listing = items.reshape(top, rows).T
    listing = listing[jax.random.permutation(jax.random.fold_in(own, 1), rows)]
    offset_by = jax.random.randint(jax.random.fold_in(own, 2), (rows, 1), 0, top)
    return jnp.take_along_axis(listing, (jnp.arange(top)[None, :] + offset_by) % top, axis=1)


def load_shares(number_of, total, most, skew, full):
    portions = [(1 << 20) // math.isqrt(grade ** skew) + 1 for grade in range(1, number_of + 1)]
    largest = most if full else min(most, max(-(-total // number_of), total * portions[0] // sum(portions)))
    least = 1 if total - largest >= number_of - 1 else 0
    holding, surplus = [largest] + [least] * (number_of - 1), total - largest - least * (number_of - 1)
    while surplus > 0:
        movable = [i for i in range(1, number_of) if holding[i] < largest] or [i for i in range(1, number_of) if holding[i] < most]
        whole, left = sum([portions[i] for i in movable]), surplus
        for i in movable:
            addition = min(most - holding[i], max(1, left * portions[i] // whole), surplus)
            holding[i] = holding[i] + addition
            surplus = surplus - addition
    return np.array(holding)


def setup_inputs(seed: int = 0) -> dict:
    keys = jax.random.split(jax.random.key(seed), 8)
    fact_block_keys = jax.random.split(jax.random.fold_in(keys[0], 1), ROWS // ROWS_DEV)
    fact_block_turns = jax.random.permutation(jax.random.fold_in(keys[0], 3), ROWS // ROWS_DEV)
    fact_block = jax.vmap(lambda own, number: routed_block(jax.random.fold_in(keys[0], 2), own, number, ROWS_DEV, DEVICES, 1, CAP, 1))(fact_block_keys, fact_block_turns).reshape((ROWS, 1))
    fact_offset = with_ends(jax.random.randint(keys[1], (ROWS,), 0, SUP_DEV), jax.random.fold_in(keys[1], 1), 0, SUP_DEV - 1).astype(jnp.int32)
    fact_date = with_ends(jax.random.randint(keys[2], (ROWS,), 0, DATES), jax.random.fold_in(keys[2], 1), 0, DATES - 1).astype(jnp.int32)
    revenue = jnp.clip(jnp.exp(math.log(4.0) - 2.0794415 * jax.random.uniform(keys[3], (ROWS,), jnp.float32) ** shard_levels(keys[3], (ROWS,), ((0, 512),), -0.2, 0.2)), 0.5, 4.0).astype(jnp.bfloat16)
    supplier_words = with_ends(jax.random.randint(keys[4], (DEVICES * MASK_WORDS,), 0, 1073741824), jax.random.fold_in(keys[4], 1), 0, 1073741823).astype(jnp.int32)
    date_words = with_ends(jax.random.randint(keys[5], (DATE_WORDS,), 0, 1073741824), jax.random.fold_in(keys[5], 1), 0, 1073741823).astype(jnp.int32)
    candidates = with_ends(jax.random.randint(keys[6], (CANDS,), 0, SUPPLIERS), jax.random.fold_in(keys[6], 1), 0, SUPPLIERS - 1).astype(jnp.int32)
    return {"fact_block": fact_block, "fact_offset": fact_offset, "fact_date": fact_date, "revenue": revenue, "supplier_words": supplier_words, "date_words": date_words, "candidates": candidates}


def unpack(words, index, place):
    return jnp.bitwise_and(jnp.right_shift(words[index], place), 1)


def reference(fact_block, fact_offset, fact_date, revenue, supplier_words, date_words, candidates):
    owner = fact_block[:, 0]
    supplier_bit = unpack(supplier_words, (owner * MASK_WORDS + fact_offset // 30).astype(jnp.int32), (fact_offset % 30).astype(jnp.int32))
    date_bit = unpack(date_words, (fact_date // 30).astype(jnp.int32), (fact_date % 30).astype(jnp.int32))
    masked = jnp.where(supplier_bit * date_bit == 1, revenue, jnp.zeros_like(revenue))
    global_id = (owner * SUP_DEV + fact_offset).astype(jnp.int32)
    supplier_revenue = jax.ops.segment_sum(masked.astype(jnp.float32), global_id, num_segments=SUPPLIERS)
    candidate_revenue = supplier_revenue[candidates]
    candidate_total = jnp.sum(candidate_revenue)
    return supplier_revenue, candidate_revenue, candidate_total
```

```python
import functools

import jax
import jax.numpy as jnp
from jax import lax
from jax.experimental import pallas as pl
from jax.experimental.pallas import tpu as pltpu
from jax.sharding import Mesh
from jax.sharding import PartitionSpec as P

ROW = ("row_0", "row_1")
COL = ("col_0", "col_1", "col_2")
ROW_COL = ROW + COL

NROW, NCOL, NDEV = 16, 32, 512
SUP_DEV = 2048
WORDS = 69
LANES = 128
CH = 24
F32, BF16, I32 = jnp.float32, jnp.bfloat16, jnp.int32
BITS_AT, DATES_AT = 72, 104


def iota(shape, dim):
    return lax.broadcasted_iota(I32, shape, dim)


def div30(x):
    return jnp.right_shift(x * 2185, 16)


def lane_gather(row, idx):
    table = jnp.broadcast_to(row, idx.shape)
    return jnp.take_along_axis(table, idx, axis=1, mode="promise_in_bounds")


def roll(x, shift):
    shift = shift % LANES
    return pltpu.roll(x, shift, 1) if shift else x


def lookup(words, idx):
    which, lane = jnp.right_shift(idx, 7), jnp.bitwise_and(idx, 127)
    out = lane_gather(words[0], lane)
    for i in range(1, len(words)):
        out = jnp.where(which == i, lane_gather(words[i], lane), out)
    return out


def k0_body(pos_ref, words_ref, dates_ref, cands_ref, out_ref):
    col = pos_ref[0]
    words = [words_ref[i : i + 1, :] for i in range(9)]
    cands = cands_ref[...]
    off = jnp.bitwise_and(cands, SUP_DEV - 1)
    block = jnp.right_shift(cands, 11) - 16 * col
    mine = (block >= 0) & (block < 16)
    slot = div30(off)
    word = lookup(words, jnp.where(mine, block * WORDS + slot, 0))
    bits = jnp.where(mine, jnp.bitwise_and(jnp.right_shift(word, off - 30 * slot), 1), 0)
    sub, lane = iota((8, LANES), 0), iota((8, LANES), 1)
    dates = jnp.broadcast_to(dates_ref[...], (8, LANES))
    for j in range(4):
        m = jnp.bitwise_and(4 * sub + j, 15)
        own = lookup(words, jnp.where(lane < WORDS, m * WORDS + lane, 0))
        row = jnp.where(lane < WORDS, own, 0)
        in_bits = (lane >= BITS_AT) & (lane < BITS_AT + 32)
        row = jnp.where(in_bits, roll(bits, BITS_AT - 32 * j), row)
        row = jnp.where((lane >= DATES_AT) & (lane < DATES_AT + 3), roll(dates, DATES_AT), row)
        out_ref[pl.ds(j, 8, stride=4), :] = row


def k1_body(block_ref, off_ref, date_ref, rev_ref, cands_ref, tab_ref, cand_ref, hot_ref, val_ref):
    block, off, date = block_ref[...], off_ref[...], date_ref[...]
    rev = rev_ref[...].astype(F32)

    def key_of(b):
        return (
            jnp.bitwise_and(jnp.right_shift(b, 5), 1) * 256
            + jnp.bitwise_and(b, 31) * 8
            + jnp.right_shift(b, 6)
        )

    key = key_of(block)
    own = iota((NDEV, LANES), 0)
    for i in range(CH):
        hot = jnp.where(own == key[i : i + 1, :], 1.0, 0.0).astype(BF16)
        hot_ref[:, i * LANES : (i + 1) * LANES] = hot
    nt = (((1,), (1,)), ((), ()))
    nn = (((1,), (0,)), ((), ()))
    dot = functools.partial(lax.dot_general, preferred_element_type=F32)
    chunk = jnp.where(
        jnp.right_shift(iota((32, CH * LANES), 1), 7) == iota((32, CH * LANES), 0), 1.0, 0.0
    ).astype(BF16)
    count = dot(chunk, hot_ref[...], nt)
    before = jnp.where(iota((32, 32), 1) < iota((32, 32), 0), 1.0, 0.0).astype(BF16)
    prefix = dot(before, count.astype(BF16), nn)
    base = dot(prefix.astype(BF16), hot_ref[...], nn)
    keys_down = jnp.transpose(jnp.concatenate([key, jnp.zeros((LANES - CH, LANES), I32)], 0))
    earlier = iota((LANES, LANES), 0) < iota((LANES, LANES), 1)
    off_hi = jnp.right_shift(off, 7)
    off_lo = jnp.bitwise_and(off, 127)
    date_q = div30(date)
    date_r = date - 30 * date_q
    date_c = jnp.right_shift(date_q * 43691, 17)
    date_l = date_c + 32 * (date_q - 3 * date_c)
    values = [off_lo.astype(F32), off_hi.astype(F32), rev, date_l.astype(F32), date_r.astype(F32)]
    slots = iota((16, LANES), 0)
    for i in range(CH):
        same = (keys_down[:, i : i + 1] == key[i : i + 1, :]) & earlier
        inside = jnp.sum(jnp.where(same, 1.0, 0.0), axis=0, keepdims=True)
        rank = inside + base[i : i + 1, i * LANES : (i + 1) * LANES]
        here = slots == rank.astype(I32)
        for g, v in enumerate(values):
            val_ref[16 * g : 16 * g + 16, i * LANES : (i + 1) * LANES] = jnp.where(
                here, v[i : i + 1, :], 0.0
            ).astype(BF16)
    table = dot(val_ref[...], hot_ref[...], nt)
    tab_ref[0:16, :] = table[0:16] + 128.0 * table[16:32]
    tab_ref[16:64, :] = table[32:80]
    cands = cands_ref[...]
    cand_key = key_of(jnp.right_shift(cands, 11))
    cand_hot = jnp.where(iota((NDEV, 1024), 0) == cand_key, 1.0, 0.0).astype(BF16)
    named = dot(table.astype(BF16), cand_hot, nn)
    cand_off = jnp.bitwise_and(cands, SUP_DEV - 1).astype(F32)
    same_off = named[0:16] + 128.0 * named[16:32] == cand_off
    cand_ref[0:16, :] = jnp.where(same_off, named[32:48], 0.0)
    cand_ref[16:48, :] = named[48:80]


def k2_body(got_ref, tab_ref, cand_ref, out_ref, tmp_ref):
    got = got_ref[...]
    src, lane = iota((NCOL, LANES), 0), iota((NCOL, LANES), 1)
    table = jnp.zeros((NCOL, LANES), I32)
    for j in range(3):
        word = jnp.broadcast_to(got[:, DATES_AT + j : DATES_AT + j + 1], (NCOL, LANES))
        table = jnp.where(lane == 32 * j + src, word, table)
    table = jnp.sum(table, axis=0, keepdims=True)
    bits = jnp.sum(got, axis=0, keepdims=True)
    bits = roll(jnp.broadcast_to(bits, (8, LANES)), 64 - BITS_AT).astype(F32)
    lane8 = iota((8, LANES), 1)
    bits = jnp.where((iota((8, LANES), 0) == 0) & (lane8 >= 64) & (lane8 < 96), bits, 0.0)

    def date_ok(where, place):
        return jnp.bitwise_and(jnp.right_shift(lane_gather(table, where.astype(I32)), place.astype(I32)), 1) == 1

    for i in range(8):
        at = slice(i * LANES, (i + 1) * LANES)
        keep = date_ok(cand_ref[16:32, at], cand_ref[32:48, at])
        tmp_ref[i : i + 1, :] = jnp.sum(jnp.where(keep, cand_ref[0:16, at], 0.0), axis=0, keepdims=True)
    part = tmp_ref[...]
    kept = []
    for i in range(4):
        at = slice(i * LANES, (i + 1) * LANES)
        keep = date_ok(tab_ref[32:48, at], tab_ref[48:64, at])
        kept.append(jnp.where(keep, tab_ref[16:32, at], 0.0))
    for h in range(2):
        at, also = slice(h * LANES, (h + 1) * LANES), slice((h + 2) * LANES, (h + 3) * LANES)
        stack = jnp.concatenate(
            [tab_ref[0:16, at], kept[h], tab_ref[0:16, also], kept[h + 2], jnp.zeros((64, LANES), F32)], 0
        )
        tiles = jnp.transpose(stack)
        for t in range(16):
            out_ref[16 * h + t, 0:8, :] = tiles[8 * t : 8 * t + 8] + bits
            out_ref[16 * h + t, 8:16, :] = part


def k3_body(got_ref, out_ref):
    lane = iota((8, LANES), 1)
    bits = jnp.zeros((8, LANES), F32)
    for j in range(4):
        rows = roll(got_ref[pl.ds(16 * j, 8, stride=64), :], 32 * j - 64)
        bits = jnp.where(jnp.right_shift(lane, 5) == j, rows, bits)
    total = got_ref[8:16, :]
    for c in range(1, NCOL):
        total = total + got_ref[16 * c + 8 : 16 * c + 16, :]
    total = total * bits
    for hi in range(8):
        rows = got_ref[pl.ds(hi, NCOL, stride=16), :]
        for lo in range(2):
            tile = roll(rows[0:8], -32 * lo)
            for q in range(1, 4):
                tile = jnp.where(jnp.right_shift(lane, 5) == q, roll(rows[8 * q : 8 * q + 8], 32 * (q - lo)), tile)
            out_ref[2 * hi + lo, 0:8, :] = tile
            out_ref[2 * hi + lo, 8:16, :] = total


def k4_body(pos_ref, got_ref, words_ref, owned_ref, cand_ref, total_ref, hi_ref, lo_ref):
    lane = iota((8, LANES), 1)
    first = jnp.bitwise_and(lane, 16) == 0
    high, low = iota((16, LANES), 0), iota((LANES, LANES), 0)
    for p in range(8):
        even, odd = got_ref[2 * p, 0:8, :], got_ref[2 * p + 1, 0:8, :]
        off = jnp.where(first, even, roll(odd, 16)).astype(I32)
        rev = jnp.where(first, roll(even, -16), odd)
        off_hi, off_lo = jnp.right_shift(off, 7), jnp.bitwise_and(off, 127)
        for s in range(8):
            at = slice((8 * p + s) * LANES, (8 * p + s + 1) * LANES)
            hi_ref[:, at] = jnp.where(off_hi[s : s + 1] == high, rev[s : s + 1], 0.0).astype(BF16)
            lo_ref[:, at] = jnp.where(off_lo[s : s + 1] == low, 1.0, 0.0).astype(BF16)
    owned = lax.dot_general(
        hi_ref[...], lo_ref[...], (((1,), (1,)), ((), ())), preferred_element_type=F32
    )
    words = words_ref[pl.ds(2 * pos_ref[1] + jnp.right_shift(pos_ref[0], 4), 1), :]
    place = iota((16, LANES), 0) * LANES + iota((16, LANES), 1)
    slot = div30(place)
    bit = jnp.bitwise_and(jnp.right_shift(lane_gather(words, slot), place - 30 * slot), 1)
    owned_ref[...] = jnp.where(bit == 1, owned, 0.0)
    cand = got_ref[0, 8:16, :]
    for r in range(1, NROW):
        cand = cand + got_ref[r, 8:16, :]
    cand_ref[...] = cand
    total_ref[0, 0] = jnp.sum(cand)


SMEM = pl.BlockSpec(memory_space=pltpu.SMEM)
VMEM = pl.BlockSpec(memory_space=pltpu.VMEM)
shape = jax.ShapeDtypeStruct


def call(body, ins, outs, scratch=(), out_specs=None):
    return pl.pallas_call(
        body,
        out_shape=outs,
        in_specs=ins,
        out_specs=out_specs or (VMEM if not isinstance(outs, (tuple, list)) else [VMEM] * len(outs)),
        scratch_shapes=list(scratch),
        name=body.__name__,
    )


def per_device(fact_block, fact_offset, fact_date, revenue, supplier_words, date_words, candidates):
    pos = jnp.stack([lax.axis_index(COL), lax.axis_index(ROW)]).astype(I32)
    cands = candidates.reshape(8, LANES)
    words = jnp.pad(supplier_words, (0, 9 * LANES - 16 * WORDS)).reshape(9, LANES)
    dates = jnp.pad(date_words, (0, LANES - 3)).reshape(1, LANES)
    give0 = call(k0_body, [SMEM, VMEM, VMEM, VMEM], shape((NCOL, LANES), I32))(pos, words, dates, cands)
    got0 = lax.all_to_all(give0.reshape(NCOL, 1, LANES), COL, 0, 0, tiled=True).reshape(NCOL, LANES)
    tab, cand = call(
        k1_body,
        [VMEM] * 5,
        [shape((64, NDEV), F32), shape((48, 1024), F32)],
        [pltpu.VMEM((NDEV, CH * LANES), BF16), pltpu.VMEM((80, CH * LANES), BF16)],
    )(
        fact_block.reshape(CH, LANES),
        fact_offset.reshape(CH, LANES),
        fact_date.reshape(CH, LANES),
        revenue.reshape(CH, LANES),
        candidates.reshape(1, 1024),
    )
    give1 = call(k2_body, [VMEM] * 3, shape((NCOL, 16, LANES), F32), [pltpu.VMEM((8, LANES), F32)])(got0, tab, cand)
    got1 = lax.all_to_all(give1, COL, 0, 0, tiled=True)
    give2 = call(k3_body, [VMEM], shape((NROW, 16, LANES), F32))(got1.reshape(NCOL * 16, LANES))
    got2 = lax.all_to_all(give2, ROW, 0, 0, tiled=True)
    owned, cand, total = call(
        k4_body,
        [SMEM, VMEM, VMEM],
        [shape((16, LANES), F32), shape((8, LANES), F32), shape((1, 1), F32)],
        [pltpu.VMEM((16, 64 * LANES), BF16), pltpu.VMEM((LANES, 64 * LANES), BF16)],
        [VMEM, VMEM, SMEM],
    )(pos, got2, got0)
    return owned.reshape(SUP_DEV), cand.reshape(1024), total.reshape(())


def solution(mesh):
    split = Mesh(mesh.devices.reshape(2, 8, 2, 8, 2), ROW_COL)
    return jax.shard_map(
        per_device,
        mesh=split,
        in_specs=(P(ROW_COL, None), P(ROW_COL), P(ROW_COL), P(ROW_COL), P(COL), P(COL), P()),
        out_specs=(P(ROW_COL), P(), P()),
        check_vma=False,
    )
```

```python
import functools

import jax
import jax.numpy as jnp
from jax import lax
from jax.experimental import pallas as pl
from jax.experimental.pallas import tpu as pltpu
from jax.sharding import Mesh
from jax.sharding import PartitionSpec as P

ROW = ("row_0", "row_1")
COL = ("col_0", "col_1", "col_2")
ROW_COL = ROW + COL

NROW, NCOL, NDEV = 16, 32, 512
SUP_DEV = 2048
WORDS = 69
LANES = 128
CH = 24
F32, BF16, I32 = jnp.float32, jnp.bfloat16, jnp.int32
BITS_AT, DATES_AT = 72, 104


def iota(shape, dim):
    return lax.broadcasted_iota(I32, shape, dim)


def div30(x):
    return jnp.right_shift(x * 2185, 16)


def lane_gather(row, idx):
    table = jnp.broadcast_to(row, idx.shape)
    return jnp.take_along_axis(table, idx, axis=1, mode="promise_in_bounds")


def roll(x, shift):
    shift = shift % LANES
    return pltpu.roll(x, shift, 1) if shift else x


def lookup(words, idx):
    which, lane = jnp.right_shift(idx, 7), jnp.bitwise_and(idx, 127)
    out = lane_gather(words[0], lane)
    for i in range(1, len(words)):
        out = jnp.where(which == i, lane_gather(words[i], lane), out)
    return out


def k0_body(words_ref, dates_ref, cands_ref, out_ref):
    col = lax.axis_index(COL)
    words = [words_ref[i * LANES : (i + 1) * LANES].reshape(1, LANES) for i in range(8)]
    last = words_ref[8 * LANES : 16 * WORDS].reshape(1, 16 * WORDS - 8 * LANES)
    words.append(jnp.concatenate([last, jnp.zeros((1, 9 * LANES - 16 * WORDS), I32)], 1))
    cands = cands_ref[...]
    off = jnp.bitwise_and(cands, SUP_DEV - 1)
    block = jnp.right_shift(cands, 11) - 16 * col
    mine = (block >= 0) & (block < 16)
    slot = div30(off)
    word = lookup(words, jnp.where(mine, block * WORDS + slot, 0))
    bits = jnp.where(mine, jnp.bitwise_and(jnp.right_shift(word, off - 30 * slot), 1), 0)
    sub, lane = iota((8, LANES), 0), iota((8, LANES), 1)
    for j in range(4):
        m = jnp.bitwise_and(4 * sub + j, 15)
        own = lookup(words, jnp.where(lane < WORDS, m * WORDS + lane, 0))
        row = jnp.where(lane < WORDS, own, 0)
        in_bits = (lane >= BITS_AT) & (lane < BITS_AT + 32)
        row = jnp.where(in_bits, roll(bits, BITS_AT - 32 * j), row)
        for d in range(3):
            row = jnp.where(lane == DATES_AT + d, dates_ref[d], row)
        out_ref[pl.ds(j, 8, stride=4), :] = row


def k1_body(block_ref, off_ref, date_ref, rev_ref, cands_ref, tab_ref, cand_ref, hot_ref, val_ref):
    block, off, date = block_ref[...], off_ref[...], date_ref[...]
    rev = rev_ref[...].astype(F32)

    def key_of(b):
        return (
            jnp.bitwise_and(jnp.right_shift(b, 5), 1) * 256
            + jnp.bitwise_and(b, 31) * 8
            + jnp.right_shift(b, 6)
        )

    key = key_of(block)
    own = iota((NDEV, LANES), 0)
    for i in range(CH):
        hot = jnp.where(own == key[i : i + 1, :], 1.0, 0.0).astype(BF16)
        hot_ref[:, i * LANES : (i + 1) * LANES] = hot
    nt = (((1,), (1,)), ((), ()))
    nn = (((1,), (0,)), ((), ()))
    dot = functools.partial(lax.dot_general, preferred_element_type=F32)
    chunk = jnp.where(
        jnp.right_shift(iota((32, CH * LANES), 1), 7) == iota((32, CH * LANES), 0), 1.0, 0.0
    ).astype(BF16)
    count = dot(chunk, hot_ref[...], nt)
    before = jnp.where(iota((32, 32), 1) < iota((32, 32), 0), 1.0, 0.0).astype(BF16)
    prefix = dot(before, count.astype(BF16), nn)
    base = dot(prefix.astype(BF16), hot_ref[...], nn)
    keys_down = jnp.transpose(jnp.concatenate([key, jnp.zeros((LANES - CH, LANES), I32)], 0))
    earlier = iota((LANES, LANES), 0) < iota((LANES, LANES), 1)
    off_hi = jnp.right_shift(off, 7)
    off_lo = jnp.bitwise_and(off, 127)
    date_q = div30(date)
    date_r = date - 30 * date_q
    date_c = jnp.right_shift(date_q * 43691, 17)
    date_l = date_c + 32 * (date_q - 3 * date_c)
    values = [off_lo.astype(F32), off_hi.astype(F32), rev, date_l.astype(F32), date_r.astype(F32)]
    slots = iota((16, LANES), 0)
    for i in range(CH):
        same = (keys_down[:, i : i + 1] == key[i : i + 1, :]) & earlier
        inside = jnp.sum(jnp.where(same, 1.0, 0.0), axis=0, keepdims=True)
        rank = inside + base[i : i + 1, i * LANES : (i + 1) * LANES]
        here = slots == rank.astype(I32)
        for g, v in enumerate(values):
            val_ref[16 * g : 16 * g + 16, i * LANES : (i + 1) * LANES] = jnp.where(
                here, v[i : i + 1, :], 0.0
            ).astype(BF16)
    table = dot(val_ref[...], hot_ref[...], nt)
    tab_ref[0:16, :] = table[0:16] + 128.0 * table[16:32]
    tab_ref[16:64, :] = table[32:80]
    cands = cands_ref[...]
    cand_key = key_of(jnp.right_shift(cands, 11))
    cand_hot = jnp.where(iota((NDEV, 1024), 0) == cand_key, 1.0, 0.0).astype(BF16)
    named = dot(table.astype(BF16), cand_hot, nn)
    cand_off = jnp.bitwise_and(cands, SUP_DEV - 1).astype(F32)
    same_off = named[0:16] + 128.0 * named[16:32] == cand_off
    cand_ref[0:16, :] = jnp.where(same_off, named[32:48], 0.0)
    cand_ref[16:48, :] = named[48:80]


def k2_body(got_ref, tab_ref, cand_ref, out_ref, tmp_ref):
    got = got_ref[...]
    src, lane = iota((NCOL, LANES), 0), iota((NCOL, LANES), 1)
    table = jnp.zeros((NCOL, LANES), I32)
    for j in range(3):
        word = jnp.broadcast_to(got[:, DATES_AT + j : DATES_AT + j + 1], (NCOL, LANES))
        table = jnp.where(lane == 32 * j + src, word, table)
    table = jnp.sum(table, axis=0, keepdims=True)
    bits = jnp.sum(got, axis=0, keepdims=True)
    bits = roll(jnp.broadcast_to(bits, (8, LANES)), 64 - BITS_AT).astype(F32)
    lane8 = iota((8, LANES), 1)
    bits = jnp.where((iota((8, LANES), 0) == 0) & (lane8 >= 64) & (lane8 < 96), bits, 0.0)

    def date_ok(where, place):
        return jnp.bitwise_and(jnp.right_shift(lane_gather(table, where.astype(I32)), place.astype(I32)), 1) == 1

    for i in range(8):
        at = slice(i * LANES, (i + 1) * LANES)
        keep = date_ok(cand_ref[16:32, at], cand_ref[32:48, at])
        tmp_ref[i : i + 1, :] = jnp.sum(jnp.where(keep, cand_ref[0:16, at], 0.0), axis=0, keepdims=True)
    part = tmp_ref[...]
    kept = []
    for i in range(4):
        at = slice(i * LANES, (i + 1) * LANES)
        keep = date_ok(tab_ref[32:48, at], tab_ref[48:64, at])
        kept.append(jnp.where(keep, tab_ref[16:32, at], 0.0))
    for h in range(2):
        at, also = slice(h * LANES, (h + 1) * LANES), slice((h + 2) * LANES, (h + 3) * LANES)
        stack = jnp.concatenate(
            [tab_ref[0:16, at], kept[h], tab_ref[0:16, also], kept[h + 2], jnp.zeros((64, LANES), F32)], 0
        )
        tiles = jnp.transpose(stack)
        for t in range(16):
            out_ref[16 * h + t, 0:8, :] = tiles[8 * t : 8 * t + 8] + bits
            out_ref[16 * h + t, 8:16, :] = part


def k3_body(got_ref, out_ref):
    lane = iota((8, LANES), 1)
    bits = jnp.zeros((8, LANES), F32)
    for j in range(4):
        rows = roll(got_ref[pl.ds(16 * j, 8, stride=64), :], 32 * j - 64)
        bits = jnp.where(jnp.right_shift(lane, 5) == j, rows, bits)
    total = got_ref[8:16, :]
    for c in range(1, NCOL):
        total = total + got_ref[16 * c + 8 : 16 * c + 16, :]
    total = total * bits
    for hi in range(8):
        rows = got_ref[pl.ds(hi, NCOL, stride=16), :]
        for lo in range(2):
            tile = roll(rows[0:8], -32 * lo)
            for q in range(1, 4):
                tile = jnp.where(jnp.right_shift(lane, 5) == q, roll(rows[8 * q : 8 * q + 8], 32 * (q - lo)), tile)
            out_ref[2 * hi + lo, 0:8, :] = tile
            out_ref[2 * hi + lo, 8:16, :] = total


def k4_body(got_ref, words_ref, owned_ref, cand_ref, total_ref, hi_ref, lo_ref):
    lane = iota((8, LANES), 1)
    first = jnp.bitwise_and(lane, 16) == 0
    high, low = iota((16, LANES), 0), iota((LANES, LANES), 0)
    for p in range(8):
        even, odd = got_ref[2 * p, 0:8, :], got_ref[2 * p + 1, 0:8, :]
        off = jnp.where(first, even, roll(odd, 16)).astype(I32)
        rev = jnp.where(first, roll(even, -16), odd)
        off_hi, off_lo = jnp.right_shift(off, 7), jnp.bitwise_and(off, 127)
        for s in range(8):
            at = slice((8 * p + s) * LANES, (8 * p + s + 1) * LANES)
            hi_ref[:, at] = jnp.where(off_hi[s : s + 1] == high, rev[s : s + 1], 0.0).astype(BF16)
            lo_ref[:, at] = jnp.where(off_lo[s : s + 1] == low, 1.0, 0.0).astype(BF16)
    owned = lax.dot_general(
        hi_ref[...], lo_ref[...], (((1,), (1,)), ((), ())), preferred_element_type=F32
    )
    words = words_ref[pl.ds(2 * lax.axis_index(ROW) + lax.axis_index("col_0"), 1), :]
    place = iota((16, LANES), 0) * LANES + iota((16, LANES), 1)
    slot = div30(place)
    bit = jnp.bitwise_and(jnp.right_shift(lane_gather(words, slot), place - 30 * slot), 1)
    owned_ref[...] = jnp.where(bit == 1, owned, 0.0)
    cand = got_ref[0, 8:16, :]
    for r in range(1, NROW):
        cand = cand + got_ref[r, 8:16, :]
    cand_ref[...] = cand
    total_ref[0, 0] = jnp.sum(cand)


SMEM = pl.BlockSpec(memory_space=pltpu.SMEM)
VMEM = pl.BlockSpec(memory_space=pltpu.VMEM)
shape, here = jax.ShapeDtypeStruct, pltpu.VMEM


def near(x):
    return pltpu.with_memory_space_constraint(x, pltpu.VMEM)


def call(body, ins, outs, scratch=(), out_specs=None):
    return pl.pallas_call(
        body,
        out_shape=outs,
        in_specs=ins,
        out_specs=out_specs or (VMEM if not isinstance(outs, (tuple, list)) else [VMEM] * len(outs)),
        scratch_shapes=list(scratch),
        name=body.__name__,
    )


def per_device(fact_block, fact_offset, fact_date, revenue, supplier_words, date_words, candidates):
    cands = candidates.reshape(8, LANES)
    give0 = call(k0_body, [VMEM, SMEM, VMEM], here((NCOL, LANES), I32))(
        supplier_words, date_words, cands
    )
    got0 = lax.all_to_all(give0.reshape(NCOL, 1, LANES), COL, 0, 0, tiled=True).reshape(NCOL, LANES)
    got0 = near(got0)
    tab, cand = call(
        k1_body,
        [VMEM] * 5,
        [here((64, NDEV), F32), here((48, 1024), F32)],
        [pltpu.VMEM((NDEV, CH * LANES), BF16), pltpu.VMEM((80, CH * LANES), BF16)],
    )(
        fact_block.reshape(CH, LANES),
        fact_offset.reshape(CH, LANES),
        fact_date.reshape(CH, LANES),
        revenue.reshape(CH, LANES),
        candidates.reshape(1, 1024),
    )
    give1 = call(k2_body, [VMEM] * 3, here((NCOL, 16, LANES), F32), [pltpu.VMEM((8, LANES), F32)])(
        got0, near(tab), near(cand)
    )
    got1 = lax.all_to_all(give1, COL, 0, 0, tiled=True)
    give2 = call(k3_body, [VMEM], here((NROW, 16, LANES), F32))(near(got1.reshape(NCOL * 16, LANES)))
    got2 = lax.all_to_all(give2, ROW, 0, 0, tiled=True)
    owned, cand, total = call(
        k4_body,
        [VMEM, VMEM],
        [shape((16, LANES), F32), shape((8, LANES), F32), shape((1, 1), F32)],
        [pltpu.VMEM((16, 64 * LANES), BF16), pltpu.VMEM((LANES, 64 * LANES), BF16)],
        [VMEM, VMEM, SMEM],
    )(near(got2), got0)
    return owned.reshape(SUP_DEV), cand.reshape(1024), total.reshape(())


def solution(mesh):
    split = Mesh(mesh.devices.reshape(2, 8, 2, 8, 2), ROW_COL)
    return jax.shard_map(
        per_device,
        mesh=split,
        in_specs=(P(ROW_COL, None), P(ROW_COL), P(ROW_COL), P(ROW_COL), P(COL), P(COL), P()),
        out_specs=(P(ROW_COL), P(), P()),
        check_vma=False,
    )
```

```python
import functools

import jax
import jax.numpy as jnp
from jax import lax
from jax.experimental import pallas as pl
from jax.experimental.pallas import tpu as pltpu
from jax.sharding import Mesh
from jax.sharding import PartitionSpec as P

ROW = ("row_0", "row_1")
COL = ("col_0", "col_1", "col_2")
ROW_COL = ROW + COL

NROW, NCOL, NDEV = 16, 32, 512
SUP_DEV = 2048
WORDS = 69
LANES = 128
CH = 24
F32, BF16, I32 = jnp.float32, jnp.bfloat16, jnp.int32
BITS_AT, DATES_AT = 72, 104
GIVE = 12


def iota(shape, dim):
    return lax.broadcasted_iota(I32, shape, dim)


def div30(x):
    return jnp.right_shift(x * 2185, 16)


def lane_gather(row, idx):
    table = jnp.broadcast_to(row, idx.shape)
    return jnp.take_along_axis(table, idx, axis=1, mode="promise_in_bounds")


def roll(x, shift):
    shift = shift % LANES
    return pltpu.roll(x, shift, 1) if shift else x


def lookup(words, idx):
    which, lane = jnp.right_shift(idx, 7), jnp.bitwise_and(idx, 127)
    out = lane_gather(words[0], lane)
    for i in range(1, len(words)):
        out = jnp.where(which == i, lane_gather(words[i], lane), out)
    return out


def k0_body(words_ref, dates_ref, cands_ref, out_ref):
    col = lax.axis_index(COL)
    words = [words_ref[i * LANES : (i + 1) * LANES].reshape(1, LANES) for i in range(8)]
    last = words_ref[8 * LANES : 16 * WORDS].reshape(1, 16 * WORDS - 8 * LANES)
    words.append(jnp.concatenate([last, jnp.zeros((1, 9 * LANES - 16 * WORDS), I32)], 1))
    cands = cands_ref[...]
    off = jnp.bitwise_and(cands, SUP_DEV - 1)
    block = jnp.right_shift(cands, 11) - 16 * col
    mine = (block >= 0) & (block < 16)
    slot = div30(off)
    word = lookup(words, jnp.where(mine, block * WORDS + slot, 0))
    bits = jnp.where(mine, jnp.bitwise_and(jnp.right_shift(word, off - 30 * slot), 1), 0)
    sub, lane = iota((8, LANES), 0), iota((8, LANES), 1)
    for j in range(4):
        m = jnp.bitwise_and(4 * sub + j, 15)
        own = lookup(words, jnp.where(lane < WORDS, m * WORDS + lane, 0))
        row = jnp.where(lane < WORDS, own, 0)
        in_bits = (lane >= BITS_AT) & (lane < BITS_AT + 32)
        row = jnp.where(in_bits, roll(bits, BITS_AT - 32 * j), row)
        for d in range(3):
            row = jnp.where(lane == DATES_AT + d, dates_ref[d], row)
        out_ref[pl.ds(j, 8, stride=4), :] = row


def k1_body(block_ref, off_ref, date_ref, rev_ref, cands_ref, tab_ref, cand_ref, hot_ref, val_ref):
    block, off, date = block_ref[...], off_ref[...], date_ref[...]
    rev = rev_ref[...].astype(F32)

    def key_of(b):
        return (
            jnp.bitwise_and(jnp.right_shift(b, 5), 3) * LANES
            + jnp.bitwise_and(b, 31) * 4
            + jnp.right_shift(b, 7)
        )

    key = key_of(block)
    own = iota((NDEV, LANES), 0)
    for i in range(CH):
        hot = jnp.where(own == key[i : i + 1, :], 1.0, 0.0).astype(BF16)
        hot_ref[:, i * LANES : (i + 1) * LANES] = hot
    nt = (((1,), (1,)), ((), ()))
    nn = (((1,), (0,)), ((), ()))
    dot = functools.partial(lax.dot_general, preferred_element_type=F32)
    chunk = jnp.where(
        jnp.right_shift(iota((32, CH * LANES), 1), 7) == iota((32, CH * LANES), 0), 1.0, 0.0
    ).astype(BF16)
    count = dot(chunk, hot_ref[...], nt)
    before = jnp.where(iota((32, 32), 1) < iota((32, 32), 0), 1.0, 0.0).astype(BF16)
    prefix = dot(before, count.astype(BF16), nn)
    base = dot(prefix.astype(BF16), hot_ref[...], nn)
    keys_down = jnp.transpose(jnp.concatenate([key, jnp.zeros((LANES - CH, LANES), I32)], 0))
    earlier = iota((LANES, LANES), 0) < iota((LANES, LANES), 1)
    off_hi = jnp.right_shift(off, 7)
    off_lo = jnp.bitwise_and(off, 127)
    date_q = div30(date)
    date_r = date - 30 * date_q
    date_c = jnp.right_shift(date_q * 43691, 17)
    date_l = date_c + 32 * (date_q - 3 * date_c)
    values = [off_lo.astype(F32), off_hi.astype(F32), rev, date_l.astype(F32), date_r.astype(F32)]
    slots = iota((16, LANES), 0)
    for i in range(CH):
        same = (keys_down[:, i : i + 1] == key[i : i + 1, :]) & earlier
        inside = jnp.sum(jnp.where(same, 1.0, 0.0), axis=0, keepdims=True)
        rank = inside + base[i : i + 1, i * LANES : (i + 1) * LANES]
        here = slots == rank.astype(I32)
        for g, v in enumerate(values):
            val_ref[16 * g : 16 * g + 16, i * LANES : (i + 1) * LANES] = jnp.where(
                here, v[i : i + 1, :], 0.0
            ).astype(BF16)
    table = dot(val_ref[...], hot_ref[...], nt)
    tab_ref[0:16, :] = table[0:16] + 128.0 * table[16:32]
    tab_ref[16:64, :] = table[32:80]
    cands = cands_ref[...]
    cand_key = key_of(jnp.right_shift(cands, 11))
    cand_hot = jnp.where(iota((NDEV, 1024), 0) == cand_key, 1.0, 0.0).astype(BF16)
    named = dot(table.astype(BF16), cand_hot, nn)
    cand_off = jnp.bitwise_and(cands, SUP_DEV - 1).astype(F32)
    same_off = named[0:16] + 128.0 * named[16:32] == cand_off
    cand_ref[0:16, :] = jnp.where(same_off, named[32:48], 0.0)
    cand_ref[16:48, :] = named[48:80]


def k2_body(got_ref, tab_ref, cand_ref, out_ref, tmp_ref):
    got = got_ref[...]
    src, lane = iota((NCOL, LANES), 0), iota((NCOL, LANES), 1)
    table = jnp.zeros((NCOL, LANES), I32)
    for j in range(3):
        word = jnp.broadcast_to(got[:, DATES_AT + j : DATES_AT + j + 1], (NCOL, LANES))
        table = jnp.where(lane == 32 * j + src, word, table)
    table = jnp.sum(table, axis=0, keepdims=True)
    bits = jnp.sum(got, axis=0, keepdims=True)
    row, at_lane = iota((LANES, LANES), 0), iota((LANES, LANES), 1)
    spare = (jnp.bitwise_and(row, 3) == 0) & (jnp.bitwise_and(at_lane, 15) >= 12)
    lane8 = iota((8, LANES), 1)
    source = BITS_AT + 4 * jnp.right_shift(lane8, 4) + jnp.bitwise_and(lane8, 3)
    bits = lane_gather(bits, source).astype(F32)[0:1]

    def date_ok(where, place):
        return jnp.bitwise_and(jnp.right_shift(lane_gather(table, where.astype(I32)), place.astype(I32)), 1) == 1

    for i in range(8):
        at = slice(i * LANES, (i + 1) * LANES)
        keep = date_ok(cand_ref[16:32, at], cand_ref[32:48, at])
        tmp_ref[i : i + 1, :] = jnp.sum(jnp.where(keep, cand_ref[0:16, at], 0.0), axis=0, keepdims=True)
    part = tmp_ref[...]
    kept = []
    for i in range(4):
        at = slice(i * LANES, (i + 1) * LANES)
        keep = date_ok(tab_ref[32:48, at], tab_ref[48:64, at])
        kept.append(jnp.where(keep, tab_ref[16:32, at], 0.0))
    stack = []
    for i in range(4):
        stack += [tab_ref[0:16, i * LANES : (i + 1) * LANES], kept[i]]
    tiles = jnp.where(spare, bits, jnp.transpose(jnp.concatenate(stack, 0)))
    for c in range(NCOL):
        out_ref[GIVE * c : GIVE * c + 4, :] = tiles[4 * c : 4 * c + 4]
        out_ref[GIVE * c + 4 : GIVE * c + 12, :] = part


def k3_body(got_ref, out_ref):
    lane = iota((8, LANES), 1)
    source = 16 * jnp.right_shift(jnp.bitwise_and(lane, 31), 2) + 12 + jnp.bitwise_and(lane, 3)
    bits = jnp.zeros((8, LANES), F32)
    for j in range(4):
        rows = got_ref[pl.ds(GIVE * j, 8, stride=4 * GIVE), :]
        rows = jnp.take_along_axis(rows, source, axis=1, mode="promise_in_bounds")
        bits = jnp.where(jnp.right_shift(lane, 5) == j, rows, bits)
    total = got_ref[4:12, :]
    for c in range(1, NCOL):
        total = total + got_ref[GIVE * c + 4 : GIVE * c + 12, :]
    total = total * bits
    for hi in range(4):
        rows = got_ref[pl.ds(hi, NCOL, stride=GIVE), :]
        for lo in range(4):
            tile = roll(rows[0:8], -32 * lo)
            for q in range(1, 4):
                tile = jnp.where(jnp.right_shift(lane, 5) == q, roll(rows[8 * q : 8 * q + 8], 32 * (q - lo)), tile)
            out_ref[4 * hi + lo, 0:8, :] = jnp.where(jnp.bitwise_and(lane, 15) < 12, tile, 0.0)
            out_ref[4 * hi + lo, 8:16, :] = total


def k4_body(got_ref, words_ref, owned_ref, cand_ref, total_ref, hi_ref, lo_ref):
    lane = iota((8, LANES), 1)
    first = jnp.bitwise_and(lane, 16) == 0
    high, low = iota((16, LANES), 0), iota((LANES, LANES), 0)
    for p in range(8):
        even, odd = got_ref[2 * p, 0:8, :], got_ref[2 * p + 1, 0:8, :]
        off = jnp.where(first, even, roll(odd, 16)).astype(I32)
        rev = jnp.where(first, roll(even, -16), odd)
        off_hi, off_lo = jnp.right_shift(off, 7), jnp.bitwise_and(off, 127)
        for s in range(8):
            at = slice((8 * p + s) * LANES, (8 * p + s + 1) * LANES)
            hi_ref[:, at] = jnp.where(off_hi[s : s + 1] == high, rev[s : s + 1], 0.0).astype(BF16)
            lo_ref[:, at] = jnp.where(off_lo[s : s + 1] == low, 1.0, 0.0).astype(BF16)
    owned = lax.dot_general(
        hi_ref[...], lo_ref[...], (((1,), (1,)), ((), ())), preferred_element_type=F32
    )
    words = words_ref[pl.ds(2 * lax.axis_index(ROW) + lax.axis_index("col_0"), 1), :]
    place = iota((16, LANES), 0) * LANES + iota((16, LANES), 1)
    slot = div30(place)
    bit = jnp.bitwise_and(jnp.right_shift(lane_gather(words, slot), place - 30 * slot), 1)
    owned_ref[...] = jnp.where(bit == 1, owned, 0.0)
    cand = got_ref[0, 8:16, :]
    for r in range(1, NROW):
        cand = cand + got_ref[r, 8:16, :]
    cand_ref[...] = cand
    total_ref[0, 0] = jnp.sum(cand)


SMEM = pl.BlockSpec(memory_space=pltpu.SMEM)
VMEM = pl.BlockSpec(memory_space=pltpu.VMEM)
shape, here = jax.ShapeDtypeStruct, pltpu.VMEM


def near(x):
    return pltpu.with_memory_space_constraint(x, pltpu.VMEM)


def call(body, ins, outs, scratch=(), out_specs=None):
    return pl.pallas_call(
        body,
        out_shape=outs,
        in_specs=ins,
        out_specs=out_specs or (VMEM if not isinstance(outs, (tuple, list)) else [VMEM] * len(outs)),
        scratch_shapes=list(scratch),
        name=body.__name__,
    )


def per_device(fact_block, fact_offset, fact_date, revenue, supplier_words, date_words, candidates):
    cands = candidates.reshape(8, LANES)
    give0 = call(k0_body, [VMEM, SMEM, VMEM], here((NCOL, LANES), I32))(
        supplier_words, date_words, cands
    )
    got0 = lax.all_to_all(give0.reshape(NCOL, 1, LANES), COL, 0, 0, tiled=True).reshape(NCOL, LANES)
    got0 = near(got0)
    tab, cand = call(
        k1_body,
        [VMEM] * 5,
        [here((64, NDEV), F32), here((48, 1024), F32)],
        [pltpu.VMEM((NDEV, CH * LANES), BF16), pltpu.VMEM((80, CH * LANES), BF16)],
    )(
        fact_block.reshape(CH, LANES),
        fact_offset.reshape(CH, LANES),
        fact_date.reshape(CH, LANES),
        revenue.reshape(CH, LANES),
        candidates.reshape(1, 1024),
    )
    give1 = call(k2_body, [VMEM] * 3, here((NCOL * GIVE, LANES), F32), [pltpu.VMEM((8, LANES), F32)])(
        got0, near(tab), near(cand)
    )
    got1 = lax.all_to_all(give1.reshape(NCOL, 1, GIVE * LANES), COL, 0, 0, tiled=True)
    give2 = call(k3_body, [VMEM], here((NROW, 16, LANES), F32))(near(got1.reshape(NCOL * GIVE, LANES)))
    got2 = lax.all_to_all(give2, ROW, 0, 0, tiled=True)
    owned, cand, total = call(
        k4_body,
        [VMEM, VMEM],
        [shape((16, LANES), F32), shape((8, LANES), F32), shape((1, 1), F32)],
        [pltpu.VMEM((16, 64 * LANES), BF16), pltpu.VMEM((LANES, 64 * LANES), BF16)],
        [VMEM, VMEM, SMEM],
    )(near(got2), got0)
    return owned.reshape(SUP_DEV), cand.reshape(1024), total.reshape(())


def solution(mesh):
    split = Mesh(mesh.devices.reshape(2, 8, 2, 8, 2), ROW_COL)
    return jax.shard_map(
        per_device,
        mesh=split,
        in_specs=(P(ROW_COL, None), P(ROW_COL), P(ROW_COL), P(ROW_COL), P(COL), P(COL), P()),
        out_specs=(P(ROW_COL), P(), P()),
        check_vma=False,
    )
```

```python
import functools

import jax
import jax.numpy as jnp
from jax import lax
from jax.experimental import pallas as pl
from jax.experimental.pallas import tpu as pltpu
from jax.sharding import Mesh
from jax.sharding import PartitionSpec as P

ROW = ("row_0", "row_1")
COL = ("col_0", "col_1", "col_2")
ROW_COL = ROW + COL
NEAR = ("col_1", "col_2")
FAR = ("row_0", "row_1", "col_0")

NNEAR, NFAR, NCOL, NDEV = 16, 32, 32, 512
SUP_DEV = 2048
WORDS = 69
LANES = 128
CH = 24
F32, BF16, I32 = jnp.float32, jnp.bfloat16, jnp.int32
DATES_AT = 104
LAST = 12


def iota(shape, dim):
    return lax.broadcasted_iota(I32, shape, dim)


def div30(x):
    return jnp.right_shift(x * 2185, 16)


def lane_gather(row, idx):
    table = jnp.broadcast_to(row, idx.shape)
    return jnp.take_along_axis(table, idx, axis=1, mode="promise_in_bounds")


def roll(x, shift):
    shift = shift % LANES
    return pltpu.roll(x, shift, 1) if shift else x


def lookup(words, idx):
    which, lane = jnp.right_shift(idx, 7), jnp.bitwise_and(idx, 127)
    out = lane_gather(words[0], lane)
    for i in range(1, len(words)):
        out = jnp.where(which == i, lane_gather(words[i], lane), out)
    return out


def k0_body(words_ref, dates_ref, cands_ref, out_ref, bits_ref):
    col = lax.axis_index(COL)
    words = [words_ref[i * LANES : (i + 1) * LANES].reshape(1, LANES) for i in range(8)]
    last = words_ref[8 * LANES : 16 * WORDS].reshape(1, 16 * WORDS - 8 * LANES)
    words.append(jnp.concatenate([last, jnp.zeros((1, 9 * LANES - 16 * WORDS), I32)], 1))
    cands = cands_ref[...]
    off = jnp.bitwise_and(cands, SUP_DEV - 1)
    block = jnp.right_shift(cands, 11) - 16 * col
    mine = (block >= 0) & (block < 16)
    slot = div30(off)
    word = lookup(words, jnp.where(mine, block * WORDS + slot, 0))
    bits = jnp.where(mine, jnp.bitwise_and(jnp.right_shift(word, off - 30 * slot), 1), 0)
    bits_ref[0:8, :] = bits
    bits_ref[8:16, :] = bits
    sub, lane = iota((8, LANES), 0), iota((8, LANES), 1)
    for j in range(4):
        m = jnp.bitwise_and(4 * sub + j, 15)
        own = lookup(words, jnp.where(lane < WORDS, m * WORDS + lane, 0))
        row = jnp.where(lane < WORDS, own, 0)
        for d in range(3):
            row = jnp.where(lane == DATES_AT + d, dates_ref[d], row)
        out_ref[pl.ds(2 * j, 8, stride=8), :] = row
        out_ref[pl.ds(2 * j + 1, 8, stride=8), :] = roll(bits_ref[pl.ds(j // 2, 8, stride=2), :], 64 * (j % 2))


def k1_body(block_ref, off_ref, date_ref, rev_ref, cands_ref, tab_ref, cand_ref, hot_ref, val_ref):
    block, off, date = block_ref[...], off_ref[...], date_ref[...]
    rev = rev_ref[...].astype(F32)

    def key_of(b):
        return (
            jnp.bitwise_and(jnp.right_shift(b, 4), 3) * LANES
            + jnp.bitwise_and(b, 15) * 8
            + jnp.right_shift(b, 6)
        )

    key = key_of(block)
    own = iota((NDEV, LANES), 0)
    for i in range(CH):
        hot = jnp.where(own == key[i : i + 1, :], 1.0, 0.0).astype(BF16)
        hot_ref[:, i * LANES : (i + 1) * LANES] = hot
    nt = (((1,), (1,)), ((), ()))
    nn = (((1,), (0,)), ((), ()))
    dot = functools.partial(lax.dot_general, preferred_element_type=F32)
    chunk = jnp.where(
        jnp.right_shift(iota((32, CH * LANES), 1), 7) == iota((32, CH * LANES), 0), 1.0, 0.0
    ).astype(BF16)
    count = dot(chunk, hot_ref[...], nt)
    before = jnp.where(iota((32, 32), 1) < iota((32, 32), 0), 1.0, 0.0).astype(BF16)
    prefix = dot(before, count.astype(BF16), nn)
    base = dot(prefix.astype(BF16), hot_ref[...], nn)
    keys_down = jnp.transpose(jnp.concatenate([key, jnp.zeros((LANES - CH, LANES), I32)], 0))
    earlier = iota((LANES, LANES), 0) < iota((LANES, LANES), 1)
    off_hi = jnp.right_shift(off, 7)
    off_lo = jnp.bitwise_and(off, 127)
    date_q = div30(date)
    date_r = date - 30 * date_q
    date_c = jnp.right_shift(date_q * 43691, 17)
    date_l = date_c + 32 * (date_q - 3 * date_c)
    values = [off_lo.astype(F32), off_hi.astype(F32), rev, date_l.astype(F32), date_r.astype(F32)]
    slots = iota((16, LANES), 0)
    for i in range(CH):
        same = (keys_down[:, i : i + 1] == key[i : i + 1, :]) & earlier
        inside = jnp.sum(jnp.where(same, 1.0, 0.0), axis=0, keepdims=True)
        rank = inside + base[i : i + 1, i * LANES : (i + 1) * LANES]
        here = slots == rank.astype(I32)
        for g, v in enumerate(values):
            val_ref[16 * g : 16 * g + 16, i * LANES : (i + 1) * LANES] = jnp.where(
                here, v[i : i + 1, :], 0.0
            ).astype(BF16)
    table = dot(val_ref[...], hot_ref[...], nt)
    tab_ref[0:16, :] = table[0:16] + 128.0 * table[16:32]
    tab_ref[16:64, :] = table[32:80]
    cands = cands_ref[...]
    cand_key = key_of(jnp.right_shift(cands, 11))
    cand_hot = jnp.where(iota((NDEV, 1024), 0) == cand_key, 1.0, 0.0).astype(BF16)
    named = dot(table.astype(BF16), cand_hot, nn)
    cand_off = jnp.bitwise_and(cands, SUP_DEV - 1).astype(F32)
    same_off = named[0:16] + 128.0 * named[16:32] == cand_off
    cand_ref[0:16, :] = jnp.where(same_off, named[32:48], 0.0)
    cand_ref[16:48, :] = named[48:80]


def k2_body(got_ref, tab_ref, cand_ref, out_ref, tmp_ref):
    got = got_ref[pl.ds(0, NCOL, stride=2), :]
    src, lane = iota((NCOL, LANES), 0), iota((NCOL, LANES), 1)
    table = jnp.zeros((NCOL, LANES), I32)
    for j in range(3):
        word = jnp.broadcast_to(got[:, DATES_AT + j : DATES_AT + j + 1], (NCOL, LANES))
        table = jnp.where(lane == 32 * j + src, word, table)
    table = jnp.sum(table, axis=0, keepdims=True)
    bits = jnp.sum(got_ref[pl.ds(1, NCOL, stride=2), :], axis=0, keepdims=True)
    row, at_lane = iota((LANES, LANES), 0), iota((LANES, LANES), 1)
    row = jnp.where(jnp.bitwise_and(at_lane, 15) >= 12, jnp.bitwise_and(row, 7), 7)
    lane8 = iota((8, LANES), 1)
    source = 4 * jnp.right_shift(lane8, 4) + jnp.bitwise_and(lane8, 3)
    bits = [lane_gather(bits, source + 32 * i).astype(F32)[0:1] for i in range(2)]

    def date_ok(where, place):
        return jnp.bitwise_and(jnp.right_shift(lane_gather(table, where.astype(I32)), place.astype(I32)), 1) == 1

    for i in range(8):
        at = slice(i * LANES, (i + 1) * LANES)
        keep = date_ok(cand_ref[16:32, at], cand_ref[32:48, at])
        tmp_ref[i : i + 1, :] = jnp.sum(jnp.where(keep, cand_ref[0:16, at], 0.0), axis=0, keepdims=True)
    part = tmp_ref[...]
    kept = []
    for i in range(4):
        at = slice(i * LANES, (i + 1) * LANES)
        keep = date_ok(tab_ref[32:48, at], tab_ref[48:64, at])
        kept.append(jnp.where(keep, tab_ref[16:32, at], 0.0))
    stack = []
    for i in range(4):
        stack += [tab_ref[0:16, i * LANES : (i + 1) * LANES], kept[i]]
    tiles = jnp.transpose(jnp.concatenate(stack, 0))
    tiles = jnp.where(row == 0, bits[0], jnp.where(row == 1, bits[1], tiles))
    for g in range(NNEAR):
        out_ref[16 * g : 16 * g + 8, :] = tiles[8 * g : 8 * g + 8]
        out_ref[16 * g + 8 : 16 * g + 16, :] = part


def k3_body(got_ref, out_ref):
    lane = iota((8, LANES), 1)
    source = 16 * jnp.right_shift(jnp.bitwise_and(lane, 31), 2) + 12 + jnp.bitwise_and(lane, 3)
    bits = jnp.zeros((8, LANES), F32)
    for j in range(4):
        rows = got_ref[pl.ds(16 * (j // 2) + j % 2, 8, stride=32), :]
        rows = jnp.take_along_axis(rows, source, axis=1, mode="promise_in_bounds")
        bits = jnp.where(jnp.right_shift(lane, 5) == j, rows, bits)
    total = got_ref[8:16, :]
    for g in range(1, NNEAR):
        total = total + got_ref[16 * g + 8 : 16 * g + 16, :]
    total = total * bits
    lane = iota((4, LANES), 1)
    for hi in range(8):
        rows = [got_ref[pl.ds(64 * q + hi, 4, stride=16), :] for q in range(4)]
        for lo in range(4):
            tile = roll(rows[0], -32 * lo)
            for q in range(1, 4):
                tile = jnp.where(jnp.right_shift(lane, 5) == q, roll(rows[q], 32 * (q - lo)), tile)
            at = LAST * (4 * hi + lo)
            out_ref[at : at + 4, :] = jnp.where(jnp.bitwise_and(lane, 15) < 12, tile, 0.0)
            out_ref[at + 4 : at + 12, :] = total


def k4_body(got_ref, words_ref, owned_ref, cand_ref, total_ref, hi_ref, lo_ref):
    lane = iota((8, LANES), 1)
    first = jnp.bitwise_and(lane, 16) == 0
    high, low = iota((32, LANES), 0), iota((64, LANES), 0)
    high = 2 * jnp.bitwise_and(high, 15) + jnp.right_shift(high, 4)
    for p in range(8):
        even = got_ref[pl.ds(16 * LAST * (p // 4) + p % 4, 8, stride=LAST), :]
        odd = got_ref[pl.ds(16 * LAST * (p // 4) + 8 * LAST + p % 4, 8, stride=LAST), :]
        off = jnp.where(first, even, roll(odd, 16)).astype(I32)
        rev = jnp.where(first, roll(even, -16), odd)
        off_hi, off_lo = jnp.right_shift(off, 6), jnp.bitwise_and(off, 63)
        for s in range(8):
            at = slice((8 * p + s) * LANES, (8 * p + s + 1) * LANES)
            hi_ref[:, at] = jnp.where(off_hi[s : s + 1] == high, rev[s : s + 1], 0.0).astype(BF16)
            lo_ref[:, at] = jnp.where(off_lo[s : s + 1] == low, 1.0, 0.0).astype(BF16)
    owned = lax.dot_general(
        hi_ref[...], lo_ref[...], (((1,), (1,)), ((), ())), preferred_element_type=F32
    )
    owned = jnp.concatenate([owned[0:16], owned[16:32]], 1)
    words = words_ref[pl.ds(2 * lax.axis_index(FAR), 1), :]
    place = iota((16, LANES), 0) * LANES + iota((16, LANES), 1)
    slot = div30(place)
    bit = jnp.bitwise_and(jnp.right_shift(lane_gather(words, slot), place - 30 * slot), 1)
    owned_ref[...] = jnp.where(bit == 1, owned, 0.0)
    cand = got_ref[4:12, :]
    for h in range(1, NFAR):
        cand = cand + got_ref[LAST * h + 4 : LAST * h + 12, :]
    cand_ref[...] = cand
    total_ref[0, 0] = jnp.sum(cand)


SMEM = pl.BlockSpec(memory_space=pltpu.SMEM)
VMEM = pl.BlockSpec(memory_space=pltpu.VMEM)
shape, here = jax.ShapeDtypeStruct, pltpu.VMEM


def near(x):
    return pltpu.with_memory_space_constraint(x, pltpu.VMEM)


def call(body, ins, outs, scratch=(), out_specs=None):
    return pl.pallas_call(
        body,
        out_shape=outs,
        in_specs=ins,
        out_specs=out_specs or (VMEM if not isinstance(outs, (tuple, list)) else [VMEM] * len(outs)),
        scratch_shapes=list(scratch),
        name=body.__name__,
    )


def per_device(fact_block, fact_offset, fact_date, revenue, supplier_words, date_words, candidates):
    cands = candidates.reshape(8, LANES)
    give0 = call(k0_body, [VMEM, SMEM, VMEM], here((2 * NCOL, LANES), I32), [pltpu.VMEM((16, LANES), I32)])(
        supplier_words, date_words, cands
    )
    got0 = lax.all_to_all(give0.reshape(NCOL, 1, 2 * LANES), COL, 0, 0, tiled=True)
    got0 = near(got0.reshape(2 * NCOL, LANES))
    tab, cand = call(
        k1_body,
        [VMEM] * 5,
        [here((64, NDEV), F32), here((48, 1024), F32)],
        [pltpu.VMEM((NDEV, CH * LANES), BF16), pltpu.VMEM((80, CH * LANES), BF16)],
    )(
        fact_block.reshape(CH, LANES),
        fact_offset.reshape(CH, LANES),
        fact_date.reshape(CH, LANES),
        revenue.reshape(CH, LANES),
        candidates.reshape(1, 1024),
    )
    give1 = call(k2_body, [VMEM] * 3, here((NNEAR * 16, LANES), F32), [pltpu.VMEM((8, LANES), F32)])(
        got0, near(tab), near(cand)
    )
    got1 = lax.all_to_all(give1.reshape(NNEAR, 1, 16 * LANES), NEAR, 0, 0, tiled=True)
    give2 = call(k3_body, [VMEM], here((NFAR * LAST, LANES), F32))(near(got1.reshape(NNEAR * 16, LANES)))
    got2 = lax.all_to_all(give2.reshape(NFAR, 1, LAST * LANES), FAR, 0, 0, tiled=True)
    got2 = got2.reshape(NFAR * LAST, LANES)
    owned, cand, total = call(
        k4_body,
        [VMEM, VMEM],
        [shape((16, LANES), F32), shape((8, LANES), F32), shape((1, 1), F32)],
        [pltpu.VMEM((32, 64 * LANES), BF16), pltpu.VMEM((64, 64 * LANES), BF16)],
        [VMEM, VMEM, SMEM],
    )(near(got2), got0)
    return owned.reshape(SUP_DEV), cand.reshape(1024), total.reshape(())


def solution(mesh):
    split = Mesh(mesh.devices.reshape(2, 8, 2, 8, 2), ROW_COL)
    return jax.shard_map(
        per_device,
        mesh=split,
        in_specs=(P(ROW_COL, None), P(ROW_COL), P(ROW_COL), P(ROW_COL), P(COL), P(COL), P()),
        out_specs=(P(ROW_COL), P(), P()),
        check_vma=False,
    )
```

```python
import functools

import jax
import jax.numpy as jnp
from jax import lax
from jax.experimental import pallas as pl
from jax.experimental.pallas import tpu as pltpu
from jax.sharding import Mesh
from jax.sharding import PartitionSpec as P

ROW = ("row_0", "row_1")
COL = ("col_0", "col_1", "col_2")
ROW_COL = ROW + COL
NEAR = ("col_1", "col_2")
FAR = ("row_0", "row_1", "col_0")

NNEAR, NFAR, NCOL, NDEV = 16, 32, 32, 512
SUP_DEV = 2048
WORDS = 69
LANES = 128
CH = 24
F32, BF16, I32 = jnp.float32, jnp.bfloat16, jnp.int32
DATES_AT = 104
LAST = 12


def iota(shape, dim):
    return lax.broadcasted_iota(I32, shape, dim)


def div30(x):
    return jnp.right_shift(x * 2185, 16)


def lane_gather(row, idx):
    table = jnp.broadcast_to(row, idx.shape)
    return jnp.take_along_axis(table, idx, axis=1, mode="promise_in_bounds")


def roll(x, shift):
    shift = shift % LANES
    return pltpu.roll(x, shift, 1) if shift else x


def lookup(words, idx):
    which, lane = jnp.right_shift(idx, 7), jnp.bitwise_and(idx, 127)
    out = lane_gather(words[0], lane)
    for i in range(1, len(words)):
        out = jnp.where(which == i, lane_gather(words[i], lane), out)
    return out


def k0_body(words_ref, dates_ref, cands_ref, out_ref, bits_ref):
    col = lax.axis_index(COL)
    words = [words_ref[i * LANES : (i + 1) * LANES].reshape(1, LANES) for i in range(8)]
    last = words_ref[8 * LANES : 16 * WORDS].reshape(1, 16 * WORDS - 8 * LANES)
    words.append(jnp.concatenate([last, jnp.zeros((1, 9 * LANES - 16 * WORDS), I32)], 1))
    cands = cands_ref[...]
    off = jnp.bitwise_and(cands, SUP_DEV - 1)
    block = jnp.right_shift(cands, 11) - 16 * col
    mine = (block >= 0) & (block < 16)
    slot = div30(off)
    word = lookup(words, jnp.where(mine, block * WORDS + slot, 0))
    bits = jnp.where(mine, jnp.bitwise_and(jnp.right_shift(word, off - 30 * slot), 1), 0)
    bits_ref[0:8, :] = bits
    bits_ref[8:16, :] = bits
    sub, lane = iota((8, LANES), 0), iota((8, LANES), 1)
    for j in range(4):
        m = jnp.bitwise_and(4 * sub + j, 15)
        own = lookup(words, jnp.where(lane < WORDS, m * WORDS + lane, 0))
        row = jnp.where(lane < WORDS, own, 0)
        for d in range(3):
            row = jnp.where(lane == DATES_AT + d, dates_ref[d], row)
        out_ref[pl.ds(2 * j, 8, stride=8), :] = row
        out_ref[pl.ds(2 * j + 1, 8, stride=8), :] = roll(bits_ref[pl.ds(j // 2, 8, stride=2), :], 64 * (j % 2))


def k1_body(block_ref, off_ref, date_ref, rev_ref, cands_ref, tab_ref, cand_ref, hot_ref, val_ref):
    block, off, date = block_ref[...], off_ref[...], date_ref[...]
    rev = rev_ref[...].astype(F32)

    def key_of(b):
        return (
            jnp.bitwise_and(jnp.right_shift(b, 4), 3) * LANES
            + jnp.bitwise_and(b, 15) * 8
            + jnp.right_shift(b, 6)
        )

    key = key_of(block)
    own = iota((NDEV, LANES), 0)
    for i in range(CH):
        hot = jnp.where(own == key[i : i + 1, :], 1.0, 0.0).astype(BF16)
        hot_ref[:, i * LANES : (i + 1) * LANES] = hot
    nt = (((1,), (1,)), ((), ()))
    nn = (((1,), (0,)), ((), ()))
    dot = functools.partial(lax.dot_general, preferred_element_type=F32)
    chunk = jnp.where(
        jnp.right_shift(iota((32, CH * LANES), 1), 7) == iota((32, CH * LANES), 0), 1.0, 0.0
    ).astype(BF16)
    count = dot(chunk, hot_ref[...], nt)
    before = jnp.where(iota((32, 32), 1) < iota((32, 32), 0), 1.0, 0.0).astype(BF16)
    prefix = dot(before, count.astype(BF16), nn)
    base = dot(prefix.astype(BF16), hot_ref[...], nn)
    keys_down = jnp.transpose(jnp.concatenate([key, jnp.zeros((LANES - CH, LANES), I32)], 0))
    earlier = iota((LANES, LANES), 0) < iota((LANES, LANES), 1)
    off_hi = jnp.right_shift(off, 7)
    off_lo = jnp.bitwise_and(off, 127)
    date_q = div30(date)
    date_r = date - 30 * date_q
    date_c = jnp.right_shift(date_q * 43691, 17)
    date_l = date_c + 32 * (date_q - 3 * date_c)
    values = [off_lo.astype(F32), off_hi.astype(F32), rev, date_l.astype(F32), date_r.astype(F32)]
    slots = iota((16, LANES), 0)
    for i in range(CH):
        same = (keys_down[:, i : i + 1] == key[i : i + 1, :]) & earlier
        inside = jnp.sum(jnp.where(same, 1.0, 0.0), axis=0, keepdims=True)
        rank = inside + base[i : i + 1, i * LANES : (i + 1) * LANES]
        here = slots == rank.astype(I32)
        for g, v in enumerate(values):
            val_ref[16 * g : 16 * g + 16, i * LANES : (i + 1) * LANES] = jnp.where(
                here, v[i : i + 1, :], 0.0
            ).astype(BF16)
    table = dot(val_ref[...], hot_ref[...], nt)
    tab_ref[0:16, :] = table[0:16] + 128.0 * table[16:32]
    tab_ref[16:64, :] = table[32:80]
    cands = cands_ref[...]
    cand_key = key_of(jnp.right_shift(cands, 11))
    cand_hot = jnp.where(iota((NDEV, 1024), 0) == cand_key, 1.0, 0.0).astype(BF16)
    named = dot(table.astype(BF16), cand_hot, nn)
    cand_off = jnp.bitwise_and(cands, SUP_DEV - 1).astype(F32)
    same_off = named[0:16] + 128.0 * named[16:32] == cand_off
    cand_ref[0:16, :] = jnp.where(same_off, named[32:48], 0.0)
    cand_ref[16:48, :] = named[48:80]


def k2_body(got_ref, tab_ref, cand_ref, out_ref, tmp_ref):
    got = got_ref[pl.ds(0, NCOL, stride=2), :]
    src, lane = iota((NCOL, LANES), 0), iota((NCOL, LANES), 1)
    table = jnp.zeros((NCOL, LANES), I32)
    for j in range(3):
        word = jnp.broadcast_to(got[:, DATES_AT + j : DATES_AT + j + 1], (NCOL, LANES))
        table = jnp.where(lane == 32 * j + src, word, table)
    table = jnp.sum(table, axis=0, keepdims=True)
    bits = jnp.sum(got_ref[pl.ds(1, NCOL, stride=2), :], axis=0, keepdims=True)
    row, at_lane = iota((LANES, LANES), 0), iota((LANES, LANES), 1)
    row = jnp.where(jnp.bitwise_and(at_lane, 15) >= 12, jnp.bitwise_and(row, 7), 7)
    lane8 = iota((8, LANES), 1)
    source = 4 * jnp.right_shift(lane8, 4) + jnp.bitwise_and(lane8, 3)
    bits = [lane_gather(bits, source + 32 * i).astype(F32)[0:1] for i in range(2)]

    def date_ok(where, place):
        return jnp.bitwise_and(jnp.right_shift(lane_gather(table, where.astype(I32)), place.astype(I32)), 1) == 1

    for i in range(8):
        at = slice(i * LANES, (i + 1) * LANES)
        keep = date_ok(cand_ref[16:32, at], cand_ref[32:48, at])
        tmp_ref[i : i + 1, :] = jnp.sum(jnp.where(keep, cand_ref[0:16, at], 0.0), axis=0, keepdims=True)
    part = tmp_ref[...]
    kept = []
    for i in range(4):
        at = slice(i * LANES, (i + 1) * LANES)
        keep = date_ok(tab_ref[32:48, at], tab_ref[48:64, at])
        kept.append(jnp.where(keep, tab_ref[16:32, at], 0.0))
    stack = []
    for i in range(4):
        stack += [tab_ref[0:16, i * LANES : (i + 1) * LANES], kept[i]]
    tiles = jnp.transpose(jnp.concatenate(stack, 0))
    tiles = jnp.where(row == 0, bits[0], jnp.where(row == 1, bits[1], tiles))
    for g in range(NNEAR):
        out_ref[16 * g : 16 * g + 8, :] = tiles[8 * g : 8 * g + 8]
        out_ref[16 * g + 8 : 16 * g + 16, :] = part


def k3_body(got_ref, out_ref):
    total = got_ref[8:16, :]
    for g in range(1, NNEAR):
        total = total + got_ref[16 * g + 8 : 16 * g + 16, :]
    lane = iota((4, LANES), 1)
    for hi in range(8):
        rows = [got_ref[pl.ds(64 * q + hi, 4, stride=16), :] for q in range(4)]
        for lo in range(4):
            tile = roll(rows[0], -32 * lo)
            for q in range(1, 4):
                tile = jnp.where(jnp.right_shift(lane, 5) == q, roll(rows[q], 32 * (q - lo)), tile)
            at = LAST * (4 * hi + lo)
            out_ref[at : at + 4, :] = jnp.where(jnp.bitwise_and(lane, 15) < 12, tile, 0.0)
            out_ref[at + 4 : at + 12, :] = total


def kb_body(got_ref, out_ref):
    lane = iota((8, LANES), 1)
    source = 16 * jnp.right_shift(jnp.bitwise_and(lane, 31), 2) + 12 + jnp.bitwise_and(lane, 3)
    bits = jnp.zeros((8, LANES), F32)
    for j in range(4):
        rows = got_ref[pl.ds(16 * (j // 2) + j % 2, 8, stride=32), :]
        rows = jnp.take_along_axis(rows, source, axis=1, mode="promise_in_bounds")
        bits = jnp.where(jnp.right_shift(lane, 5) == j, rows, bits)
    out_ref[...] = bits


def ka_body(words_ref, out_ref):
    words = words_ref[pl.ds(2 * lax.axis_index(FAR), 1), :]
    place = iota((16, LANES), 0) * LANES + iota((16, LANES), 1)
    slot = div30(place)
    out_ref[...] = jnp.bitwise_and(jnp.right_shift(lane_gather(words, slot), place - 30 * slot), 1)


def k4_body(got_ref, own_ref, bits_ref, owned_ref, cand_ref, total_ref, hi_ref, lo_ref):
    lane = iota((8, LANES), 1)
    first = jnp.bitwise_and(lane, 16) == 0
    high, low = iota((32, LANES), 0), iota((64, LANES), 0)
    high = 2 * jnp.bitwise_and(high, 15) + jnp.right_shift(high, 4)
    for p in range(8):
        even = got_ref[pl.ds(16 * LAST * (p // 4) + p % 4, 8, stride=LAST), :]
        odd = got_ref[pl.ds(16 * LAST * (p // 4) + 8 * LAST + p % 4, 8, stride=LAST), :]
        off = jnp.where(first, even, roll(odd, 16)).astype(I32)
        rev = jnp.where(first, roll(even, -16), odd)
        off_hi, off_lo = jnp.right_shift(off, 6), jnp.bitwise_and(off, 63)
        for s in range(8):
            at = slice((8 * p + s) * LANES, (8 * p + s + 1) * LANES)
            hi_ref[:, at] = jnp.where(off_hi[s : s + 1] == high, rev[s : s + 1], 0.0).astype(BF16)
            lo_ref[:, at] = jnp.where(off_lo[s : s + 1] == low, 1.0, 0.0).astype(BF16)
    owned = lax.dot_general(
        hi_ref[...], lo_ref[...], (((1,), (1,)), ((), ())), preferred_element_type=F32
    )
    owned = jnp.concatenate([owned[0:16], owned[16:32]], 1)
    owned_ref[...] = jnp.where(own_ref[...] == 1, owned, 0.0)
    cand = got_ref[4:12, :]
    for h in range(1, NFAR):
        cand = cand + got_ref[LAST * h + 4 : LAST * h + 12, :]
    cand = cand * bits_ref[...]
    cand_ref[...] = cand
    total_ref[0, 0] = jnp.sum(cand)


SMEM = pl.BlockSpec(memory_space=pltpu.SMEM)
VMEM = pl.BlockSpec(memory_space=pltpu.VMEM)
shape, here = jax.ShapeDtypeStruct, pltpu.VMEM


def near(x):
    return pltpu.with_memory_space_constraint(x, pltpu.VMEM)


def call(body, ins, outs, scratch=(), out_specs=None):
    return pl.pallas_call(
        body,
        out_shape=outs,
        in_specs=ins,
        out_specs=out_specs or (VMEM if not isinstance(outs, (tuple, list)) else [VMEM] * len(outs)),
        scratch_shapes=list(scratch),
        name=body.__name__,
    )


def per_device(fact_block, fact_offset, fact_date, revenue, supplier_words, date_words, candidates):
    cands = candidates.reshape(8, LANES)
    give0 = call(k0_body, [VMEM, SMEM, VMEM], here((2 * NCOL, LANES), I32), [pltpu.VMEM((16, LANES), I32)])(
        supplier_words, date_words, cands
    )
    got0 = lax.all_to_all(give0.reshape(NCOL, 1, 2 * LANES), COL, 0, 0, tiled=True)
    got0 = near(got0.reshape(2 * NCOL, LANES))
    tab, cand = call(
        k1_body,
        [VMEM] * 5,
        [here((64, NDEV), F32), here((48, 1024), F32)],
        [pltpu.VMEM((NDEV, CH * LANES), BF16), pltpu.VMEM((80, CH * LANES), BF16)],
    )(
        fact_block.reshape(CH, LANES),
        fact_offset.reshape(CH, LANES),
        fact_date.reshape(CH, LANES),
        revenue.reshape(CH, LANES),
        candidates.reshape(1, 1024),
    )
    give1 = call(k2_body, [VMEM] * 3, here((NNEAR * 16, LANES), F32), [pltpu.VMEM((8, LANES), F32)])(
        got0, near(tab), near(cand)
    )
    got1 = lax.all_to_all(give1.reshape(NNEAR, 1, 16 * LANES), NEAR, 0, 0, tiled=True)
    own = call(ka_body, [VMEM], here((16, LANES), I32))(got0)
    bits = call(kb_body, [VMEM], here((8, LANES), F32))(near(got1.reshape(NNEAR * 16, LANES)))
    give2 = call(k3_body, [VMEM], here((NFAR * LAST, LANES), F32))(near(got1.reshape(NNEAR * 16, LANES)))
    got2 = lax.all_to_all(give2.reshape(NFAR, 1, LAST * LANES), FAR, 0, 0, tiled=True)
    got2 = got2.reshape(NFAR * LAST, LANES)
    owned, cand, total = call(
        k4_body,
        [VMEM, VMEM, VMEM],
        [shape((16, LANES), F32), shape((8, LANES), F32), shape((1, 1), F32)],
        [pltpu.VMEM((32, 64 * LANES), BF16), pltpu.VMEM((64, 64 * LANES), BF16)],
        [VMEM, VMEM, SMEM],
    )(near(got2), near(own), near(bits))
    return owned.reshape(SUP_DEV), cand.reshape(1024), total.reshape(())


def solution(mesh):
    split = Mesh(mesh.devices.reshape(2, 8, 2, 8, 2), ROW_COL)
    return jax.shard_map(
        per_device,
        mesh=split,
        in_specs=(P(ROW_COL, None), P(ROW_COL), P(ROW_COL), P(ROW_COL), P(COL), P(COL), P()),
        out_specs=(P(ROW_COL), P(), P()),
        check_vma=False,
    )
```

```python
import functools

import jax
import jax.numpy as jnp
from jax import lax
from jax.experimental import pallas as pl
from jax.experimental.pallas import tpu as pltpu
from jax.sharding import Mesh
from jax.sharding import PartitionSpec as P

ROW = ("row_0", "row_1")
COL = ("col_0", "col_1", "col_2")
ROW_COL = ROW + COL
NEAR = ("col_1", "col_2")
FAR = ("row_0", "row_1", "col_0")
FAR_SENT = ("row_1", "row_0", "col_0")

NNEAR, NFAR, NCOL, NDEV = 16, 32, 32, 512
SUP_DEV = 2048
WORDS = 69
LANES = 128
CH = 24
F32, BF16, I32 = jnp.float32, jnp.bfloat16, jnp.int32
DATES_AT = 104
LAST = 12


def iota(shape, dim):
    return lax.broadcasted_iota(I32, shape, dim)


def div30(x):
    return jnp.right_shift(x * 2185, 16)


def lane_gather(row, idx):
    table = jnp.broadcast_to(row, idx.shape)
    return jnp.take_along_axis(table, idx, axis=1, mode="promise_in_bounds")


def roll(x, shift):
    shift = shift % LANES
    return pltpu.roll(x, shift, 1) if shift else x


def lookup(words, idx):
    which, lane = jnp.right_shift(idx, 7), jnp.bitwise_and(idx, 127)
    out = lane_gather(words[0], lane)
    for i in range(1, len(words)):
        out = jnp.where(which == i, lane_gather(words[i], lane), out)
    return out


def k0_body(words_ref, dates_ref, cands_ref, out_ref, bits_ref):
    col = lax.axis_index(COL)
    words = [words_ref[i * LANES : (i + 1) * LANES].reshape(1, LANES) for i in range(8)]
    last = words_ref[8 * LANES : 16 * WORDS].reshape(1, 16 * WORDS - 8 * LANES)
    words.append(jnp.concatenate([last, jnp.zeros((1, 9 * LANES - 16 * WORDS), I32)], 1))
    cands = cands_ref[...]
    off = jnp.bitwise_and(cands, SUP_DEV - 1)
    block = jnp.right_shift(cands, 11) - 16 * col
    mine = (block >= 0) & (block < 16)
    slot = div30(off)
    word = lookup(words, jnp.where(mine, block * WORDS + slot, 0))
    bits = jnp.where(mine, jnp.bitwise_and(jnp.right_shift(word, off - 30 * slot), 1), 0)
    bits_ref[0:8, :] = bits
    bits_ref[8:16, :] = bits
    sub, lane = iota((8, LANES), 0), iota((8, LANES), 1)
    for j in range(4):
        m = jnp.bitwise_and(4 * sub + j, 15)
        own = lookup(words, jnp.where(lane < WORDS, m * WORDS + lane, 0))
        row = jnp.where(lane < WORDS, own, 0)
        for d in range(3):
            row = jnp.where(lane == DATES_AT + d, dates_ref[d], row)
        out_ref[pl.ds(2 * j, 8, stride=8), :] = row
        out_ref[pl.ds(2 * j + 1, 8, stride=8), :] = roll(bits_ref[pl.ds(j // 2, 8, stride=2), :], 64 * (j % 2))


def k1_body(block_ref, off_ref, date_ref, rev_ref, cands_ref, tab_ref, cand_ref, hot_ref, val_ref):
    block, off, date = block_ref[...], off_ref[...], date_ref[...]
    rev = rev_ref[...].astype(F32)

    def key_of(b):
        return (
            jnp.bitwise_and(jnp.right_shift(b, 4), 3) * LANES
            + jnp.bitwise_and(b, 15) * 8
            + jnp.right_shift(b, 6)
        )

    key = key_of(block)
    own = iota((NDEV, LANES), 0)
    for i in range(CH):
        hot = jnp.where(own == key[i : i + 1, :], 1.0, 0.0).astype(BF16)
        hot_ref[:, i * LANES : (i + 1) * LANES] = hot
    nt = (((1,), (1,)), ((), ()))
    nn = (((1,), (0,)), ((), ()))
    dot = functools.partial(lax.dot_general, preferred_element_type=F32)
    chunk = jnp.where(
        jnp.right_shift(iota((32, CH * LANES), 1), 7) == iota((32, CH * LANES), 0), 1.0, 0.0
    ).astype(BF16)
    count = dot(chunk, hot_ref[...], nt)
    before = jnp.where(iota((32, 32), 1) < iota((32, 32), 0), 1.0, 0.0).astype(BF16)
    prefix = dot(before, count.astype(BF16), nn)
    base = dot(prefix.astype(BF16), hot_ref[...], nn)
    keys_down = jnp.transpose(jnp.concatenate([key, jnp.zeros((LANES - CH, LANES), I32)], 0))
    earlier = iota((LANES, LANES), 0) < iota((LANES, LANES), 1)
    off_hi = jnp.right_shift(off, 7)
    off_lo = jnp.bitwise_and(off, 127)
    date_q = div30(date)
    date_r = date - 30 * date_q
    date_c = jnp.right_shift(date_q * 43691, 17)
    date_l = date_c + 32 * (date_q - 3 * date_c)
    values = [off_lo.astype(F32), off_hi.astype(F32), rev, date_l.astype(F32), date_r.astype(F32)]
    slots = iota((16, LANES), 0)
    for i in range(CH):
        same = (keys_down[:, i : i + 1] == key[i : i + 1, :]) & earlier
        inside = jnp.sum(jnp.where(same, 1.0, 0.0), axis=0, keepdims=True)
        rank = inside + base[i : i + 1, i * LANES : (i + 1) * LANES]
        here = slots == rank.astype(I32)
        for g, v in enumerate(values):
            val_ref[16 * g : 16 * g + 16, i * LANES : (i + 1) * LANES] = jnp.where(
                here, v[i : i + 1, :], 0.0
            ).astype(BF16)
    table = dot(val_ref[...], hot_ref[...], nt)
    tab_ref[0:16, :] = table[0:16] + 128.0 * table[16:32]
    tab_ref[16:64, :] = table[32:80]
    cands = cands_ref[...]
    cand_key = key_of(jnp.right_shift(cands, 11))
    cand_hot = jnp.where(iota((NDEV, 1024), 0) == cand_key, 1.0, 0.0).astype(BF16)
    named = dot(table.astype(BF16), cand_hot, nn)
    cand_off = jnp.bitwise_and(cands, SUP_DEV - 1).astype(F32)
    same_off = named[0:16] + 128.0 * named[16:32] == cand_off
    cand_ref[0:16, :] = jnp.where(same_off, named[32:48], 0.0)
    cand_ref[16:48, :] = named[48:80]


def k2_body(got_ref, tab_ref, cand_ref, out_ref, tmp_ref):
    got = got_ref[pl.ds(0, NCOL, stride=2), :]
    src, lane = iota((NCOL, LANES), 0), iota((NCOL, LANES), 1)
    table = jnp.zeros((NCOL, LANES), I32)
    for j in range(3):
        word = jnp.broadcast_to(got[:, DATES_AT + j : DATES_AT + j + 1], (NCOL, LANES))
        table = jnp.where(lane == 32 * j + src, word, table)
    table = jnp.sum(table, axis=0, keepdims=True)
    bits = jnp.sum(got_ref[pl.ds(1, NCOL, stride=2), :], axis=0, keepdims=True)
    row, at_lane = iota((LANES, LANES), 0), iota((LANES, LANES), 1)
    row = jnp.where(jnp.bitwise_and(at_lane, 15) >= 12, jnp.bitwise_and(row, 7), 7)
    lane8 = iota((8, LANES), 1)
    source = 4 * jnp.right_shift(lane8, 4) + jnp.bitwise_and(lane8, 3)
    bits = [lane_gather(bits, source + 32 * i).astype(F32)[0:1] for i in range(2)]

    def date_ok(where, place):
        return jnp.bitwise_and(jnp.right_shift(lane_gather(table, where.astype(I32)), place.astype(I32)), 1) == 1

    for i in range(8):
        at = slice(i * LANES, (i + 1) * LANES)
        keep = date_ok(cand_ref[16:32, at], cand_ref[32:48, at])
        tmp_ref[i : i + 1, :] = jnp.sum(jnp.where(keep, cand_ref[0:16, at], 0.0), axis=0, keepdims=True)
    part = tmp_ref[...]
    kept = []
    for i in range(4):
        at = slice(i * LANES, (i + 1) * LANES)
        keep = date_ok(tab_ref[32:48, at], tab_ref[48:64, at])
        kept.append(jnp.where(keep, tab_ref[16:32, at], 0.0))
    stack = []
    for i in range(4):
        stack += [tab_ref[0:16, i * LANES : (i + 1) * LANES], kept[i]]
    tiles = jnp.transpose(jnp.concatenate(stack, 0))
    tiles = jnp.where(row == 0, bits[0], jnp.where(row == 1, bits[1], tiles))
    for g in range(NNEAR):
        out_ref[16 * g : 16 * g + 8, :] = tiles[8 * g : 8 * g + 8]
        out_ref[16 * g + 8 : 16 * g + 16, :] = part


def k3_body(got_ref, out_ref):
    lane = iota((8, LANES), 1)
    source = 16 * jnp.right_shift(jnp.bitwise_and(lane, 31), 2) + 12 + jnp.bitwise_and(lane, 3)
    bits = jnp.zeros((8, LANES), F32)
    for j in range(4):
        rows = got_ref[pl.ds(16 * (j // 2) + j % 2, 8, stride=32), :]
        rows = jnp.take_along_axis(rows, source, axis=1, mode="promise_in_bounds")
        bits = jnp.where(jnp.right_shift(lane, 5) == j, rows, bits)
    total = got_ref[8:16, :]
    for g in range(1, NNEAR):
        total = total + got_ref[16 * g + 8 : 16 * g + 16, :]
    total = total * bits
    lane = iota((4, LANES), 1)
    for hi in range(8):
        rows = [got_ref[pl.ds(64 * q + hi, 4, stride=16), :] for q in range(4)]
        for lo in range(4):
            tile = roll(rows[0], -32 * lo)
            for q in range(1, 4):
                tile = jnp.where(jnp.right_shift(lane, 5) == q, roll(rows[q], 32 * (q - lo)), tile)
            to = 4 * hi + lo
            at = LAST * (4 * (to // 2 % 8) + 2 * (to // 16) + to % 2)
            out_ref[at : at + 4, :] = jnp.where(jnp.bitwise_and(lane, 15) < 12, tile, 0.0)
            out_ref[at + 4 : at + 12, :] = total


def k4_body(got_ref, words_ref, owned_ref, cand_ref, total_ref, hi_ref, lo_ref):
    lane = iota((8, LANES), 1)
    first = jnp.bitwise_and(lane, 16) == 0
    high, low = iota((32, LANES), 0), iota((64, LANES), 0)
    high = 2 * jnp.bitwise_and(high, 15) + jnp.right_shift(high, 4)
    for p in range(8):
        even = got_ref[pl.ds(16 * LAST * (p // 4) + p % 4, 8, stride=LAST), :]
        odd = got_ref[pl.ds(16 * LAST * (p // 4) + 8 * LAST + p % 4, 8, stride=LAST), :]
        off = jnp.where(first, even, roll(odd, 16)).astype(I32)
        rev = jnp.where(first, roll(even, -16), odd)
        off_hi, off_lo = jnp.right_shift(off, 6), jnp.bitwise_and(off, 63)
        for s in range(8):
            at = slice((8 * p + s) * LANES, (8 * p + s + 1) * LANES)
            hi_ref[:, at] = jnp.where(off_hi[s : s + 1] == high, rev[s : s + 1], 0.0).astype(BF16)
            lo_ref[:, at] = jnp.where(off_lo[s : s + 1] == low, 1.0, 0.0).astype(BF16)
    owned = lax.dot_general(
        hi_ref[...], lo_ref[...], (((1,), (1,)), ((), ())), preferred_element_type=F32
    )
    owned = jnp.concatenate([owned[0:16], owned[16:32]], 1)
    words = words_ref[pl.ds(2 * lax.axis_index(FAR), 1), :]
    place = iota((16, LANES), 0) * LANES + iota((16, LANES), 1)
    slot = div30(place)
    bit = jnp.bitwise_and(jnp.right_shift(lane_gather(words, slot), place - 30 * slot), 1)
    owned_ref[...] = jnp.where(bit == 1, owned, 0.0)
    cand = got_ref[4:12, :]
    for h in range(1, NFAR):
        cand = cand + got_ref[LAST * h + 4 : LAST * h + 12, :]
    cand_ref[...] = cand
    total_ref[0, 0] = jnp.sum(cand)


SMEM = pl.BlockSpec(memory_space=pltpu.SMEM)
VMEM = pl.BlockSpec(memory_space=pltpu.VMEM)
shape, here = jax.ShapeDtypeStruct, pltpu.VMEM


def near(x):
    return pltpu.with_memory_space_constraint(x, pltpu.VMEM)


def call(body, ins, outs, scratch=(), out_specs=None):
    return pl.pallas_call(
        body,
        out_shape=outs,
        in_specs=ins,
        out_specs=out_specs or (VMEM if not isinstance(outs, (tuple, list)) else [VMEM] * len(outs)),
        scratch_shapes=list(scratch),
        name=body.__name__,
    )


def per_device(fact_block, fact_offset, fact_date, revenue, supplier_words, date_words, candidates):
    cands = candidates.reshape(8, LANES)
    give0 = call(k0_body, [VMEM, SMEM, VMEM], here((2 * NCOL, LANES), I32), [pltpu.VMEM((16, LANES), I32)])(
        supplier_words, date_words, cands
    )
    got0 = lax.all_to_all(give0.reshape(NCOL, 1, 2 * LANES), COL, 0, 0, tiled=True)
    got0 = near(got0.reshape(2 * NCOL, LANES))
    tab, cand = call(
        k1_body,
        [VMEM] * 5,
        [here((64, NDEV), F32), here((48, 1024), F32)],
        [pltpu.VMEM((NDEV, CH * LANES), BF16), pltpu.VMEM((80, CH * LANES), BF16)],
    )(
        fact_block.reshape(CH, LANES),
        fact_offset.reshape(CH, LANES),
        fact_date.reshape(CH, LANES),
        revenue.reshape(CH, LANES),
        candidates.reshape(1, 1024),
    )
    give1 = call(k2_body, [VMEM] * 3, here((NNEAR * 16, LANES), F32), [pltpu.VMEM((8, LANES), F32)])(
        got0, near(tab), near(cand)
    )
    got1 = lax.all_to_all(give1.reshape(NNEAR, 1, 16 * LANES), NEAR, 0, 0, tiled=True)
    give2 = call(k3_body, [VMEM], here((NFAR * LAST, LANES), F32))(near(got1.reshape(NNEAR * 16, LANES)))
    got2 = lax.all_to_all(give2.reshape(NFAR, 1, LAST * LANES), FAR_SENT, 0, 0, tiled=True)
    got2 = got2.reshape(NFAR * LAST, LANES)
    owned, cand, total = call(
        k4_body,
        [VMEM, VMEM],
        [shape((16, LANES), F32), shape((8, LANES), F32), shape((1, 1), F32)],
        [pltpu.VMEM((32, 64 * LANES), BF16), pltpu.VMEM((64, 64 * LANES), BF16)],
        [VMEM, VMEM, SMEM],
    )(near(got2), got0)
    return owned.reshape(SUP_DEV), cand.reshape(1024), total.reshape(())


def solution(mesh):
    split = Mesh(mesh.devices.reshape(2, 8, 2, 8, 2), ROW_COL)
    return jax.shard_map(
        per_device,
        mesh=split,
        in_specs=(P(ROW_COL, None), P(ROW_COL), P(ROW_COL), P(ROW_COL), P(COL), P(COL), P()),
        out_specs=(P(ROW_COL), P(), P()),
        check_vma=False,
    )
```

```python
import functools

import jax
import jax.numpy as jnp
from jax import lax
from jax.experimental import pallas as pl
from jax.experimental.pallas import tpu as pltpu
from jax.sharding import Mesh
from jax.sharding import PartitionSpec as P

XH, Y2, Y1, Y0, XL, Z2, Z1, Z0, CORE = AXES = ("xh", "y2", "y1", "y0", "xl", "z2", "z1", "z0", "core")
COL = (XL, Z2, Z1, Z0, CORE)
NEAR = (Z2, Z1, Z0, CORE)
FAR = (XH, Y2, Y1, Y0, XL)
COL_SENT = (Z2, Z1, Z0, CORE, XL)
FAR_SENT = (Y0, Y1, Y2, XL, XH)

NNEAR, NFAR, NCOL, NDEV = 16, 32, 32, 512
SUP_DEV = 2048
WORDS = 69
LANES = 128
CH = 24
F32, BF16, I32 = jnp.float32, jnp.bfloat16, jnp.int32
DATES_AT = 104
LAST = 12


def iota(shape, dim):
    return lax.broadcasted_iota(I32, shape, dim)


def div30(x):
    return jnp.right_shift(x * 2185, 16)


def lane_gather(row, idx):
    table = jnp.broadcast_to(row, idx.shape)
    return jnp.take_along_axis(table, idx, axis=1, mode="promise_in_bounds")


def roll(x, shift):
    shift = shift % LANES
    return pltpu.roll(x, shift, 1) if shift else x


def lookup(words, idx):
    which, lane = jnp.right_shift(idx, 7), jnp.bitwise_and(idx, 127)
    out = lane_gather(words[0], lane)
    for i in range(1, len(words)):
        out = jnp.where(which == i, lane_gather(words[i], lane), out)
    return out


def k0_body(words_ref, dates_ref, cands_ref, out_ref):
    col = lax.axis_index(COL)
    words = [words_ref[i * LANES : (i + 1) * LANES].reshape(1, LANES) for i in range(8)]
    last = words_ref[8 * LANES : 16 * WORDS].reshape(1, 16 * WORDS - 8 * LANES)
    words.append(jnp.concatenate([last, jnp.zeros((1, 9 * LANES - 16 * WORDS), I32)], 1))
    cands = cands_ref[...]
    off = jnp.bitwise_and(cands, SUP_DEV - 1)
    block = jnp.right_shift(cands, 11) - 16 * col
    mine = (block >= 0) & (block < 16)
    slot = div30(off)
    word = lookup(words, jnp.where(mine, block * WORDS + slot, 0))
    bits = jnp.where(mine, jnp.bitwise_and(jnp.right_shift(word, off - 30 * slot), 1), 0)
    sub, lane = iota((8, LANES), 0), iota((8, LANES), 1)
    for i in range(2):
        m = 2 * sub + i
        own = lookup(words, jnp.where(lane < WORDS, m * WORDS + lane, 0))
        row = jnp.where(lane < WORDS, own, 0)
        for d in range(3):
            row = jnp.where(lane == DATES_AT + d, dates_ref[d], row)
        for j in (4 * i, 4 * i + 2):
            out_ref[pl.ds(j, 8, stride=8), :] = row
            out_ref[pl.ds(j + 1, 8, stride=8), :] = roll(bits, 64 * i)


def k1_body(block_ref, off_ref, date_ref, rev_ref, cands_ref, tab_ref, cand_ref, hot_ref, val_ref):
    block, off, date = block_ref[...], off_ref[...], date_ref[...]
    rev = rev_ref[...].astype(F32)

    def key_of(b):
        return (
            jnp.bitwise_and(jnp.right_shift(b, 4), 3) * LANES
            + jnp.bitwise_and(b, 15) * 8
            + jnp.right_shift(b, 6)
        )

    key = key_of(block)
    own = iota((NDEV, LANES), 0)
    for i in range(CH):
        hot = jnp.where(own == key[i : i + 1, :], 1.0, 0.0).astype(BF16)
        hot_ref[:, i * LANES : (i + 1) * LANES] = hot
    nt = (((1,), (1,)), ((), ()))
    nn = (((1,), (0,)), ((), ()))
    dot = functools.partial(lax.dot_general, preferred_element_type=F32)
    chunk = jnp.where(
        jnp.right_shift(iota((32, CH * LANES), 1), 7) == iota((32, CH * LANES), 0), 1.0, 0.0
    ).astype(BF16)
    count = dot(chunk, hot_ref[...], nt)
    before = jnp.where(iota((32, 32), 1) < iota((32, 32), 0), 1.0, 0.0).astype(BF16)
    prefix = dot(before, count.astype(BF16), nn)
    base = dot(prefix.astype(BF16), hot_ref[...], nn)
    keys_down = jnp.transpose(jnp.concatenate([key, jnp.zeros((LANES - CH, LANES), I32)], 0))
    earlier = iota((LANES, LANES), 0) < iota((LANES, LANES), 1)
    off_hi = jnp.right_shift(off, 7)
    off_lo = jnp.bitwise_and(off, 127)
    date_q = div30(date)
    date_r = date - 30 * date_q
    date_c = jnp.right_shift(date_q * 43691, 17)
    date_l = date_c + 32 * (date_q - 3 * date_c)
    values = [off_lo.astype(F32), off_hi.astype(F32), rev, date_l.astype(F32), date_r.astype(F32)]
    slots = iota((16, LANES), 0)
    for i in range(CH):
        same = (keys_down[:, i : i + 1] == key[i : i + 1, :]) & earlier
        inside = jnp.sum(jnp.where(same, 1.0, 0.0), axis=0, keepdims=True)
        rank = inside + base[i : i + 1, i * LANES : (i + 1) * LANES]
        here = slots == rank.astype(I32)
        for g, v in enumerate(values):
            val_ref[16 * g : 16 * g + 16, i * LANES : (i + 1) * LANES] = jnp.where(
                here, v[i : i + 1, :], 0.0
            ).astype(BF16)
    table = dot(val_ref[...], hot_ref[...], nt)
    tab_ref[0:16, :] = table[0:16] + 128.0 * table[16:32]
    tab_ref[16:64, :] = table[32:80]
    cands = cands_ref[...]
    cand_key = key_of(jnp.right_shift(cands, 11))
    cand_hot = jnp.where(iota((NDEV, 1024), 0) == cand_key, 1.0, 0.0).astype(BF16)
    named = dot(table.astype(BF16), cand_hot, nn)
    cand_off = jnp.bitwise_and(cands, SUP_DEV - 1).astype(F32)
    same_off = named[0:16] + 128.0 * named[16:32] == cand_off
    cand_ref[0:16, :] = jnp.where(same_off, named[32:48], 0.0)
    cand_ref[16:48, :] = named[48:80]


def k2_body(got_ref, tab_ref, cand_ref, out_ref, tmp_ref):
    got = got_ref[pl.ds(0, NCOL, stride=2), :]
    src, lane = iota((NCOL, LANES), 0), iota((NCOL, LANES), 1)
    src = 16 * jnp.bitwise_and(src, 1) + jnp.right_shift(src, 1)
    table = jnp.zeros((NCOL, LANES), I32)
    for j in range(3):
        word = jnp.broadcast_to(got[:, DATES_AT + j : DATES_AT + j + 1], (NCOL, LANES))
        table = jnp.where(lane == 32 * j + src, word, table)
    table = jnp.sum(table, axis=0, keepdims=True)
    bits = jnp.sum(got_ref[pl.ds(1, NCOL, stride=2), :], axis=0, keepdims=True)
    row, at_lane = iota((LANES, LANES), 0), iota((LANES, LANES), 1)
    row = jnp.where(jnp.bitwise_and(at_lane, 15) >= 12, jnp.bitwise_and(row, 7), 7)
    lane8 = iota((8, LANES), 1)
    source = 4 * jnp.right_shift(lane8, 4) + jnp.bitwise_and(lane8, 3)
    bits = [lane_gather(bits, source + 32 * i).astype(F32)[0:1] for i in range(2)]

    def date_ok(where, place):
        return jnp.bitwise_and(jnp.right_shift(lane_gather(table, where.astype(I32)), place.astype(I32)), 1) == 1

    for i in range(8):
        at = slice(i * LANES, (i + 1) * LANES)
        keep = date_ok(cand_ref[16:32, at], cand_ref[32:48, at])
        tmp_ref[i : i + 1, :] = jnp.sum(jnp.where(keep, cand_ref[0:16, at], 0.0), axis=0, keepdims=True)
    part = tmp_ref[...]
    kept = []
    for i in range(4):
        at = slice(i * LANES, (i + 1) * LANES)
        keep = date_ok(tab_ref[32:48, at], tab_ref[48:64, at])
        kept.append(jnp.where(keep, tab_ref[16:32, at], 0.0))
    stack = []
    for i in range(4):
        stack += [tab_ref[0:16, i * LANES : (i + 1) * LANES], kept[i]]
    tiles = jnp.transpose(jnp.concatenate(stack, 0))
    tiles = jnp.where(row == 0, bits[0], jnp.where(row == 1, bits[1], tiles))
    for g in range(NNEAR):
        out_ref[16 * g : 16 * g + 8, :] = tiles[8 * g : 8 * g + 8]
        out_ref[16 * g + 8 : 16 * g + 16, :] = part


def k3_body(got_ref, out_ref):
    lane = iota((8, LANES), 1)
    source = 16 * jnp.right_shift(jnp.bitwise_and(lane, 31), 2) + 12 + jnp.bitwise_and(lane, 3)
    bits = jnp.zeros((8, LANES), F32)
    for j in range(4):
        rows = got_ref[pl.ds(16 * (j // 2) + j % 2, 8, stride=32), :]
        rows = jnp.take_along_axis(rows, source, axis=1, mode="promise_in_bounds")
        bits = jnp.where(jnp.right_shift(lane, 5) == j, rows, bits)
    total = got_ref[8:16, :]
    for g in range(1, NNEAR):
        total = total + got_ref[16 * g + 8 : 16 * g + 16, :]
    total = total * bits
    lane = iota((4, LANES), 1)
    for hi in range(8):
        rows = [got_ref[pl.ds(64 * q + hi, 4, stride=16), :] for q in range(4)]
        for lo in range(4):
            tile = roll(rows[0], -32 * lo)
            for q in range(1, 4):
                tile = jnp.where(jnp.right_shift(lane, 5) == q, roll(rows[q], 32 * (q - lo)), tile)
            to = 4 * hi + lo
            at = LAST * sum((to >> b & 1) << p for b, p in ((4, 0), (3, 2), (2, 3), (1, 4), (0, 1)))
            out_ref[at : at + 4, :] = jnp.where(jnp.bitwise_and(lane, 15) < 12, tile, 0.0)
            out_ref[at + 4 : at + 12, :] = total


def k4_body(got_ref, words_ref, owned_ref, cand_ref, total_ref, hi_ref, lo_ref):
    lane = iota((8, LANES), 1)
    first = jnp.bitwise_and(lane, 16) == 0
    high, low = iota((32, LANES), 0), iota((64, LANES), 0)
    high = 2 * jnp.bitwise_and(high, 15) + jnp.right_shift(high, 4)
    for p in range(8):
        even = got_ref[pl.ds(16 * LAST * (p // 4) + p % 4, 8, stride=LAST), :]
        odd = got_ref[pl.ds(16 * LAST * (p // 4) + 8 * LAST + p % 4, 8, stride=LAST), :]
        off = jnp.where(first, even, roll(odd, 16)).astype(I32)
        rev = jnp.where(first, roll(even, -16), odd)
        off_hi, off_lo = jnp.right_shift(off, 6), jnp.bitwise_and(off, 63)
        for s in range(8):
            at = slice((8 * p + s) * LANES, (8 * p + s + 1) * LANES)
            hi_ref[:, at] = jnp.where(off_hi[s : s + 1] == high, rev[s : s + 1], 0.0).astype(BF16)
            lo_ref[:, at] = jnp.where(off_lo[s : s + 1] == low, 1.0, 0.0).astype(BF16)
    owned = lax.dot_general(
        hi_ref[...], lo_ref[...], (((1,), (1,)), ((), ())), preferred_element_type=F32
    )
    owned = jnp.concatenate([owned[0:16], owned[16:32]], 1)
    far = lax.axis_index(FAR)
    words = words_ref[pl.ds(4 * jnp.bitwise_and(far, 15) + 2 * jnp.right_shift(far, 4), 1), :]
    place = iota((16, LANES), 0) * LANES + iota((16, LANES), 1)
    slot = div30(place)
    bit = jnp.bitwise_and(jnp.right_shift(lane_gather(words, slot), place - 30 * slot), 1)
    owned_ref[...] = jnp.where(bit == 1, owned, 0.0)
    cand = got_ref[4:12, :]
    for h in range(1, NFAR):
        cand = cand + got_ref[LAST * h + 4 : LAST * h + 12, :]
    cand_ref[...] = cand
    total_ref[...] = jnp.sum(jnp.sum(cand, axis=0, keepdims=True), axis=1, keepdims=True)


SMEM = pl.BlockSpec(memory_space=pltpu.SMEM)
VMEM = pl.BlockSpec(memory_space=pltpu.VMEM)
shape, here = jax.ShapeDtypeStruct, pltpu.VMEM


def near(x):
    return pltpu.with_memory_space_constraint(x, pltpu.VMEM)


def call(body, ins, outs, scratch=(), out_specs=None):
    return pl.pallas_call(
        body,
        out_shape=outs,
        in_specs=ins,
        out_specs=out_specs or (VMEM if not isinstance(outs, (tuple, list)) else [VMEM] * len(outs)),
        scratch_shapes=list(scratch),
        name=body.__name__,
    )


def per_device(fact_block, fact_offset, fact_date, revenue, supplier_words, date_words, candidates):
    cands = candidates.reshape(8, LANES)
    give0 = call(k0_body, [VMEM, SMEM, VMEM], here((2 * NCOL, LANES), I32))(
        supplier_words, date_words, cands
    )
    got0 = lax.all_to_all(give0.reshape(NCOL, 1, 2 * LANES), COL_SENT, 0, 0, tiled=True)
    got0 = near(got0.reshape(2 * NCOL, LANES))
    tab, cand = call(
        k1_body,
        [VMEM] * 5,
        [here((64, NDEV), F32), here((48, 1024), F32)],
        [pltpu.VMEM((NDEV, CH * LANES), BF16), pltpu.VMEM((80, CH * LANES), BF16)],
    )(
        fact_block.reshape(CH, LANES),
        fact_offset.reshape(CH, LANES),
        fact_date.reshape(CH, LANES),
        revenue.reshape(CH, LANES),
        candidates.reshape(1, 1024),
    )
    give1 = call(k2_body, [VMEM] * 3, here((NNEAR * 16, LANES), F32), [pltpu.VMEM((8, LANES), F32)])(
        got0, near(tab), near(cand)
    )
    got1 = lax.all_to_all(give1.reshape(NNEAR, 1, 16 * LANES), NEAR, 0, 0, tiled=True)
    give2 = call(k3_body, [VMEM], here((NFAR * LAST, LANES), F32))(near(got1.reshape(NNEAR * 16, LANES)))
    got2 = lax.all_to_all(give2.reshape(NFAR, 1, LAST * LANES), FAR_SENT, 0, 0, tiled=True)
    got2 = got2.reshape(NFAR * LAST, LANES)
    owned, cand, total = call(
        k4_body,
        [VMEM, VMEM],
        [shape((16, LANES), F32), shape((8, LANES), F32), shape((1, 1), F32)],
        [pltpu.VMEM((32, 64 * LANES), BF16), pltpu.VMEM((64, 64 * LANES), BF16)],
    )(near(got2), got0)
    return owned.reshape(SUP_DEV), cand.reshape(1024), total.reshape(())


def solution(mesh):
    split = Mesh(mesh.devices.reshape((2,) * 9), AXES)
    return jax.shard_map(
        per_device,
        mesh=split,
        in_specs=(P(AXES, None), P(AXES), P(AXES), P(AXES), P(COL), P(COL), P()),
        out_specs=(P(AXES), P(), P()),
        check_vma=False,
    )
```

```python
import functools

import jax
import jax.numpy as jnp
from jax import lax
from jax.experimental import pallas as pl
from jax.experimental.pallas import tpu as pltpu
from jax.sharding import Mesh
from jax.sharding import PartitionSpec as P

XH, Y2, Y1, Y0, XL, Z2, Z1, Z0, CORE = AXES = ("xh", "y2", "y1", "y0", "xl", "z2", "z1", "z0", "core")
COL = (XL, Z2, Z1, Z0, CORE)
NEAR = (Z2, Z1, Z0, CORE)
FAR = (XH, Y2, Y1, Y0, XL)
COL_SENT = (Z2, Z1, Z0, CORE, XL)
FAR_SENT = (Y0, Y2, Y1, XL, XH)

NNEAR, NFAR, NCOL, NDEV = 16, 32, 32, 512
SUP_DEV = 2048
WORDS = 69
LANES = 128
CH = 24
F32, BF16, I32 = jnp.float32, jnp.bfloat16, jnp.int32
DATES_AT = 104
LAST = 12


def iota(shape, dim):
    return lax.broadcasted_iota(I32, shape, dim)


def div30(x):
    return jnp.right_shift(x * 2185, 16)


def lane_gather(row, idx):
    table = jnp.broadcast_to(row, idx.shape)
    return jnp.take_along_axis(table, idx, axis=1, mode="promise_in_bounds")


def roll(x, shift):
    shift = shift % LANES
    return pltpu.roll(x, shift, 1) if shift else x


def lookup(words, idx):
    which, lane = jnp.right_shift(idx, 7), jnp.bitwise_and(idx, 127)
    out = lane_gather(words[0], lane)
    for i in range(1, len(words)):
        out = jnp.where(which == i, lane_gather(words[i], lane), out)
    return out


def k0_body(words_ref, dates_ref, cands_ref, out_ref):
    col = lax.axis_index(COL)
    words = [words_ref[i * LANES : (i + 1) * LANES].reshape(1, LANES) for i in range(8)]
    last = words_ref[8 * LANES : 16 * WORDS].reshape(1, 16 * WORDS - 8 * LANES)
    words.append(jnp.concatenate([last, jnp.zeros((1, 9 * LANES - 16 * WORDS), I32)], 1))
    cands = cands_ref[...]
    off = jnp.bitwise_and(cands, SUP_DEV - 1)
    block = jnp.right_shift(cands, 11) - 16 * col
    mine = (block >= 0) & (block < 16)
    slot = div30(off)
    word = lookup(words, jnp.where(mine, block * WORDS + slot, 0))
    bits = jnp.where(mine, jnp.bitwise_and(jnp.right_shift(word, off - 30 * slot), 1), 0)
    sub, lane = iota((8, LANES), 0), iota((8, LANES), 1)
    dates = jnp.concatenate([dates_ref[...].reshape(1, 3), jnp.zeros((1, LANES - 3), I32)], 1)
    dates = roll(jnp.broadcast_to(dates, (8, LANES)), DATES_AT)
    for i in range(2):
        m = 2 * sub + i
        own = lookup(words, jnp.where(lane < WORDS, m * WORDS + lane, 0))
        row = jnp.where(lane < WORDS, own, dates)
        for j in (4 * i, 4 * i + 2):
            out_ref[pl.ds(j, 8, stride=8), :] = row
            out_ref[pl.ds(j + 1, 8, stride=8), :] = roll(bits, 64 * i)


def k1_body(block_ref, off_ref, date_ref, rev_ref, cands_ref, tab_ref, cand_ref, hot_ref, val_ref):
    block, off, date = block_ref[...], off_ref[...], date_ref[...]
    rev = rev_ref[...].astype(F32)

    def key_of(b):
        return (
            jnp.bitwise_and(jnp.right_shift(b, 4), 3) * LANES
            + jnp.bitwise_and(b, 15) * 8
            + jnp.right_shift(b, 6)
        )

    key = key_of(block)
    own = iota((NDEV, LANES), 0)
    for i in range(CH):
        hot = jnp.where(own == key[i : i + 1, :], 1.0, 0.0).astype(BF16)
        hot_ref[:, i * LANES : (i + 1) * LANES] = hot
    nt = (((1,), (1,)), ((), ()))
    nn = (((1,), (0,)), ((), ()))
    dot = functools.partial(lax.dot_general, preferred_element_type=F32)
    chunk = jnp.where(
        jnp.right_shift(iota((32, CH * LANES), 1), 7) == iota((32, CH * LANES), 0), 1.0, 0.0
    ).astype(BF16)
    count = dot(chunk, hot_ref[...], nt)
    before = jnp.where(iota((32, 32), 1) < iota((32, 32), 0), 1.0, 0.0).astype(BF16)
    prefix = dot(before, count.astype(BF16), nn)
    base = dot(prefix.astype(BF16), hot_ref[...], nn)
    keys_down = jnp.transpose(jnp.concatenate([key, jnp.zeros((LANES - CH, LANES), I32)], 0))
    earlier = iota((LANES, LANES), 0) < iota((LANES, LANES), 1)
    off_hi = jnp.right_shift(off, 7)
    off_lo = jnp.bitwise_and(off, 127)
    date_q = div30(date)
    date_r = date - 30 * date_q
    date_c = jnp.right_shift(date_q * 43691, 17)
    date_l = date_c + 32 * (date_q - 3 * date_c)
    values = [off_lo.astype(F32), off_hi.astype(F32), rev, date_l.astype(F32), date_r.astype(F32)]
    slots = iota((16, LANES), 0)
    for i in range(CH):
        same = (keys_down[:, i : i + 1] == key[i : i + 1, :]) & earlier
        inside = jnp.sum(jnp.where(same, 1.0, 0.0), axis=0, keepdims=True)
        rank = inside + base[i : i + 1, i * LANES : (i + 1) * LANES]
        here = slots == rank.astype(I32)
        for g, v in enumerate(values):
            val_ref[16 * g : 16 * g + 16, i * LANES : (i + 1) * LANES] = jnp.where(
                here, v[i : i + 1, :], 0.0
            ).astype(BF16)
    table = dot(val_ref[...], hot_ref[...], nt)
    tab_ref[0:16, :] = table[0:16] + 128.0 * table[16:32]
    tab_ref[16:64, :] = table[32:80]
    cands = cands_ref[...]
    cand_key = key_of(jnp.right_shift(cands, 11))
    cand_hot = jnp.where(iota((NDEV, 1024), 0) == cand_key, 1.0, 0.0).astype(BF16)
    named = dot(table.astype(BF16), cand_hot, nn)
    cand_off = jnp.bitwise_and(cands, SUP_DEV - 1).astype(F32)
    same_off = named[0:16] + 128.0 * named[16:32] == cand_off
    cand_ref[0:16, :] = jnp.where(same_off, named[32:48], 0.0)
    cand_ref[16:48, :] = named[48:80]


def k2_body(got_ref, tab_ref, cand_ref, out_ref, tmp_ref):
    got = got_ref[pl.ds(0, NCOL, stride=2), :]
    src, lane = iota((NCOL, LANES), 0), iota((NCOL, LANES), 1)
    src = 16 * jnp.bitwise_and(src, 1) + jnp.right_shift(src, 1)
    table = jnp.zeros((NCOL, LANES), I32)
    for j in range(3):
        word = jnp.broadcast_to(got[:, DATES_AT + j : DATES_AT + j + 1], (NCOL, LANES))
        table = jnp.where(lane == 32 * j + src, word, table)
    table = jnp.sum(table, axis=0, keepdims=True)
    bits = jnp.sum(got_ref[pl.ds(1, NCOL, stride=2), :], axis=0, keepdims=True)
    row, at_lane = iota((LANES, LANES), 0), iota((LANES, LANES), 1)
    row = jnp.where(jnp.bitwise_and(at_lane, 15) >= 12, jnp.bitwise_and(row, 7), 7)
    lane8 = iota((8, LANES), 1)
    source = 4 * jnp.right_shift(lane8, 4) + jnp.bitwise_and(lane8, 3)
    bits = [lane_gather(bits, source + 32 * i).astype(F32)[0:1] for i in range(2)]

    def date_ok(where, place):
        return jnp.bitwise_and(jnp.right_shift(lane_gather(table, where.astype(I32)), place.astype(I32)), 1) == 1

    for i in range(8):
        at = slice(i * LANES, (i + 1) * LANES)
        keep = date_ok(cand_ref[16:32, at], cand_ref[32:48, at])
        tmp_ref[i : i + 1, :] = jnp.sum(jnp.where(keep, cand_ref[0:16, at], 0.0), axis=0, keepdims=True)
    part = tmp_ref[...]
    kept = []
    for i in range(4):
        at = slice(i * LANES, (i + 1) * LANES)
        keep = date_ok(tab_ref[32:48, at], tab_ref[48:64, at])
        kept.append(jnp.where(keep, tab_ref[16:32, at], 0.0))
    stack = []
    for i in range(4):
        stack += [tab_ref[0:16, i * LANES : (i + 1) * LANES], kept[i]]
    tiles = jnp.transpose(jnp.concatenate(stack, 0))
    tiles = jnp.where(row == 0, bits[0], jnp.where(row == 1, bits[1], tiles))
    for g in range(NNEAR):
        out_ref[16 * g : 16 * g + 8, :] = tiles[8 * g : 8 * g + 8]
        out_ref[16 * g + 8 : 16 * g + 16, :] = part


def k3_body(got_ref, out_ref):
    lane = iota((8, LANES), 1)
    source = 16 * jnp.right_shift(jnp.bitwise_and(lane, 31), 2) + 12 + jnp.bitwise_and(lane, 3)
    bits = jnp.zeros((8, LANES), F32)
    for j in range(4):
        rows = got_ref[pl.ds(16 * (j // 2) + j % 2, 8, stride=32), :]
        rows = jnp.take_along_axis(rows, source, axis=1, mode="promise_in_bounds")
        bits = jnp.where(jnp.right_shift(lane, 5) == j, rows, bits)
    total = got_ref[8:16, :]
    for g in range(1, NNEAR):
        total = total + got_ref[16 * g + 8 : 16 * g + 16, :]
    total = total * bits
    lane = iota((4, LANES), 1)
    for hi in range(8):
        rows = [got_ref[pl.ds(64 * q + hi, 4, stride=16), :] for q in range(4)]
        for lo in range(4):
            tile = roll(rows[0], -32 * lo)
            for q in range(1, 4):
                tile = jnp.where(jnp.right_shift(lane, 5) == q, roll(rows[q], 32 * (q - lo)), tile)
            to = 4 * hi + lo
            at = LAST * sum((to >> b & 1) << p for b, p in ((4, 0), (3, 3), (2, 2), (1, 4), (0, 1)))
            out_ref[at : at + 4, :] = jnp.where(jnp.bitwise_and(lane, 15) < 12, tile, 0.0)
            out_ref[at + 4 : at + 12, :] = total


def k4_body(got_ref, words_ref, owned_ref, cand_ref, total_ref, hi_ref, lo_ref):
    lane = iota((8, LANES), 1)
    first = jnp.bitwise_and(lane, 16) == 0
    high, low = iota((32, LANES), 0), iota((64, LANES), 0)
    high = 2 * jnp.bitwise_and(high, 15) + jnp.right_shift(high, 4)
    for p in range(8):
        even = got_ref[pl.ds(16 * LAST * (p // 4) + p % 4, 8, stride=LAST), :]
        odd = got_ref[pl.ds(16 * LAST * (p // 4) + 8 * LAST + p % 4, 8, stride=LAST), :]
        off = jnp.where(first, even, roll(odd, 16)).astype(I32)
        rev = jnp.where(first, roll(even, -16), odd)
        off_hi, off_lo = jnp.right_shift(off, 6), jnp.bitwise_and(off, 63)
        for s in range(8):
            at = slice((8 * p + s) * LANES, (8 * p + s + 1) * LANES)
            hi_ref[:, at] = jnp.where(off_hi[s : s + 1] == high, rev[s : s + 1], 0.0).astype(BF16)
            lo_ref[:, at] = jnp.where(off_lo[s : s + 1] == low, 1.0, 0.0).astype(BF16)
    owned = lax.dot_general(
        hi_ref[...], lo_ref[...], (((1,), (1,)), ((), ())), preferred_element_type=F32
    )
    owned = jnp.concatenate([owned[0:16], owned[16:32]], 1)
    far = lax.axis_index(FAR)
    words = words_ref[pl.ds(4 * jnp.bitwise_and(far, 15) + 2 * jnp.right_shift(far, 4), 1), :]
    place = iota((16, LANES), 0) * LANES + iota((16, LANES), 1)
    slot = div30(place)
    bit = jnp.bitwise_and(jnp.right_shift(lane_gather(words, slot), place - 30 * slot), 1)
    owned_ref[...] = jnp.where(bit == 1, owned, 0.0)
    cand = got_ref[4:12, :]
    for h in range(1, NFAR):
        cand = cand + got_ref[LAST * h + 4 : LAST * h + 12, :]
    cand_ref[...] = cand
    total_ref[...] = jnp.sum(jnp.sum(cand, axis=0, keepdims=True), axis=1, keepdims=True)


SMEM = pl.BlockSpec(memory_space=pltpu.SMEM)
VMEM = pl.BlockSpec(memory_space=pltpu.VMEM)
shape, here = jax.ShapeDtypeStruct, pltpu.VMEM


def near(x):
    return pltpu.with_memory_space_constraint(x, pltpu.VMEM)


def call(body, ins, outs, scratch=(), out_specs=None):
    return pl.pallas_call(
        body,
        out_shape=outs,
        in_specs=ins,
        out_specs=out_specs or (VMEM if not isinstance(outs, (tuple, list)) else [VMEM] * len(outs)),
        scratch_shapes=list(scratch),
        name=body.__name__,
    )


def per_device(fact_block, fact_offset, fact_date, revenue, supplier_words, date_words, candidates):
    cands = candidates.reshape(8, LANES)
    give0 = call(k0_body, [VMEM, VMEM, VMEM], here((2 * NCOL, LANES), I32))(
        supplier_words, date_words, cands
    )
    got0 = lax.all_to_all(give0.reshape(NCOL, 1, 2 * LANES), COL_SENT, 0, 0, tiled=True)
    got0 = near(got0.reshape(2 * NCOL, LANES))
    tab, cand = call(
        k1_body,
        [VMEM] * 5,
        [here((64, NDEV), F32), here((48, 1024), F32)],
        [pltpu.VMEM((NDEV, CH * LANES), BF16), pltpu.VMEM((80, CH * LANES), BF16)],
    )(
        fact_block.reshape(CH, LANES),
        fact_offset.reshape(CH, LANES),
        fact_date.reshape(CH, LANES),
        revenue.reshape(CH, LANES),
        candidates.reshape(1, 1024),
    )
    give1 = call(k2_body, [VMEM] * 3, here((NNEAR * 16, LANES), F32), [pltpu.VMEM((8, LANES), F32)])(
        got0, near(tab), near(cand)
    )
    got1 = lax.all_to_all(give1.reshape(NNEAR, 1, 16 * LANES), NEAR, 0, 0, tiled=True)
    give2 = call(k3_body, [VMEM], here((NFAR * LAST, LANES), F32))(near(got1.reshape(NNEAR * 16, LANES)))
    got2 = lax.all_to_all(give2.reshape(NFAR, 1, LAST * LANES), FAR_SENT, 0, 0, tiled=True)
    got2 = got2.reshape(NFAR * LAST, LANES)
    owned, cand, total = call(
        k4_body,
        [VMEM, VMEM],
        [shape((16, LANES), F32), shape((8, LANES), F32), shape((1, 1), F32)],
        [pltpu.VMEM((32, 64 * LANES), BF16), pltpu.VMEM((64, 64 * LANES), BF16)],
    )(near(got2), got0)
    return owned.reshape(SUP_DEV), cand.reshape(1024), total.reshape(())


def solution(mesh):
    split = Mesh(mesh.devices.reshape((2,) * 9), AXES)
    return jax.shard_map(
        per_device,
        mesh=split,
        in_specs=(P(AXES, None), P(AXES), P(AXES), P(AXES), P(COL), P(COL), P()),
        out_specs=(P(AXES), P(), P()),
        check_vma=False,
    )
```

```python
import functools

import jax
import jax.numpy as jnp
from jax import lax
from jax.experimental import pallas as pl
from jax.experimental.pallas import tpu as pltpu
from jax.sharding import Mesh
from jax.sharding import PartitionSpec as P

XH, Y2, Y1, Y0, XL, Z2, Z1, Z0, CORE = AXES = ("xh", "y2", "y1", "y0", "xl", "z2", "z1", "z0", "core")
COL = (XL, Z2, Z1, Z0, CORE)
NEAR = (Z2, Z1, Z0, CORE)
FAR = (XH, Y2, Y1, Y0, XL)
COL_SENT = (Z2, Z1, Z0, CORE, XL)
FAR_SENT = (Y0, Y1, XL, XH, Y2)

NNEAR, NFAR, NCOL, NDEV = 16, 32, 32, 512
SUP_DEV = 2048
WORDS = 69
LANES = 128
CH = 24
F32, BF16, I32 = jnp.float32, jnp.bfloat16, jnp.int32
DATES_AT = 104
LAST = 12


def iota(shape, dim):
    return lax.broadcasted_iota(I32, shape, dim)


def div30(x):
    return jnp.right_shift(x * 2185, 16)


def lane_gather(row, idx):
    table = jnp.broadcast_to(row, idx.shape)
    return jnp.take_along_axis(table, idx, axis=1, mode="promise_in_bounds")


def roll(x, shift):
    shift = shift % LANES
    return pltpu.roll(x, shift, 1) if shift else x


def lookup(words, idx):
    which, lane = jnp.right_shift(idx, 7), jnp.bitwise_and(idx, 127)
    out = lane_gather(words[0], lane)
    for i in range(1, len(words)):
        out = jnp.where(which == i, lane_gather(words[i], lane), out)
    return out


def k0_body(words_ref, dates_ref, cands_ref, out_ref):
    col = lax.axis_index(COL)
    words = [words_ref[i * LANES : (i + 1) * LANES].reshape(1, LANES) for i in range(8)]
    last = words_ref[8 * LANES : 16 * WORDS].reshape(1, 16 * WORDS - 8 * LANES)
    words.append(jnp.concatenate([last, jnp.zeros((1, 9 * LANES - 16 * WORDS), I32)], 1))
    cands = cands_ref[...]
    off = jnp.bitwise_and(cands, SUP_DEV - 1)
    block = jnp.right_shift(cands, 11) - 16 * col
    mine = (block >= 0) & (block < 16)
    slot = div30(off)
    word = lookup(words, jnp.where(mine, block * WORDS + slot, 0))
    bits = jnp.where(mine, jnp.bitwise_and(jnp.right_shift(word, off - 30 * slot), 1), 0)
    sub, lane = iota((8, LANES), 0), iota((8, LANES), 1)
    dates = jnp.concatenate([dates_ref[...].reshape(1, 3), jnp.zeros((1, LANES - 3), I32)], 1)
    dates = roll(jnp.broadcast_to(dates, (8, LANES)), DATES_AT)
    for i in range(2):
        m = 2 * sub + i
        own = lookup(words, jnp.where(lane < WORDS, m * WORDS + lane, 0))
        row = jnp.where(lane < WORDS, own, dates)
        for j in (4 * i, 4 * i + 2):
            out_ref[pl.ds(j, 8, stride=8), :] = row
            out_ref[pl.ds(j + 1, 8, stride=8), :] = roll(bits, 64 * i)


def k1_body(block_ref, off_ref, date_ref, rev_ref, cands_ref, tab_ref, cand_ref, hot_ref, val_ref):
    block, off, date = block_ref[...], off_ref[...], date_ref[...]
    rev = rev_ref[...].astype(F32)

    def key_of(b):
        return (
            jnp.bitwise_and(jnp.right_shift(b, 4), 3) * LANES
            + jnp.bitwise_and(b, 15) * 8
            + jnp.right_shift(b, 6)
        )

    key = key_of(block)
    own = iota((NDEV, LANES), 0)
    for i in range(CH):
        hot = jnp.where(own == key[i : i + 1, :], 1.0, 0.0).astype(BF16)
        hot_ref[:, i * LANES : (i + 1) * LANES] = hot
    nt = (((1,), (1,)), ((), ()))
    nn = (((1,), (0,)), ((), ()))
    dot = functools.partial(lax.dot_general, preferred_element_type=F32)
    chunk = jnp.where(
        jnp.right_shift(iota((32, CH * LANES), 1), 7) == iota((32, CH * LANES), 0), 1.0, 0.0
    ).astype(BF16)
    count = dot(chunk, hot_ref[...], nt)
    before = jnp.where(iota((32, 32), 1) < iota((32, 32), 0), 1.0, 0.0).astype(BF16)
    prefix = dot(before, count.astype(BF16), nn)
    base = dot(prefix.astype(BF16), hot_ref[...], nn)
    keys_down = jnp.transpose(jnp.concatenate([key, jnp.zeros((LANES - CH, LANES), I32)], 0))
    earlier = iota((LANES, LANES), 0) < iota((LANES, LANES), 1)
    off_hi = jnp.right_shift(off, 7)
    off_lo = jnp.bitwise_and(off, 127)
    date_q = div30(date)
    date_r = date - 30 * date_q
    date_c = jnp.right_shift(date_q * 43691, 17)
    date_l = date_c + 32 * (date_q - 3 * date_c)
    values = [off_lo.astype(F32), off_hi.astype(F32), rev, date_l.astype(F32), date_r.astype(F32)]
    slots = iota((16, LANES), 0)
    for i in range(CH):
        same = (keys_down[:, i : i + 1] == key[i : i + 1, :]) & earlier
        inside = jnp.sum(jnp.where(same, 1.0, 0.0), axis=0, keepdims=True)
        rank = inside + base[i : i + 1, i * LANES : (i + 1) * LANES]
        here = slots == rank.astype(I32)
        for g, v in enumerate(values):
            val_ref[16 * g : 16 * g + 16, i * LANES : (i + 1) * LANES] = jnp.where(
                here, v[i : i + 1, :], 0.0
            ).astype(BF16)
    table = dot(val_ref[...], hot_ref[...], nt)
    tab_ref[0:16, :] = table[0:16] + 128.0 * table[16:32]
    tab_ref[16:64, :] = table[32:80]
    cands = cands_ref[...]
    cand_key = key_of(jnp.right_shift(cands, 11))
    cand_hot = jnp.where(iota((NDEV, 1024), 0) == cand_key, 1.0, 0.0).astype(BF16)
    named = dot(table.astype(BF16), cand_hot, nn)
    cand_off = jnp.bitwise_and(cands, SUP_DEV - 1).astype(F32)
    same_off = named[0:16] + 128.0 * named[16:32] == cand_off
    cand_ref[0:16, :] = jnp.where(same_off, named[32:48], 0.0)
    cand_ref[16:48, :] = named[48:80]


def k2_body(got_ref, tab_ref, cand_ref, out_ref, tmp_ref):
    got = got_ref[pl.ds(0, NCOL, stride=2), :]
    src, lane = iota((NCOL, LANES), 0), iota((NCOL, LANES), 1)
    src = 16 * jnp.bitwise_and(src, 1) + jnp.right_shift(src, 1)
    table = jnp.zeros((NCOL, LANES), I32)
    for j in range(3):
        word = jnp.broadcast_to(got[:, DATES_AT + j : DATES_AT + j + 1], (NCOL, LANES))
        table = jnp.where(lane == 32 * j + src, word, table)
    table = jnp.sum(table, axis=0, keepdims=True)
    bits = jnp.sum(got_ref[pl.ds(1, NCOL, stride=2), :], axis=0, keepdims=True)
    row, at_lane = iota((LANES, LANES), 0), iota((LANES, LANES), 1)
    row = jnp.where(jnp.bitwise_and(at_lane, 15) >= 12, jnp.bitwise_and(row, 7), 7)
    lane8 = iota((8, LANES), 1)
    source = 4 * jnp.right_shift(lane8, 4) + jnp.bitwise_and(lane8, 3)
    bits = [lane_gather(bits, source + 32 * i).astype(F32)[0:1] for i in range(2)]

    def date_ok(where, place):
        return jnp.bitwise_and(jnp.right_shift(lane_gather(table, where.astype(I32)), place.astype(I32)), 1) == 1

    for i in range(8):
        at = slice(i * LANES, (i + 1) * LANES)
        keep = date_ok(cand_ref[16:32, at], cand_ref[32:48, at])
        tmp_ref[i : i + 1, :] = jnp.sum(jnp.where(keep, cand_ref[0:16, at], 0.0), axis=0, keepdims=True)
    part = tmp_ref[...]
    kept = []
    for i in range(4):
        at = slice(i * LANES, (i + 1) * LANES)
        keep = date_ok(tab_ref[32:48, at], tab_ref[48:64, at])
        kept.append(jnp.where(keep, tab_ref[16:32, at], 0.0))
    stack = []
    for i in range(4):
        stack += [tab_ref[0:16, i * LANES : (i + 1) * LANES], kept[i]]
    tiles = jnp.transpose(jnp.concatenate(stack, 0))
    tiles = jnp.where(row == 0, bits[0], jnp.where(row == 1, bits[1], tiles))
    for g in range(NNEAR):
        out_ref[16 * g : 16 * g + 8, :] = tiles[8 * g : 8 * g + 8]
        out_ref[16 * g + 8 : 16 * g + 16, :] = part


def k3_body(got_ref, out_ref):
    lane = iota((8, LANES), 1)
    source = 16 * jnp.right_shift(jnp.bitwise_and(lane, 31), 2) + 12 + jnp.bitwise_and(lane, 3)
    bits = jnp.zeros((8, LANES), F32)
    for j in range(4):
        rows = got_ref[pl.ds(16 * (j // 2) + j % 2, 8, stride=32), :]
        rows = jnp.take_along_axis(rows, source, axis=1, mode="promise_in_bounds")
        bits = jnp.where(jnp.right_shift(lane, 5) == j, rows, bits)
    total = got_ref[8:16, :]
    for g in range(1, NNEAR):
        total = total + got_ref[16 * g + 8 : 16 * g + 16, :]
    total = total * bits
    lane = iota((4, LANES), 1)
    for hi in range(8):
        rows = [got_ref[pl.ds(64 * q + hi, 4, stride=16), :] for q in range(4)]
        for lo in range(4):
            tile = roll(rows[0], -32 * lo)
            for q in range(1, 4):
                tile = jnp.where(jnp.right_shift(lane, 5) == q, roll(rows[q], 32 * (q - lo)), tile)
            to = 4 * hi + lo
            at = LAST * sum((to >> b & 1) << p for b, p in ((4, 1), (3, 0), (2, 3), (1, 4), (0, 2)))
            out_ref[at : at + 4, :] = jnp.where(jnp.bitwise_and(lane, 15) < 12, tile, 0.0)
            out_ref[at + 4 : at + 12, :] = total


def k4_body(got_ref, words_ref, owned_ref, cand_ref, total_ref, hi_ref, lo_ref):
    lane = iota((8, LANES), 1)
    first = jnp.bitwise_and(lane, 16) == 0
    high, low = iota((32, LANES), 0), iota((64, LANES), 0)
    high = 2 * jnp.bitwise_and(high, 15) + jnp.right_shift(high, 4)
    for p in range(8):
        even = got_ref[pl.ds(16 * LAST * (p // 4) + p % 4, 8, stride=LAST), :]
        odd = got_ref[pl.ds(16 * LAST * (p // 4) + 8 * LAST + p % 4, 8, stride=LAST), :]
        off = jnp.where(first, even, roll(odd, 16)).astype(I32)
        rev = jnp.where(first, roll(even, -16), odd)
        off_hi, off_lo = jnp.right_shift(off, 6), jnp.bitwise_and(off, 63)
        for s in range(8):
            at = slice((8 * p + s) * LANES, (8 * p + s + 1) * LANES)
            hi_ref[:, at] = jnp.where(off_hi[s : s + 1] == high, rev[s : s + 1], 0.0).astype(BF16)
            lo_ref[:, at] = jnp.where(off_lo[s : s + 1] == low, 1.0, 0.0).astype(BF16)
    owned = lax.dot_general(
        hi_ref[...], lo_ref[...], (((1,), (1,)), ((), ())), preferred_element_type=F32
    )
    owned = jnp.concatenate([owned[0:16], owned[16:32]], 1)
    far = lax.axis_index(FAR)
    words = words_ref[pl.ds(4 * jnp.bitwise_and(far, 15) + 2 * jnp.right_shift(far, 4), 1), :]
    place = iota((16, LANES), 0) * LANES + iota((16, LANES), 1)
    slot = div30(place)
    bit = jnp.bitwise_and(jnp.right_shift(lane_gather(words, slot), place - 30 * slot), 1)
    owned_ref[...] = jnp.where(bit == 1, owned, 0.0)
    cand = got_ref[4:12, :]
    for h in range(1, NFAR):
        cand = cand + got_ref[LAST * h + 4 : LAST * h + 12, :]
    cand_ref[...] = cand
    total_ref[...] = jnp.sum(jnp.sum(cand, axis=0, keepdims=True), axis=1, keepdims=True)


SMEM = pl.BlockSpec(memory_space=pltpu.SMEM)
VMEM = pl.BlockSpec(memory_space=pltpu.VMEM)
shape, here = jax.ShapeDtypeStruct, pltpu.VMEM


def near(x):
    return pltpu.with_memory_space_constraint(x, pltpu.VMEM)


def call(body, ins, outs, scratch=(), out_specs=None):
    return pl.pallas_call(
        body,
        out_shape=outs,
        in_specs=ins,
        out_specs=out_specs or (VMEM if not isinstance(outs, (tuple, list)) else [VMEM] * len(outs)),
        scratch_shapes=list(scratch),
        name=body.__name__,
    )


def per_device(fact_block, fact_offset, fact_date, revenue, supplier_words, date_words, candidates):
    cands = candidates.reshape(8, LANES)
    give0 = call(k0_body, [VMEM, VMEM, VMEM], here((2 * NCOL, LANES), I32))(
        supplier_words, date_words, cands
    )
    got0 = lax.all_to_all(give0.reshape(NCOL, 1, 2 * LANES), COL_SENT, 0, 0, tiled=True)
    got0 = near(got0.reshape(2 * NCOL, LANES))
    tab, cand = call(
        k1_body,
        [VMEM] * 5,
        [here((64, NDEV), F32), here((48, 1024), F32)],
        [pltpu.VMEM((NDEV, CH * LANES), BF16), pltpu.VMEM((80, CH * LANES), BF16)],
    )(
        fact_block.reshape(CH, LANES),
        fact_offset.reshape(CH, LANES),
        fact_date.reshape(CH, LANES),
        revenue.reshape(CH, LANES),
        candidates.reshape(1, 1024),
    )
    give1 = call(k2_body, [VMEM] * 3, here((NNEAR * 16, LANES), F32), [pltpu.VMEM((8, LANES), F32)])(
        got0, near(tab), near(cand)
    )
    got1 = lax.all_to_all(give1.reshape(NNEAR, 1, 16 * LANES), NEAR, 0, 0, tiled=True)
    give2 = call(k3_body, [VMEM], here((NFAR * LAST, LANES), F32))(near(got1.reshape(NNEAR * 16, LANES)))
    got2 = lax.all_to_all(give2.reshape(NFAR, 1, LAST * LANES), FAR_SENT, 0, 0, tiled=True)
    got2 = got2.reshape(NFAR * LAST, LANES)
    owned, cand, total = call(
        k4_body,
        [VMEM, VMEM],
        [shape((16, LANES), F32), shape((8, LANES), F32), shape((1, 1), F32)],
        [pltpu.VMEM((32, 64 * LANES), BF16), pltpu.VMEM((64, 64 * LANES), BF16)],
    )(near(got2), got0)
    return owned.reshape(SUP_DEV), cand.reshape(1024), total.reshape(())


def solution(mesh):
    split = Mesh(mesh.devices.reshape((2,) * 9), AXES)
    return jax.shard_map(
        per_device,
        mesh=split,
        in_specs=(P(AXES, None), P(AXES), P(AXES), P(AXES), P(COL), P(COL), P()),
        out_specs=(P(AXES), P(), P()),
        check_vma=False,
    )
```

```python
import functools

import jax
import jax.numpy as jnp
from jax import lax
from jax.experimental import pallas as pl
from jax.experimental.pallas import tpu as pltpu
from jax.sharding import Mesh
from jax.sharding import PartitionSpec as P

XH, Y2, Y1, Y0, XL, Z2, Z1, Z0, CORE = AXES = ("xh", "y2", "y1", "y0", "xl", "z2", "z1", "z0", "core")
COL = (XL, Z2, Z1, Z0, CORE)
NEAR = (Z0, Z1, Z2, CORE)
FAR = (XH, Y2, Y1, Y0, XL)
COL_SENT = (Z0, Z1, Z2, CORE, XL)
FAR_SENT = (Y0, Y1, Y2, XL, XH)

NNEAR, NFAR, NCOL, NDEV = 16, 32, 32, 512
SUP_DEV = 2048
WORDS = 69
LANES = 128
CH = 24
F32, BF16, I32 = jnp.float32, jnp.bfloat16, jnp.int32
DATES_AT = 104
LAST = 12


def iota(shape, dim):
    return lax.broadcasted_iota(I32, shape, dim)


def turned(z):
    low, mid = jnp.bitwise_and(z, 1), jnp.bitwise_and(z, 2)
    return 4 * low + mid + jnp.right_shift(z, 2)


def div30(x):
    return jnp.right_shift(x * 2185, 16)


def lane_gather(row, idx):
    table = jnp.broadcast_to(row, idx.shape)
    return jnp.take_along_axis(table, idx, axis=1, mode="promise_in_bounds")


def roll(x, shift):
    shift = shift % LANES
    return pltpu.roll(x, shift, 1) if shift else x


def lookup(words, idx):
    which, lane = jnp.right_shift(idx, 7), jnp.bitwise_and(idx, 127)
    out = lane_gather(words[0], lane)
    for i in range(1, len(words)):
        out = jnp.where(which == i, lane_gather(words[i], lane), out)
    return out


def k0_body(words_ref, dates_ref, cands_ref, out_ref):
    col = lax.axis_index(COL)
    words = [words_ref[i * LANES : (i + 1) * LANES].reshape(1, LANES) for i in range(8)]
    last = words_ref[8 * LANES : 16 * WORDS].reshape(1, 16 * WORDS - 8 * LANES)
    words.append(jnp.concatenate([last, jnp.zeros((1, 9 * LANES - 16 * WORDS), I32)], 1))
    cands = cands_ref[...]
    off = jnp.bitwise_and(cands, SUP_DEV - 1)
    block = jnp.right_shift(cands, 11) - 16 * col
    mine = (block >= 0) & (block < 16)
    slot = div30(off)
    word = lookup(words, jnp.where(mine, block * WORDS + slot, 0))
    bits = jnp.where(mine, jnp.bitwise_and(jnp.right_shift(word, off - 30 * slot), 1), 0)
    sub, lane = iota((8, LANES), 0), iota((8, LANES), 1)
    dates = jnp.concatenate([dates_ref[...].reshape(1, 3), jnp.zeros((1, LANES - 3), I32)], 1)
    dates = roll(jnp.broadcast_to(dates, (8, LANES)), DATES_AT)
    for i in range(2):
        m = 2 * turned(sub) + i
        own = lookup(words, jnp.where(lane < WORDS, m * WORDS + lane, 0))
        row = jnp.where(lane < WORDS, own, dates)
        for j in (4 * i, 4 * i + 2):
            out_ref[pl.ds(j, 8, stride=8), :] = row
            out_ref[pl.ds(j + 1, 8, stride=8), :] = roll(bits, 64 * i)


def k1_body(block_ref, off_ref, date_ref, rev_ref, cands_ref, tab_ref, cand_ref, hot_ref, val_ref):
    block, off, date = block_ref[...], off_ref[...], date_ref[...]
    rev = rev_ref[...].astype(F32)

    def key_of(b):
        return (
            jnp.bitwise_and(jnp.right_shift(b, 4), 3) * LANES
            + jnp.bitwise_and(b, 15) * 8
            + jnp.right_shift(b, 6)
        )

    key = key_of(block)
    own = iota((NDEV, LANES), 0)
    for i in range(CH):
        hot = jnp.where(own == key[i : i + 1, :], 1.0, 0.0).astype(BF16)
        hot_ref[:, i * LANES : (i + 1) * LANES] = hot
    nt = (((1,), (1,)), ((), ()))
    nn = (((1,), (0,)), ((), ()))
    dot = functools.partial(lax.dot_general, preferred_element_type=F32)
    chunk = jnp.where(
        jnp.right_shift(iota((32, CH * LANES), 1), 7) == iota((32, CH * LANES), 0), 1.0, 0.0
    ).astype(BF16)
    count = dot(chunk, hot_ref[...], nt)
    before = jnp.where(iota((32, 32), 1) < iota((32, 32), 0), 1.0, 0.0).astype(BF16)
    prefix = dot(before, count.astype(BF16), nn)
    base = dot(prefix.astype(BF16), hot_ref[...], nn)
    keys_down = jnp.transpose(jnp.concatenate([key, jnp.zeros((LANES - CH, LANES), I32)], 0))
    earlier = iota((LANES, LANES), 0) < iota((LANES, LANES), 1)
    off_hi = jnp.right_shift(off, 7)
    off_lo = jnp.bitwise_and(off, 127)
    date_q = div30(date)
    date_r = date - 30 * date_q
    date_c = jnp.right_shift(date_q * 43691, 17)
    date_l = date_c + 32 * (date_q - 3 * date_c)
    values = [off_lo.astype(F32), off_hi.astype(F32), rev, date_l.astype(F32), date_r.astype(F32)]
    slots = iota((16, LANES), 0)
    for i in range(CH):
        same = (keys_down[:, i : i + 1] == key[i : i + 1, :]) & earlier
        inside = jnp.sum(jnp.where(same, 1.0, 0.0), axis=0, keepdims=True)
        rank = inside + base[i : i + 1, i * LANES : (i + 1) * LANES]
        here = slots == rank.astype(I32)
        for g, v in enumerate(values):
            val_ref[16 * g : 16 * g + 16, i * LANES : (i + 1) * LANES] = jnp.where(
                here, v[i : i + 1, :], 0.0
            ).astype(BF16)
    table = dot(val_ref[...], hot_ref[...], nt)
    tab_ref[0:16, :] = table[0:16] + 128.0 * table[16:32]
    tab_ref[16:64, :] = table[32:80]
    cands = cands_ref[...]
    cand_key = key_of(jnp.right_shift(cands, 11))
    cand_hot = jnp.where(iota((NDEV, 1024), 0) == cand_key, 1.0, 0.0).astype(BF16)
    named = dot(table.astype(BF16), cand_hot, nn)
    cand_off = jnp.bitwise_and(cands, SUP_DEV - 1).astype(F32)
    same_off = named[0:16] + 128.0 * named[16:32] == cand_off
    cand_ref[0:16, :] = jnp.where(same_off, named[32:48], 0.0)
    cand_ref[16:48, :] = named[48:80]


def k2_body(got_ref, tab_ref, cand_ref, out_ref, tmp_ref):
    got = got_ref[pl.ds(0, NCOL, stride=2), :]
    src, lane = iota((NCOL, LANES), 0), iota((NCOL, LANES), 1)
    src = 16 * jnp.bitwise_and(src, 1) + 2 * turned(jnp.right_shift(src, 2)) + jnp.bitwise_and(jnp.right_shift(src, 1), 1)
    table = jnp.zeros((NCOL, LANES), I32)
    for j in range(3):
        word = jnp.broadcast_to(got[:, DATES_AT + j : DATES_AT + j + 1], (NCOL, LANES))
        table = jnp.where(lane == 32 * j + src, word, table)
    table = jnp.sum(table, axis=0, keepdims=True)
    bits = jnp.sum(got_ref[pl.ds(1, NCOL, stride=2), :], axis=0, keepdims=True)
    row, at_lane = iota((LANES, LANES), 0), iota((LANES, LANES), 1)
    row = jnp.where(jnp.bitwise_and(at_lane, 15) >= 12, jnp.bitwise_and(row, 7), 7)
    lane8 = iota((8, LANES), 1)
    source = 4 * jnp.right_shift(lane8, 4) + jnp.bitwise_and(lane8, 3)
    bits = [lane_gather(bits, source + 32 * i).astype(F32)[0:1] for i in range(2)]

    def date_ok(where, place):
        return jnp.bitwise_and(jnp.right_shift(lane_gather(table, where.astype(I32)), place.astype(I32)), 1) == 1

    for i in range(8):
        at = slice(i * LANES, (i + 1) * LANES)
        keep = date_ok(cand_ref[16:32, at], cand_ref[32:48, at])
        tmp_ref[i : i + 1, :] = jnp.sum(jnp.where(keep, cand_ref[0:16, at], 0.0), axis=0, keepdims=True)
    part = tmp_ref[...]
    kept = []
    for i in range(4):
        at = slice(i * LANES, (i + 1) * LANES)
        keep = date_ok(tab_ref[32:48, at], tab_ref[48:64, at])
        kept.append(jnp.where(keep, tab_ref[16:32, at], 0.0))
    stack = []
    for i in range(4):
        stack += [tab_ref[0:16, i * LANES : (i + 1) * LANES], kept[i]]
    tiles = jnp.transpose(jnp.concatenate(stack, 0))
    tiles = jnp.where(row == 0, bits[0], jnp.where(row == 1, bits[1], tiles))
    for g in range(NNEAR):
        at = 16 * (((g >> 1) & 1) * 8 + ((g >> 2) & 1) * 4 + ((g >> 3) & 1) * 2 + (g & 1))
        out_ref[at : at + 8, :] = tiles[8 * g : 8 * g + 8]
        out_ref[at + 8 : at + 16, :] = part


def k3_body(got_ref, out_ref):
    lane = iota((8, LANES), 1)
    source = 16 * jnp.right_shift(jnp.bitwise_and(lane, 31), 2) + 12 + jnp.bitwise_and(lane, 3)
    bits = jnp.zeros((8, LANES), F32)
    for j in range(4):
        rows = got_ref[pl.ds(16 * (j // 2) + j % 2, 8, stride=32), :]
        rows = jnp.take_along_axis(rows, source, axis=1, mode="promise_in_bounds")
        bits = jnp.where(jnp.right_shift(lane, 5) == j, rows, bits)
    total = got_ref[8:16, :]
    for g in range(1, NNEAR):
        total = total + got_ref[16 * g + 8 : 16 * g + 16, :]
    total = total * bits
    lane = iota((4, LANES), 1)
    for hi in range(8):
        rows = [got_ref[pl.ds(64 * q + hi, 4, stride=16), :] for q in range(4)]
        for lo in range(4):
            tile = roll(rows[0], -32 * lo)
            for q in range(1, 4):
                tile = jnp.where(jnp.right_shift(lane, 5) == q, roll(rows[q], 32 * (q - lo)), tile)
            to = 4 * hi + lo
            at = LAST * sum((to >> b & 1) << p for b, p in ((4, 0), (3, 2), (2, 3), (1, 4), (0, 1)))
            out_ref[at : at + 4, :] = jnp.where(jnp.bitwise_and(lane, 15) < 12, tile, 0.0)
            out_ref[at + 4 : at + 12, :] = total


def k4_body(got_ref, words_ref, owned_ref, cand_ref, total_ref, hi_ref, lo_ref):
    lane = iota((8, LANES), 1)
    first = jnp.bitwise_and(lane, 16) == 0
    high, low = iota((32, LANES), 0), iota((64, LANES), 0)
    high = 2 * jnp.bitwise_and(high, 15) + jnp.right_shift(high, 4)
    for p in range(8):
        even = got_ref[pl.ds(16 * LAST * (p // 4) + p % 4, 8, stride=LAST), :]
        odd = got_ref[pl.ds(16 * LAST * (p // 4) + 8 * LAST + p % 4, 8, stride=LAST), :]
        off = jnp.where(first, even, roll(odd, 16)).astype(I32)
        rev = jnp.where(first, roll(even, -16), odd)
        off_hi, off_lo = jnp.right_shift(off, 6), jnp.bitwise_and(off, 63)
        for s in range(8):
            at = slice((8 * p + s) * LANES, (8 * p + s + 1) * LANES)
            hi_ref[:, at] = jnp.where(off_hi[s : s + 1] == high, rev[s : s + 1], 0.0).astype(BF16)
            lo_ref[:, at] = jnp.where(off_lo[s : s + 1] == low, 1.0, 0.0).astype(BF16)
    owned = lax.dot_general(
        hi_ref[...], lo_ref[...], (((1,), (1,)), ((), ())), preferred_element_type=F32
    )
    owned = jnp.concatenate([owned[0:16], owned[16:32]], 1)
    far = lax.axis_index(FAR)
    row = 4 * turned(jnp.bitwise_and(jnp.right_shift(far, 1), 7)) + 2 * jnp.bitwise_and(far, 1)
    words = words_ref[pl.ds(2 * (row + jnp.right_shift(far, 4)), 1), :]
    place = iota((16, LANES), 0) * LANES + iota((16, LANES), 1)
    slot = div30(place)
    bit = jnp.bitwise_and(jnp.right_shift(lane_gather(words, slot), place - 30 * slot), 1)
    owned_ref[...] = jnp.where(bit == 1, owned, 0.0)
    cand = got_ref[4:12, :]
    for h in range(1, NFAR):
        cand = cand + got_ref[LAST * h + 4 : LAST * h + 12, :]
    cand_ref[...] = cand
    total_ref[...] = jnp.sum(jnp.sum(cand, axis=0, keepdims=True), axis=1, keepdims=True)


SMEM = pl.BlockSpec(memory_space=pltpu.SMEM)
VMEM = pl.BlockSpec(memory_space=pltpu.VMEM)
shape, here = jax.ShapeDtypeStruct, pltpu.VMEM


def near(x):
    return pltpu.with_memory_space_constraint(x, pltpu.VMEM)


def call(body, ins, outs, scratch=(), out_specs=None):
    return pl.pallas_call(
        body,
        out_shape=outs,
        in_specs=ins,
        out_specs=out_specs or (VMEM if not isinstance(outs, (tuple, list)) else [VMEM] * len(outs)),
        scratch_shapes=list(scratch),
        name=body.__name__,
    )


def per_device(fact_block, fact_offset, fact_date, revenue, supplier_words, date_words, candidates):
    cands = candidates.reshape(8, LANES)
    give0 = call(k0_body, [VMEM, VMEM, VMEM], here((2 * NCOL, LANES), I32))(
        supplier_words, date_words, cands
    )
    got0 = lax.all_to_all(give0.reshape(NCOL, 1, 2 * LANES), COL_SENT, 0, 0, tiled=True)
    got0 = near(got0.reshape(2 * NCOL, LANES))
    tab, cand = call(
        k1_body,
        [VMEM] * 5,
        [here((64, NDEV), F32), here((48, 1024), F32)],
        [pltpu.VMEM((NDEV, CH * LANES), BF16), pltpu.VMEM((80, CH * LANES), BF16)],
    )(
        fact_block.reshape(CH, LANES),
        fact_offset.reshape(CH, LANES),
        fact_date.reshape(CH, LANES),
        revenue.reshape(CH, LANES),
        candidates.reshape(1, 1024),
    )
    give1 = call(k2_body, [VMEM] * 3, here((NNEAR * 16, LANES), F32), [pltpu.VMEM((8, LANES), F32)])(
        got0, near(tab), near(cand)
    )
    got1 = lax.all_to_all(give1.reshape(NNEAR, 1, 16 * LANES), NEAR, 0, 0, tiled=True)
    give2 = call(k3_body, [VMEM], here((NFAR * LAST, LANES), F32))(near(got1.reshape(NNEAR * 16, LANES)))
    got2 = lax.all_to_all(give2.reshape(NFAR, 1, LAST * LANES), FAR_SENT, 0, 0, tiled=True)
    got2 = got2.reshape(NFAR * LAST, LANES)
    owned, cand, total = call(
        k4_body,
        [VMEM, VMEM],
        [shape((16, LANES), F32), shape((8, LANES), F32), shape((1, 1), F32)],
        [pltpu.VMEM((32, 64 * LANES), BF16), pltpu.VMEM((64, 64 * LANES), BF16)],
    )(near(got2), got0)
    return owned.reshape(SUP_DEV), cand.reshape(1024), total.reshape(())


def solution(mesh):
    split = Mesh(mesh.devices.reshape((2,) * 9), AXES)
    return jax.shard_map(
        per_device,
        mesh=split,
        in_specs=(P(AXES, None), P(AXES), P(AXES), P(AXES), P(COL), P(COL), P()),
        out_specs=(P(AXES), P(), P()),
        check_vma=False,
    )
```

```python
import functools

import jax
import jax.numpy as jnp
from jax import lax
from jax.experimental import pallas as pl
from jax.experimental.pallas import tpu as pltpu
from jax.sharding import Mesh
from jax.sharding import PartitionSpec as P

XH, Y2, Y1, Y0, XL, Z2, Z1, Z0, CORE = AXES = ("xh", "y2", "y1", "y0", "xl", "z2", "z1", "z0", "core")
COL = (XL, Z2, Z1, Z0, CORE)
NEAR = (Z2, Z1, Z0, CORE)
FAR = (XH, Y2, Y1, Y0, XL)
COL_SENT = (Z2, Z1, Z0, CORE, XL)
FAR_SENT = (Y0, Y1, Y2, XH, XL)

NNEAR, NFAR, NCOL, NDEV = 16, 32, 32, 512
SUP_DEV = 2048
WORDS = 69
LANES = 128
CH = 24
F32, BF16, I32 = jnp.float32, jnp.bfloat16, jnp.int32
DATES_AT = 104
LAST = 12


def iota(shape, dim):
    return lax.broadcasted_iota(I32, shape, dim)


def div30(x):
    return jnp.right_shift(x * 2185, 16)


def lane_gather(row, idx):
    table = jnp.broadcast_to(row, idx.shape)
    return jnp.take_along_axis(table, idx, axis=1, mode="promise_in_bounds")


def roll(x, shift):
    shift = shift % LANES
    return pltpu.roll(x, shift, 1) if shift else x


def lookup(words, idx):
    which, lane = jnp.right_shift(idx, 7), jnp.bitwise_and(idx, 127)
    out = lane_gather(words[0], lane)
    for i in range(1, len(words)):
        out = jnp.where(which == i, lane_gather(words[i], lane), out)
    return out


def k0_body(words_ref, dates_ref, cands_ref, out_ref):
    col = lax.axis_index(COL)
    words = [words_ref[i * LANES : (i + 1) * LANES].reshape(1, LANES) for i in range(8)]
    last = words_ref[8 * LANES : 16 * WORDS].reshape(1, 16 * WORDS - 8 * LANES)
    words.append(jnp.concatenate([last, jnp.zeros((1, 9 * LANES - 16 * WORDS), I32)], 1))
    cands = cands_ref[...]
    off = jnp.bitwise_and(cands, SUP_DEV - 1)
    block = jnp.right_shift(cands, 11) - 16 * col
    mine = (block >= 0) & (block < 16)
    slot = div30(off)
    word = lookup(words, jnp.where(mine, block * WORDS + slot, 0))
    bits = jnp.where(mine, jnp.bitwise_and(jnp.right_shift(word, off - 30 * slot), 1), 0)
    sub, lane = iota((8, LANES), 0), iota((8, LANES), 1)
    dates = jnp.concatenate([dates_ref[...].reshape(1, 3), jnp.zeros((1, LANES - 3), I32)], 1)
    dates = roll(jnp.broadcast_to(dates, (8, LANES)), DATES_AT)
    for i in range(2):
        m = 2 * sub + i
        own = lookup(words, jnp.where(lane < WORDS, m * WORDS + lane, 0))
        row = jnp.where(lane < WORDS, own, dates)
        for j in (4 * i, 4 * i + 2):
            out_ref[pl.ds(j, 8, stride=8), :] = row
            out_ref[pl.ds(j + 1, 8, stride=8), :] = roll(bits, 64 * i)


def k1_body(block_ref, off_ref, date_ref, rev_ref, cands_ref, tab_ref, cand_ref, hot_ref, val_ref):
    block, off, date = block_ref[...], off_ref[...], date_ref[...]
    rev = rev_ref[...].astype(F32)

    def key_of(b):
        return (
            jnp.bitwise_and(jnp.right_shift(b, 4), 3) * LANES
            + jnp.bitwise_and(b, 15) * 8
            + jnp.right_shift(b, 6)
        )

    key = key_of(block)
    own = iota((NDEV, LANES), 0)
    for i in range(CH):
        hot = jnp.where(own == key[i : i + 1, :], 1.0, 0.0).astype(BF16)
        hot_ref[:, i * LANES : (i + 1) * LANES] = hot
    nt = (((1,), (1,)), ((), ()))
    nn = (((1,), (0,)), ((), ()))
    dot = functools.partial(lax.dot_general, preferred_element_type=F32)
    chunk = jnp.where(
        jnp.right_shift(iota((32, CH * LANES), 1), 7) == iota((32, CH * LANES), 0), 1.0, 0.0
    ).astype(BF16)
    count = dot(chunk, hot_ref[...], nt)
    before = jnp.where(iota((32, 32), 1) < iota((32, 32), 0), 1.0, 0.0).astype(BF16)
    prefix = dot(before, count.astype(BF16), nn)
    base = dot(prefix.astype(BF16), hot_ref[...], nn)
    keys_down = jnp.transpose(jnp.concatenate([key, jnp.zeros((LANES - CH, LANES), I32)], 0))
    earlier = iota((LANES, LANES), 0) < iota((LANES, LANES), 1)
    off_hi = jnp.right_shift(off, 7)
    off_lo = jnp.bitwise_and(off, 127)
    date_q = div30(date)
    date_r = date - 30 * date_q
    date_c = jnp.right_shift(date_q * 43691, 17)
    date_l = date_c + 32 * (date_q - 3 * date_c)
    values = [off_lo.astype(F32), off_hi.astype(F32), rev, date_l.astype(F32), date_r.astype(F32)]
    slots = iota((16, LANES), 0)
    for i in range(CH):
        same = (keys_down[:, i : i + 1] == key[i : i + 1, :]) & earlier
        inside = jnp.sum(jnp.where(same, 1.0, 0.0), axis=0, keepdims=True)
        rank = inside + base[i : i + 1, i * LANES : (i + 1) * LANES]
        here = slots == rank.astype(I32)
        for g, v in enumerate(values):
            val_ref[16 * g : 16 * g + 16, i * LANES : (i + 1) * LANES] = jnp.where(
                here, v[i : i + 1, :], 0.0
            ).astype(BF16)
    table = dot(val_ref[...], hot_ref[...], nt)
    tab_ref[0:16, :] = table[0:16] + 128.0 * table[16:32]
    tab_ref[16:64, :] = table[32:80]
    cands = cands_ref[...]
    cand_key = key_of(jnp.right_shift(cands, 11))
    cand_hot = jnp.where(iota((NDEV, 1024), 0) == cand_key, 1.0, 0.0).astype(BF16)
    named = dot(table.astype(BF16), cand_hot, nn)
    cand_off = jnp.bitwise_and(cands, SUP_DEV - 1).astype(F32)
    same_off = named[0:16] + 128.0 * named[16:32] == cand_off
    cand_ref[0:16, :] = jnp.where(same_off, named[32:48], 0.0)
    cand_ref[16:48, :] = named[48:80]


def k2_body(got_ref, tab_ref, cand_ref, out_ref, tmp_ref):
    got = got_ref[pl.ds(0, NCOL, stride=2), :]
    src, lane = iota((NCOL, LANES), 0), iota((NCOL, LANES), 1)
    src = 16 * jnp.bitwise_and(src, 1) + jnp.right_shift(src, 1)
    table = jnp.zeros((NCOL, LANES), I32)
    for j in range(3):
        word = jnp.broadcast_to(got[:, DATES_AT + j : DATES_AT + j + 1], (NCOL, LANES))
        table = jnp.where(lane == 32 * j + src, word, table)
    table = jnp.sum(table, axis=0, keepdims=True)
    bits = jnp.sum(got_ref[pl.ds(1, NCOL, stride=2), :], axis=0, keepdims=True)
    row, at_lane = iota((LANES, LANES), 0), iota((LANES, LANES), 1)
    row = jnp.where(jnp.bitwise_and(at_lane, 15) >= 12, jnp.bitwise_and(row, 7), 7)
    lane8 = iota((8, LANES), 1)
    source = 4 * jnp.right_shift(lane8, 4) + jnp.bitwise_and(lane8, 3)
    bits = [lane_gather(bits, source + 32 * i).astype(F32)[0:1] for i in range(2)]

    def date_ok(where, place):
        return jnp.bitwise_and(jnp.right_shift(lane_gather(table, where.astype(I32)), place.astype(I32)), 1) == 1

    for i in range(8):
        at = slice(i * LANES, (i + 1) * LANES)
        keep = date_ok(cand_ref[16:32, at], cand_ref[32:48, at])
        tmp_ref[i : i + 1, :] = jnp.sum(jnp.where(keep, cand_ref[0:16, at], 0.0), axis=0, keepdims=True)
    part = tmp_ref[...]
    kept = []
    for i in range(4):
        at = slice(i * LANES, (i + 1) * LANES)
        keep = date_ok(tab_ref[32:48, at], tab_ref[48:64, at])
        kept.append(jnp.where(keep, tab_ref[16:32, at], 0.0))
    stack = []
    for i in range(4):
        stack += [tab_ref[0:16, i * LANES : (i + 1) * LANES], kept[i]]
    tiles = jnp.transpose(jnp.concatenate(stack, 0))
    tiles = jnp.where(row == 0, bits[0], jnp.where(row == 1, bits[1], tiles))
    for g in range(NNEAR):
        out_ref[16 * g : 16 * g + 8, :] = tiles[8 * g : 8 * g + 8]
        out_ref[16 * g + 8 : 16 * g + 16, :] = part


def k3_body(got_ref, out_ref):
    lane = iota((8, LANES), 1)
    source = 16 * jnp.right_shift(jnp.bitwise_and(lane, 31), 2) + 12 + jnp.bitwise_and(lane, 3)
    bits = jnp.zeros((8, LANES), F32)
    for j in range(4):
        rows = got_ref[pl.ds(16 * (j // 2) + j % 2, 8, stride=32), :]
        rows = jnp.take_along_axis(rows, source, axis=1, mode="promise_in_bounds")
        bits = jnp.where(jnp.right_shift(lane, 5) == j, rows, bits)
    total = got_ref[8:16, :]
    for g in range(1, NNEAR):
        total = total + got_ref[16 * g + 8 : 16 * g + 16, :]
    total = total * bits
    lane = iota((4, LANES), 1)
    for hi in range(8):
        rows = [got_ref[pl.ds(64 * q + hi, 4, stride=16), :] for q in range(4)]
        for lo in range(4):
            tile = roll(rows[0], -32 * lo)
            for q in range(1, 4):
                tile = jnp.where(jnp.right_shift(lane, 5) == q, roll(rows[q], 32 * (q - lo)), tile)
            to = 4 * hi + lo
            at = LAST * sum((to >> b & 1) << p for b, p in ((4, 1), (3, 2), (2, 3), (1, 4), (0, 0)))
            out_ref[at : at + 4, :] = jnp.where(jnp.bitwise_and(lane, 15) < 12, tile, 0.0)
            out_ref[at + 4 : at + 12, :] = total


def k4_body(got_ref, words_ref, owned_ref, cand_ref, total_ref, hi_ref, lo_ref):
    lane = iota((8, LANES), 1)
    first = jnp.bitwise_and(lane, 16) == 0
    high, low = iota((32, LANES), 0), iota((64, LANES), 0)
    high = 2 * jnp.bitwise_and(high, 15) + jnp.right_shift(high, 4)
    for p in range(8):
        even = got_ref[pl.ds(16 * LAST * (p // 4) + p % 4, 8, stride=LAST), :]
        odd = got_ref[pl.ds(16 * LAST * (p // 4) + 8 * LAST + p % 4, 8, stride=LAST), :]
        off = jnp.where(first, even, roll(odd, 16)).astype(I32)
        rev = jnp.where(first, roll(even, -16), odd)
        off_hi, off_lo = jnp.right_shift(off, 6), jnp.bitwise_and(off, 63)
        for s in range(8):
            at = slice((8 * p + s) * LANES, (8 * p + s + 1) * LANES)
            hi_ref[:, at] = jnp.where(off_hi[s : s + 1] == high, rev[s : s + 1], 0.0).astype(BF16)
            lo_ref[:, at] = jnp.where(off_lo[s : s + 1] == low, 1.0, 0.0).astype(BF16)
    owned = lax.dot_general(
        hi_ref[...], lo_ref[...], (((1,), (1,)), ((), ())), preferred_element_type=F32
    )
    owned = jnp.concatenate([owned[0:16], owned[16:32]], 1)
    far = lax.axis_index(FAR)
    words = words_ref[pl.ds(4 * jnp.bitwise_and(far, 15) + 2 * jnp.right_shift(far, 4), 1), :]
    place = iota((16, LANES), 0) * LANES + iota((16, LANES), 1)
    slot = div30(place)
    bit = jnp.bitwise_and(jnp.right_shift(lane_gather(words, slot), place - 30 * slot), 1)
    owned_ref[...] = jnp.where(bit == 1, owned, 0.0)
    cand = got_ref[4:12, :]
    for h in range(1, NFAR):
        cand = cand + got_ref[LAST * h + 4 : LAST * h + 12, :]
    cand_ref[...] = cand
    total_ref[...] = jnp.sum(jnp.sum(cand, axis=0, keepdims=True), axis=1, keepdims=True)


SMEM = pl.BlockSpec(memory_space=pltpu.SMEM)
VMEM = pl.BlockSpec(memory_space=pltpu.VMEM)
shape, here = jax.ShapeDtypeStruct, pltpu.VMEM


def near(x):
    return pltpu.with_memory_space_constraint(x, pltpu.VMEM)


def call(body, ins, outs, scratch=(), out_specs=None):
    return pl.pallas_call(
        body,
        out_shape=outs,
        in_specs=ins,
        out_specs=out_specs or (VMEM if not isinstance(outs, (tuple, list)) else [VMEM] * len(outs)),
        scratch_shapes=list(scratch),
        name=body.__name__,
    )


def per_device(fact_block, fact_offset, fact_date, revenue, supplier_words, date_words, candidates):
    cands = candidates.reshape(8, LANES)
    give0 = call(k0_body, [VMEM, VMEM, VMEM], here((2 * NCOL, LANES), I32))(
        supplier_words, date_words, cands
    )
    got0 = lax.all_to_all(give0.reshape(NCOL, 1, 2 * LANES), COL_SENT, 0, 0, tiled=True)
    got0 = near(got0.reshape(2 * NCOL, LANES))
    tab, cand = call(
        k1_body,
        [VMEM] * 5,
        [here((64, NDEV), F32), here((48, 1024), F32)],
        [pltpu.VMEM((NDEV, CH * LANES), BF16), pltpu.VMEM((80, CH * LANES), BF16)],
    )(
        fact_block.reshape(CH, LANES),
        fact_offset.reshape(CH, LANES),
        fact_date.reshape(CH, LANES),
        revenue.reshape(CH, LANES),
        candidates.reshape(1, 1024),
    )
    give1 = call(k2_body, [VMEM] * 3, here((NNEAR * 16, LANES), F32), [pltpu.VMEM((8, LANES), F32)])(
        got0, near(tab), near(cand)
    )
    got1 = lax.all_to_all(give1.reshape(NNEAR, 1, 16 * LANES), NEAR, 0, 0, tiled=True)
    give2 = call(k3_body, [VMEM], here((NFAR * LAST, LANES), F32))(near(got1.reshape(NNEAR * 16, LANES)))
    got2 = lax.all_to_all(give2.reshape(NFAR, 1, LAST * LANES), FAR_SENT, 0, 0, tiled=True)
    got2 = got2.reshape(NFAR * LAST, LANES)
    owned, cand, total = call(
        k4_body,
        [VMEM, VMEM],
        [shape((16, LANES), F32), shape((8, LANES), F32), shape((1, 1), F32)],
        [pltpu.VMEM((32, 64 * LANES), BF16), pltpu.VMEM((64, 64 * LANES), BF16)],
    )(near(got2), got0)
    return owned.reshape(SUP_DEV), cand.reshape(1024), total.reshape(())


def solution(mesh):
    split = Mesh(mesh.devices.reshape((2,) * 9), AXES)
    return jax.shard_map(
        per_device,
        mesh=split,
        in_specs=(P(AXES, None), P(AXES), P(AXES), P(AXES), P(COL), P(COL), P()),
        out_specs=(P(AXES), P(), P()),
        check_vma=False,
    )
```

```python
import functools

import jax
import jax.numpy as jnp
from jax import lax
from jax.experimental import pallas as pl
from jax.experimental.pallas import tpu as pltpu
from jax.sharding import Mesh
from jax.sharding import PartitionSpec as P

XH, Y2, Y1, Y0, XL, Z2, Z1, Z0, CORE = AXES = ("xh", "y2", "y1", "y0", "xl", "z2", "z1", "z0", "core")
COL = (XL, Z2, Z1, Z0, CORE)
NEAR = (Z2, Z1, Z0, CORE)
FAR = (XH, Y2, Y1, Y0, XL)
COL_SENT = (Z2, Z1, Z0, CORE, XL)
FAR_SENT = (XL, Y0, Y1, Y2, XH)

NNEAR, NFAR, NCOL, NDEV = 16, 32, 32, 512
SUP_DEV = 2048
WORDS = 69
LANES = 128
CH = 24
F32, BF16, I32 = jnp.float32, jnp.bfloat16, jnp.int32
DATES_AT = 104
LAST = 12


def iota(shape, dim):
    return lax.broadcasted_iota(I32, shape, dim)


def div30(x):
    return jnp.right_shift(x * 2185, 16)


def lane_gather(row, idx):
    table = jnp.broadcast_to(row, idx.shape)
    return jnp.take_along_axis(table, idx, axis=1, mode="promise_in_bounds")


def roll(x, shift):
    shift = shift % LANES
    return pltpu.roll(x, shift, 1) if shift else x


def lookup(words, idx):
    which, lane = jnp.right_shift(idx, 7), jnp.bitwise_and(idx, 127)
    out = lane_gather(words[0], lane)
    for i in range(1, len(words)):
        out = jnp.where(which == i, lane_gather(words[i], lane), out)
    return out


def k0_body(words_ref, dates_ref, cands_ref, out_ref):
    col = lax.axis_index(COL)
    words = [words_ref[i * LANES : (i + 1) * LANES].reshape(1, LANES) for i in range(8)]
    last = words_ref[8 * LANES : 16 * WORDS].reshape(1, 16 * WORDS - 8 * LANES)
    words.append(jnp.concatenate([last, jnp.zeros((1, 9 * LANES - 16 * WORDS), I32)], 1))
    cands = cands_ref[...]
    off = jnp.bitwise_and(cands, SUP_DEV - 1)
    block = jnp.right_shift(cands, 11) - 16 * col
    mine = (block >= 0) & (block < 16)
    slot = div30(off)
    word = lookup(words, jnp.where(mine, block * WORDS + slot, 0))
    bits = jnp.where(mine, jnp.bitwise_and(jnp.right_shift(word, off - 30 * slot), 1), 0)
    sub, lane = iota((8, LANES), 0), iota((8, LANES), 1)
    dates = jnp.concatenate([dates_ref[...].reshape(1, 3), jnp.zeros((1, LANES - 3), I32)], 1)
    dates = roll(jnp.broadcast_to(dates, (8, LANES)), DATES_AT)
    for i in range(2):
        m = 2 * sub + i
        own = lookup(words, jnp.where(lane < WORDS, m * WORDS + lane, 0))
        row = jnp.where(lane < WORDS, own, dates)
        for j in (4 * i, 4 * i + 2):
            out_ref[pl.ds(j, 8, stride=8), :] = row
            out_ref[pl.ds(j + 1, 8, stride=8), :] = roll(bits, 64 * i)


def k1_body(block_ref, off_ref, date_ref, rev_ref, cands_ref, tab_ref, cand_ref, hot_ref, val_ref):
    block, off, date = block_ref[...], off_ref[...], date_ref[...]
    rev = rev_ref[...].astype(F32)

    def key_of(b):
        return (
            jnp.bitwise_and(jnp.right_shift(b, 4), 3) * LANES
            + jnp.bitwise_and(b, 15) * 8
            + jnp.right_shift(b, 6)
        )

    key = key_of(block)
    own = iota((NDEV, LANES), 0)
    for i in range(CH):
        hot = jnp.where(own == key[i : i + 1, :], 1.0, 0.0).astype(BF16)
        hot_ref[:, i * LANES : (i + 1) * LANES] = hot
    nt = (((1,), (1,)), ((), ()))
    nn = (((1,), (0,)), ((), ()))
    dot = functools.partial(lax.dot_general, preferred_element_type=F32)
    chunk = jnp.where(
        jnp.right_shift(iota((32, CH * LANES), 1), 7) == iota((32, CH * LANES), 0), 1.0, 0.0
    ).astype(BF16)
    count = dot(chunk, hot_ref[...], nt)
    before = jnp.where(iota((32, 32), 1) < iota((32, 32), 0), 1.0, 0.0).astype(BF16)
    prefix = dot(before, count.astype(BF16), nn)
    base = dot(prefix.astype(BF16), hot_ref[...], nn)
    keys_down = jnp.transpose(jnp.concatenate([key, jnp.zeros((LANES - CH, LANES), I32)], 0))
    earlier = iota((LANES, LANES), 0) < iota((LANES, LANES), 1)
    off_hi = jnp.right_shift(off, 7)
    off_lo = jnp.bitwise_and(off, 127)
    date_q = div30(date)
    date_r = date - 30 * date_q
    date_c = jnp.right_shift(date_q * 43691, 17)
    date_l = date_c + 32 * (date_q - 3 * date_c)
    values = [off_lo.astype(F32), off_hi.astype(F32), rev, date_l.astype(F32), date_r.astype(F32)]
    slots = iota((16, LANES), 0)
    for i in range(CH):
        same = (keys_down[:, i : i + 1] == key[i : i + 1, :]) & earlier
        inside = jnp.sum(jnp.where(same, 1.0, 0.0), axis=0, keepdims=True)
        rank = inside + base[i : i + 1, i * LANES : (i + 1) * LANES]
        here = slots == rank.astype(I32)
        for g, v in enumerate(values):
            val_ref[16 * g : 16 * g + 16, i * LANES : (i + 1) * LANES] = jnp.where(
                here, v[i : i + 1, :], 0.0
            ).astype(BF16)
    table = dot(val_ref[...], hot_ref[...], nt)
    tab_ref[0:16, :] = table[0:16] + 128.0 * table[16:32]
    tab_ref[16:64, :] = table[32:80]
    cands = cands_ref[...]
    cand_key = key_of(jnp.right_shift(cands, 11))
    cand_hot = jnp.where(iota((NDEV, 1024), 0) == cand_key, 1.0, 0.0).astype(BF16)
    named = dot(table.astype(BF16), cand_hot, nn)
    cand_off = jnp.bitwise_and(cands, SUP_DEV - 1).astype(F32)
    same_off = named[0:16] + 128.0 * named[16:32] == cand_off
    cand_ref[0:16, :] = jnp.where(same_off, named[32:48], 0.0)
    cand_ref[16:48, :] = named[48:80]


def k2_body(got_ref, tab_ref, cand_ref, out_ref, tmp_ref):
    got = got_ref[pl.ds(0, NCOL, stride=2), :]
    src, lane = iota((NCOL, LANES), 0), iota((NCOL, LANES), 1)
    src = 16 * jnp.bitwise_and(src, 1) + jnp.right_shift(src, 1)
    table = jnp.zeros((NCOL, LANES), I32)
    for j in range(3):
        word = jnp.broadcast_to(got[:, DATES_AT + j : DATES_AT + j + 1], (NCOL, LANES))
        table = jnp.where(lane == 32 * j + src, word, table)
    table = jnp.sum(table, axis=0, keepdims=True)
    bits = jnp.sum(got_ref[pl.ds(1, NCOL, stride=2), :], axis=0, keepdims=True)
    row, at_lane = iota((LANES, LANES), 0), iota((LANES, LANES), 1)
    row = jnp.where(jnp.bitwise_and(at_lane, 15) >= 12, jnp.bitwise_and(row, 7), 7)
    lane8 = iota((8, LANES), 1)
    source = 4 * jnp.right_shift(lane8, 4) + jnp.bitwise_and(lane8, 3)
    bits = [lane_gather(bits, source + 32 * i).astype(F32)[0:1] for i in range(2)]

    def date_ok(where, place):
        return jnp.bitwise_and(jnp.right_shift(lane_gather(table, where.astype(I32)), place.astype(I32)), 1) == 1

    for i in range(8):
        at = slice(i * LANES, (i + 1) * LANES)
        keep = date_ok(cand_ref[16:32, at], cand_ref[32:48, at])
        tmp_ref[i : i + 1, :] = jnp.sum(jnp.where(keep, cand_ref[0:16, at], 0.0), axis=0, keepdims=True)
    part = tmp_ref[...]
    kept = []
    for i in range(4):
        at = slice(i * LANES, (i + 1) * LANES)
        keep = date_ok(tab_ref[32:48, at], tab_ref[48:64, at])
        kept.append(jnp.where(keep, tab_ref[16:32, at], 0.0))
    stack = []
    for i in range(4):
        stack += [tab_ref[0:16, i * LANES : (i + 1) * LANES], kept[i]]
    tiles = jnp.transpose(jnp.concatenate(stack, 0))
    tiles = jnp.where(row == 0, bits[0], jnp.where(row == 1, bits[1], tiles))
    for g in range(NNEAR):
        out_ref[16 * g : 16 * g + 8, :] = tiles[8 * g : 8 * g + 8]
        out_ref[16 * g + 8 : 16 * g + 16, :] = part


def k3_body(got_ref, out_ref):
    lane = iota((8, LANES), 1)
    source = 16 * jnp.right_shift(jnp.bitwise_and(lane, 31), 2) + 12 + jnp.bitwise_and(lane, 3)
    bits = jnp.zeros((8, LANES), F32)
    for j in range(4):
        rows = got_ref[pl.ds(16 * (j // 2) + j % 2, 8, stride=32), :]
        rows = jnp.take_along_axis(rows, source, axis=1, mode="promise_in_bounds")
        bits = jnp.where(jnp.right_shift(lane, 5) == j, rows, bits)
    total = got_ref[8:16, :]
    for g in range(1, NNEAR):
        total = total + got_ref[16 * g + 8 : 16 * g + 16, :]
    total = total * bits
    lane = iota((4, LANES), 1)
    for hi in range(8):
        rows = [got_ref[pl.ds(64 * q + hi, 4, stride=16), :] for q in range(4)]
        for lo in range(4):
            tile = roll(rows[0], -32 * lo)
            for q in range(1, 4):
                tile = jnp.where(jnp.right_shift(lane, 5) == q, roll(rows[q], 32 * (q - lo)), tile)
            to = 4 * hi + lo
            at = LAST * sum((to >> b & 1) << p for b, p in ((4, 0), (3, 1), (2, 2), (1, 3), (0, 4)))
            out_ref[at : at + 4, :] = jnp.where(jnp.bitwise_and(lane, 15) < 12, tile, 0.0)
            out_ref[at + 4 : at + 12, :] = total


def k4_body(got_ref, words_ref, owned_ref, cand_ref, total_ref, hi_ref, lo_ref):
    lane = iota((8, LANES), 1)
    first = jnp.bitwise_and(lane, 16) == 0
    high, low = iota((32, LANES), 0), iota((64, LANES), 0)
    high = 2 * jnp.bitwise_and(high, 15) + jnp.right_shift(high, 4)
    for p in range(8):
        even = got_ref[pl.ds(16 * LAST * (p // 4) + p % 4, 8, stride=LAST), :]
        odd = got_ref[pl.ds(16 * LAST * (p // 4) + 8 * LAST + p % 4, 8, stride=LAST), :]
        off = jnp.where(first, even, roll(odd, 16)).astype(I32)
        rev = jnp.where(first, roll(even, -16), odd)
        off_hi, off_lo = jnp.right_shift(off, 6), jnp.bitwise_and(off, 63)
        for s in range(8):
            at = slice((8 * p + s) * LANES, (8 * p + s + 1) * LANES)
            hi_ref[:, at] = jnp.where(off_hi[s : s + 1] == high, rev[s : s + 1], 0.0).astype(BF16)
            lo_ref[:, at] = jnp.where(off_lo[s : s + 1] == low, 1.0, 0.0).astype(BF16)
    owned = lax.dot_general(
        hi_ref[...], lo_ref[...], (((1,), (1,)), ((), ())), preferred_element_type=F32
    )
    owned = jnp.concatenate([owned[0:16], owned[16:32]], 1)
    far = lax.axis_index(FAR)
    words = words_ref[pl.ds(4 * jnp.bitwise_and(far, 15) + 2 * jnp.right_shift(far, 4), 1), :]
    place = iota((16, LANES), 0) * LANES + iota((16, LANES), 1)
    slot = div30(place)
    bit = jnp.bitwise_and(jnp.right_shift(lane_gather(words, slot), place - 30 * slot), 1)
    owned_ref[...] = jnp.where(bit == 1, owned, 0.0)
    cand = got_ref[4:12, :]
    for h in range(1, NFAR):
        cand = cand + got_ref[LAST * h + 4 : LAST * h + 12, :]
    cand_ref[...] = cand
    total_ref[...] = jnp.sum(jnp.sum(cand, axis=0, keepdims=True), axis=1, keepdims=True)


SMEM = pl.BlockSpec(memory_space=pltpu.SMEM)
VMEM = pl.BlockSpec(memory_space=pltpu.VMEM)
shape, here = jax.ShapeDtypeStruct, pltpu.VMEM


def near(x):
    return pltpu.with_memory_space_constraint(x, pltpu.VMEM)


def call(body, ins, outs, scratch=(), out_specs=None):
    return pl.pallas_call(
        body,
        out_shape=outs,
        in_specs=ins,
        out_specs=out_specs or (VMEM if not isinstance(outs, (tuple, list)) else [VMEM] * len(outs)),
        scratch_shapes=list(scratch),
        name=body.__name__,
    )


def per_device(fact_block, fact_offset, fact_date, revenue, supplier_words, date_words, candidates):
    cands = candidates.reshape(8, LANES)
    give0 = call(k0_body, [VMEM, VMEM, VMEM], here((2 * NCOL, LANES), I32))(
        supplier_words, date_words, cands
    )
    got0 = lax.all_to_all(give0.reshape(NCOL, 1, 2 * LANES), COL_SENT, 0, 0, tiled=True)
    got0 = near(got0.reshape(2 * NCOL, LANES))
    tab, cand = call(
        k1_body,
        [VMEM] * 5,
        [here((64, NDEV), F32), here((48, 1024), F32)],
        [pltpu.VMEM((NDEV, CH * LANES), BF16), pltpu.VMEM((80, CH * LANES), BF16)],
    )(
        fact_block.reshape(CH, LANES),
        fact_offset.reshape(CH, LANES),
        fact_date.reshape(CH, LANES),
        revenue.reshape(CH, LANES),
        candidates.reshape(1, 1024),
    )
    give1 = call(k2_body, [VMEM] * 3, here((NNEAR * 16, LANES), F32), [pltpu.VMEM((8, LANES), F32)])(
        got0, near(tab), near(cand)
    )
    got1 = lax.all_to_all(give1.reshape(NNEAR, 1, 16 * LANES), NEAR, 0, 0, tiled=True)
    give2 = call(k3_body, [VMEM], here((NFAR * LAST, LANES), F32))(near(got1.reshape(NNEAR * 16, LANES)))
    got2 = lax.all_to_all(give2.reshape(NFAR, 1, LAST * LANES), FAR_SENT, 0, 0, tiled=True)
    got2 = got2.reshape(NFAR * LAST, LANES)
    owned, cand, total = call(
        k4_body,
        [VMEM, VMEM],
        [shape((16, LANES), F32), shape((8, LANES), F32), shape((1, 1), F32)],
        [pltpu.VMEM((32, 64 * LANES), BF16), pltpu.VMEM((64, 64 * LANES), BF16)],
    )(near(got2), got0)
    return owned.reshape(SUP_DEV), cand.reshape(1024), total.reshape(())


def solution(mesh):
    split = Mesh(mesh.devices.reshape((2,) * 9), AXES)
    return jax.shard_map(
        per_device,
        mesh=split,
        in_specs=(P(AXES, None), P(AXES), P(AXES), P(AXES), P(COL), P(COL), P()),
        out_specs=(P(AXES), P(), P()),
        check_vma=False,
    )
```

```python
import functools

import jax
import jax.numpy as jnp
from jax import lax
from jax.experimental import pallas as pl
from jax.experimental.pallas import tpu as pltpu
from jax.sharding import Mesh
from jax.sharding import PartitionSpec as P

XH, Y2, Y1, Y0, XL, Z2, Z1, Z0, CORE = AXES = ("xh", "y2", "y1", "y0", "xl", "z2", "z1", "z0", "core")
COL = (XL, Z2, Z1, Z0, CORE)
NEAR = (Z2, Z1, Z0, CORE)
FAR = (XH, Y2, Y1, Y0, XL)
COL_SENT = (Z2, Z1, Z0, CORE, XL)
FAR_SENT = (Y0, Y1, Y2, XL, XH)

NNEAR, NFAR, NCOL, NDEV = 16, 32, 32, 512
SUP_DEV = 2048
WORDS = 69
LANES = 128
CH = 24
F32, BF16, I32 = jnp.float32, jnp.bfloat16, jnp.int32
DATES_AT = 104
LAST = 11


def iota(shape, dim):
    return lax.broadcasted_iota(I32, shape, dim)


def div30(x):
    return jnp.right_shift(x * 2185, 16)


def lane_gather(row, idx):
    table = jnp.broadcast_to(row, idx.shape)
    return jnp.take_along_axis(table, idx, axis=1, mode="promise_in_bounds")


def roll(x, shift):
    shift = shift % LANES
    return pltpu.roll(x, shift, 1) if shift else x


def lookup(words, idx):
    which, lane = jnp.right_shift(idx, 7), jnp.bitwise_and(idx, 127)
    out = lane_gather(words[0], lane)
    for i in range(1, len(words)):
        out = jnp.where(which == i, lane_gather(words[i], lane), out)
    return out


def k0_body(words_ref, dates_ref, cands_ref, out_ref):
    col = lax.axis_index(COL)
    words = [words_ref[i * LANES : (i + 1) * LANES].reshape(1, LANES) for i in range(8)]
    last = words_ref[8 * LANES : 16 * WORDS].reshape(1, 16 * WORDS - 8 * LANES)
    words.append(jnp.concatenate([last, jnp.zeros((1, 9 * LANES - 16 * WORDS), I32)], 1))
    cands = cands_ref[...]
    off = jnp.bitwise_and(cands, SUP_DEV - 1)
    block = jnp.right_shift(cands, 11) - 16 * col
    mine = (block >= 0) & (block < 16)
    slot = div30(off)
    word = lookup(words, jnp.where(mine, block * WORDS + slot, 0))
    bits = jnp.where(mine, jnp.bitwise_and(jnp.right_shift(word, off - 30 * slot), 1), 0)
    sub, lane = iota((8, LANES), 0), iota((8, LANES), 1)
    dates = jnp.concatenate([dates_ref[...].reshape(1, 3), jnp.zeros((1, LANES - 3), I32)], 1)
    dates = roll(jnp.broadcast_to(dates, (8, LANES)), DATES_AT)
    for i in range(2):
        m = 2 * sub + i
        own = lookup(words, jnp.where(lane < WORDS, m * WORDS + lane, 0))
        row = jnp.where(lane < WORDS, own, dates)
        for j in (4 * i, 4 * i + 2):
            out_ref[pl.ds(j, 8, stride=8), :] = row
            out_ref[pl.ds(j + 1, 8, stride=8), :] = roll(bits, 64 * i)


def k1_body(block_ref, off_ref, date_ref, rev_ref, cands_ref, tab_ref, cand_ref, hot_ref, val_ref):
    block, off, date = block_ref[...], off_ref[...], date_ref[...]
    rev = rev_ref[...].astype(F32)

    def key_of(b):
        return (
            jnp.bitwise_and(jnp.right_shift(b, 4), 3) * LANES
            + jnp.bitwise_and(b, 15) * 8
            + jnp.right_shift(b, 6)
        )

    key = key_of(block)
    own = iota((NDEV, LANES), 0)
    for i in range(CH):
        hot = jnp.where(own == key[i : i + 1, :], 1.0, 0.0).astype(BF16)
        hot_ref[:, i * LANES : (i + 1) * LANES] = hot
    nt = (((1,), (1,)), ((), ()))
    nn = (((1,), (0,)), ((), ()))
    dot = functools.partial(lax.dot_general, preferred_element_type=F32)
    chunk = jnp.where(
        jnp.right_shift(iota((32, CH * LANES), 1), 7) == iota((32, CH * LANES), 0), 1.0, 0.0
    ).astype(BF16)
    count = dot(chunk, hot_ref[...], nt)
    before = jnp.where(iota((32, 32), 1) < iota((32, 32), 0), 1.0, 0.0).astype(BF16)
    prefix = dot(before, count.astype(BF16), nn)
    base = dot(prefix.astype(BF16), hot_ref[...], nn)
    keys_down = jnp.transpose(jnp.concatenate([key, jnp.zeros((LANES - CH, LANES), I32)], 0))
    earlier = iota((LANES, LANES), 0) < iota((LANES, LANES), 1)
    off_hi = jnp.right_shift(off, 7)
    off_lo = jnp.bitwise_and(off, 127)
    date_q = div30(date)
    date_r = date - 30 * date_q
    date_c = jnp.right_shift(date_q * 43691, 17)
    date_l = date_c + 32 * (date_q - 3 * date_c)
    values = [off_lo.astype(F32), off_hi.astype(F32), rev, date_l.astype(F32), date_r.astype(F32)]
    slots = iota((16, LANES), 0)
    for i in range(CH):
        same = (keys_down[:, i : i + 1] == key[i : i + 1, :]) & earlier
        inside = jnp.sum(jnp.where(same, 1.0, 0.0), axis=0, keepdims=True)
        rank = inside + base[i : i + 1, i * LANES : (i + 1) * LANES]
        here = slots == rank.astype(I32)
        for g, v in enumerate(values):
            val_ref[16 * g : 16 * g + 16, i * LANES : (i + 1) * LANES] = jnp.where(
                here, v[i : i + 1, :], 0.0
            ).astype(BF16)
    table = dot(val_ref[...], hot_ref[...], nt)
    tab_ref[0:16, :] = table[0:16] + 128.0 * table[16:32]
    tab_ref[16:64, :] = table[32:80]
    cands = cands_ref[...]
    cand_key = key_of(jnp.right_shift(cands, 11))
    cand_hot = jnp.where(iota((NDEV, 1024), 0) == cand_key, 1.0, 0.0).astype(BF16)
    named = dot(table.astype(BF16), cand_hot, nn)
    cand_off = jnp.bitwise_and(cands, SUP_DEV - 1).astype(F32)
    same_off = named[0:16] + 128.0 * named[16:32] == cand_off
    cand_ref[0:16, :] = jnp.where(same_off, named[32:48], 0.0)
    cand_ref[16:48, :] = named[48:80]


def k2_body(got_ref, tab_ref, cand_ref, out_ref, tmp_ref):
    got = got_ref[pl.ds(0, NCOL, stride=2), :]
    src, lane = iota((NCOL, LANES), 0), iota((NCOL, LANES), 1)
    src = 16 * jnp.bitwise_and(src, 1) + jnp.right_shift(src, 1)
    table = jnp.zeros((NCOL, LANES), I32)
    for j in range(3):
        word = jnp.broadcast_to(got[:, DATES_AT + j : DATES_AT + j + 1], (NCOL, LANES))
        table = jnp.where(lane == 32 * j + src, word, table)
    table = jnp.sum(table, axis=0, keepdims=True)
    bits = jnp.sum(got_ref[pl.ds(1, NCOL, stride=2), :], axis=0, keepdims=True)
    row, at_lane = iota((LANES, LANES), 0), iota((LANES, LANES), 1)
    row = jnp.where(jnp.bitwise_and(at_lane, 15) >= 12, jnp.bitwise_and(row, 7), 7)
    lane8 = iota((8, LANES), 1)
    source = 4 * jnp.right_shift(lane8, 4) + jnp.bitwise_and(lane8, 3)
    bits = [lane_gather(bits, source + 32 * i).astype(F32)[0:1] for i in range(2)]

    def date_ok(where, place):
        return jnp.bitwise_and(jnp.right_shift(lane_gather(table, where.astype(I32)), place.astype(I32)), 1) == 1

    for i in range(8):
        at = slice(i * LANES, (i + 1) * LANES)
        keep = date_ok(cand_ref[16:32, at], cand_ref[32:48, at])
        tmp_ref[i : i + 1, :] = jnp.sum(jnp.where(keep, cand_ref[0:16, at], 0.0), axis=0, keepdims=True)
    part = tmp_ref[...]
    kept = []
    for i in range(4):
        at = slice(i * LANES, (i + 1) * LANES)
        keep = date_ok(tab_ref[32:48, at], tab_ref[48:64, at])
        kept.append(jnp.where(keep, tab_ref[16:32, at], 0.0))
    stack = []
    for i in range(4):
        stack += [tab_ref[0:16, i * LANES : (i + 1) * LANES], kept[i]]
    tiles = jnp.transpose(jnp.concatenate(stack, 0))
    tiles = jnp.where(row == 0, bits[0], jnp.where(row == 1, bits[1], tiles))
    for g in range(NNEAR):
        out_ref[16 * g : 16 * g + 8, :] = tiles[8 * g : 8 * g + 8]
        out_ref[16 * g + 8 : 16 * g + 16, :] = part


def k3_body(got_ref, out_ref):
    lane = iota((8, LANES), 1)
    source = 16 * jnp.right_shift(jnp.bitwise_and(lane, 31), 2) + 12 + jnp.bitwise_and(lane, 3)
    bits = jnp.zeros((8, LANES), F32)
    for j in range(4):
        rows = got_ref[pl.ds(16 * (j // 2) + j % 2, 8, stride=32), :]
        rows = jnp.take_along_axis(rows, source, axis=1, mode="promise_in_bounds")
        bits = jnp.where(jnp.right_shift(lane, 5) == j, rows, bits)
    total = got_ref[8:16, :]
    for g in range(1, NNEAR):
        total = total + got_ref[16 * g + 8 : 16 * g + 16, :]
    total = total * bits
    sub, lane = iota((4, LANES), 0), iota((4, LANES), 1)
    for hi in range(8):
        rows = [got_ref[pl.ds(64 * q + hi, 4, stride=16), :] for q in range(4)]
        for lo in range(4):
            tile = roll(rows[0], -32 * lo)
            for q in range(1, 4):
                tile = jnp.where(jnp.right_shift(lane, 5) == q, roll(rows[q], 32 * (q - lo)), tile)
            to = 4 * hi + lo
            at = LAST * sum((to >> b & 1) << p for b, p in ((4, 0), (3, 2), (2, 3), (1, 4), (0, 1)))
            fourth = jnp.broadcast_to(tile[3:4], (4, LANES))
            moved = jnp.where(sub == 0, roll(fourth, 12), jnp.where(sub == 1, roll(fourth, 8), roll(fourth, 4)))
            tile = jnp.where(jnp.bitwise_and(lane, 15) < 12, tile, moved)
            out_ref[at : at + 3, :] = tile[0:3]
            out_ref[at + 3 : at + 11, :] = total


def k4_body(got_ref, words_ref, owned_ref, cand_ref, total_ref, hi_ref, lo_ref):
    lane = iota((8, LANES), 1)
    first = jnp.bitwise_and(lane, 16) == 0
    high, low = iota((32, LANES), 0), iota((64, LANES), 0)
    high = 2 * jnp.bitwise_and(high, 15) + jnp.right_shift(high, 4)
    place = jnp.bitwise_and(lane, 15)

    def slots(eight):
        sent = [got_ref[pl.ds(8 * LAST * eight + u, 8, stride=LAST), :] for u in range(3)]
        fourth = jnp.zeros((8, LANES), F32)
        for u in range(3):
            fourth = jnp.where(jnp.right_shift(place, 2) == u, roll(sent[u], 4 * u - 12), fourth)
        return [jnp.where(place < 12, x, 0.0) for x in sent] + [fourth]

    tiles = [slots(eight) for eight in range(4)]
    for p in range(8):
        even, odd = tiles[2 * (p // 4)][p % 4], tiles[2 * (p // 4) + 1][p % 4]
        off = jnp.where(first, even, roll(odd, 16)).astype(I32)
        rev = jnp.where(first, roll(even, -16), odd)
        off_hi, off_lo = jnp.right_shift(off, 6), jnp.bitwise_and(off, 63)
        for s in range(8):
            at = slice((8 * p + s) * LANES, (8 * p + s + 1) * LANES)
            hi_ref[:, at] = jnp.where(off_hi[s : s + 1] == high, rev[s : s + 1], 0.0).astype(BF16)
            lo_ref[:, at] = jnp.where(off_lo[s : s + 1] == low, 1.0, 0.0).astype(BF16)
    owned = lax.dot_general(
        hi_ref[...], lo_ref[...], (((1,), (1,)), ((), ())), preferred_element_type=F32
    )
    owned = jnp.concatenate([owned[0:16], owned[16:32]], 1)
    far = lax.axis_index(FAR)
    words = words_ref[pl.ds(4 * jnp.bitwise_and(far, 15) + 2 * jnp.right_shift(far, 4), 1), :]
    place = iota((16, LANES), 0) * LANES + iota((16, LANES), 1)
    slot = div30(place)
    bit = jnp.bitwise_and(jnp.right_shift(lane_gather(words, slot), place - 30 * slot), 1)
    owned_ref[...] = jnp.where(bit == 1, owned, 0.0)
    cand = got_ref[3:11, :]
    for h in range(1, NFAR):
        cand = cand + got_ref[LAST * h + 3 : LAST * h + 11, :]
    cand_ref[...] = cand
    total_ref[...] = jnp.sum(jnp.sum(cand, axis=0, keepdims=True), axis=1, keepdims=True)


SMEM = pl.BlockSpec(memory_space=pltpu.SMEM)
VMEM = pl.BlockSpec(memory_space=pltpu.VMEM)
shape, here = jax.ShapeDtypeStruct, pltpu.VMEM


def near(x):
    return pltpu.with_memory_space_constraint(x, pltpu.VMEM)


def call(body, ins, outs, scratch=(), out_specs=None):
    return pl.pallas_call(
        body,
        out_shape=outs,
        in_specs=ins,
        out_specs=out_specs or (VMEM if not isinstance(outs, (tuple, list)) else [VMEM] * len(outs)),
        scratch_shapes=list(scratch),
        name=body.__name__,
    )


def per_device(fact_block, fact_offset, fact_date, revenue, supplier_words, date_words, candidates):
    cands = candidates.reshape(8, LANES)
    give0 = call(k0_body, [VMEM, VMEM, VMEM], here((2 * NCOL, LANES), I32))(
        supplier_words, date_words, cands
    )
    got0 = lax.all_to_all(give0.reshape(NCOL, 1, 2 * LANES), COL_SENT, 0, 0, tiled=True)
    got0 = near(got0.reshape(2 * NCOL, LANES))
    tab, cand = call(
        k1_body,
        [VMEM] * 5,
        [here((64, NDEV), F32), here((48, 1024), F32)],
        [pltpu.VMEM((NDEV, CH * LANES), BF16), pltpu.VMEM((80, CH * LANES), BF16)],
    )(
        fact_block.reshape(CH, LANES),
        fact_offset.reshape(CH, LANES),
        fact_date.reshape(CH, LANES),
        revenue.reshape(CH, LANES),
        candidates.reshape(1, 1024),
    )
    give1 = call(k2_body, [VMEM] * 3, here((NNEAR * 16, LANES), F32), [pltpu.VMEM((8, LANES), F32)])(
        got0, near(tab), near(cand)
    )
    got1 = lax.all_to_all(give1.reshape(NNEAR, 1, 16 * LANES), NEAR, 0, 0, tiled=True)
    give2 = call(k3_body, [VMEM], here((NFAR * LAST, LANES), F32))(near(got1.reshape(NNEAR * 16, LANES)))
    got2 = lax.all_to_all(give2.reshape(NFAR, 1, LAST * LANES), FAR_SENT, 0, 0, tiled=True)
    got2 = got2.reshape(NFAR * LAST, LANES)
    owned, cand, total = call(
        k4_body,
        [VMEM, VMEM],
        [shape((16, LANES), F32), shape((8, LANES), F32), shape((1, 1), F32)],
        [pltpu.VMEM((32, 64 * LANES), BF16), pltpu.VMEM((64, 64 * LANES), BF16)],
    )(near(got2), got0)
    return owned.reshape(SUP_DEV), cand.reshape(1024), total.reshape(())


def solution(mesh):
    split = Mesh(mesh.devices.reshape((2,) * 9), AXES)
    return jax.shard_map(
        per_device,
        mesh=split,
        in_specs=(P(AXES, None), P(AXES), P(AXES), P(AXES), P(COL), P(COL), P()),
        out_specs=(P(AXES), P(), P()),
        check_vma=False,
    )
```

```python
import functools

import jax
import jax.numpy as jnp
from jax import lax
from jax.experimental import pallas as pl
from jax.experimental.pallas import tpu as pltpu
from jax.sharding import Mesh
from jax.sharding import PartitionSpec as P

XH, Y2, Y1, Y0, XL, Z2, Z1, Z0, CORE = AXES = ("xh", "y2", "y1", "y0", "xl", "z2", "z1", "z0", "core")
COL = (XL, Z2, Z1, Z0, CORE)
NEAR = (Z2, Z1, Z0, CORE)
FAR = (XH, Y2, Y1, Y0, XL)
COL_SENT = (Z2, Z1, Z0, CORE, XL)
FAR_SENT = (Y0, Y1, Y2, XL, XH)

NNEAR, NFAR, NCOL, NDEV = 16, 32, 32, 512
SUP_DEV = 2048
WORDS = 69
LANES = 128
CH = 24
F32, BF16, I32 = jnp.float32, jnp.bfloat16, jnp.int32
DATES_AT = 104
LAST = 11


def iota(shape, dim):
    return lax.broadcasted_iota(I32, shape, dim)


def div30(x):
    return jnp.right_shift(x * 2185, 16)


def lane_gather(row, idx):
    table = jnp.broadcast_to(row, idx.shape)
    return jnp.take_along_axis(table, idx, axis=1, mode="promise_in_bounds")


def roll(x, shift):
    shift = shift % LANES
    return pltpu.roll(x, shift, 1) if shift else x


def lookup(words, idx):
    which, lane = jnp.right_shift(idx, 7), jnp.bitwise_and(idx, 127)
    out = lane_gather(words[0], lane)
    for i in range(1, len(words)):
        out = jnp.where(which == i, lane_gather(words[i], lane), out)
    return out


def k0_body(words_ref, dates_ref, cands_ref, out_ref):
    col = lax.axis_index(COL)
    words = [words_ref[i * LANES : (i + 1) * LANES].reshape(1, LANES) for i in range(8)]
    last = words_ref[8 * LANES : 16 * WORDS].reshape(1, 16 * WORDS - 8 * LANES)
    words.append(jnp.concatenate([last, jnp.zeros((1, 9 * LANES - 16 * WORDS), I32)], 1))
    cands = cands_ref[...]
    off = jnp.bitwise_and(cands, SUP_DEV - 1)
    block = jnp.right_shift(cands, 11) - 16 * col
    mine = (block >= 0) & (block < 16)
    slot = div30(off)
    word = lookup(words, jnp.where(mine, block * WORDS + slot, 0))
    bits = jnp.where(mine, jnp.bitwise_and(jnp.right_shift(word, off - 30 * slot), 1), 0)
    sub, lane = iota((8, LANES), 0), iota((8, LANES), 1)
    dates = jnp.concatenate([dates_ref[...].reshape(1, 3), jnp.zeros((1, LANES - 3), I32)], 1)
    dates = roll(jnp.broadcast_to(dates, (8, LANES)), DATES_AT)
    for i in range(2):
        m = 2 * sub + i
        own = lookup(words, jnp.where(lane < WORDS, m * WORDS + lane, 0))
        row = jnp.where(lane < WORDS, own, dates)
        for j in (4 * i, 4 * i + 2):
            out_ref[pl.ds(j, 8, stride=8), :] = row
            out_ref[pl.ds(j + 1, 8, stride=8), :] = roll(bits, 64 * i)


def k1_body(block_ref, off_ref, date_ref, rev_ref, cands_ref, tab_ref, cand_ref, hot_ref, val_ref):
    block, off, date = block_ref[...], off_ref[...], date_ref[...]
    rev = rev_ref[...].astype(F32)

    def key_of(b):
        return (
            jnp.bitwise_and(jnp.right_shift(b, 4), 3) * LANES
            + jnp.bitwise_and(b, 15) * 8
            + jnp.right_shift(b, 6)
        )

    key = key_of(block)
    own = iota((NDEV, LANES), 0)
    for i in range(CH):
        hot = jnp.where(own == key[i : i + 1, :], 1.0, 0.0).astype(BF16)
        hot_ref[:, i * LANES : (i + 1) * LANES] = hot
    nt = (((1,), (1,)), ((), ()))
    nn = (((1,), (0,)), ((), ()))
    dot = functools.partial(lax.dot_general, preferred_element_type=F32)
    chunk = jnp.where(
        jnp.right_shift(iota((32, CH * LANES), 1), 7) == iota((32, CH * LANES), 0), 1.0, 0.0
    ).astype(BF16)
    count = dot(chunk, hot_ref[...], nt)
    before = jnp.where(iota((32, 32), 1) < iota((32, 32), 0), 1.0, 0.0).astype(BF16)
    prefix = dot(before, count.astype(BF16), nn)
    base = dot(prefix.astype(BF16), hot_ref[...], nn)
    keys_down = jnp.transpose(jnp.concatenate([key, jnp.zeros((LANES - CH, LANES), I32)], 0))
    earlier = iota((LANES, LANES), 0) < iota((LANES, LANES), 1)
    off_hi = jnp.right_shift(off, 7)
    off_lo = jnp.bitwise_and(off, 127)
    date_q = div30(date)
    date_r = date - 30 * date_q
    date_c = jnp.right_shift(date_q * 43691, 17)
    date_l = date_c + 32 * (date_q - 3 * date_c)
    values = [off_lo.astype(F32), off_hi.astype(F32), rev, date_l.astype(F32), date_r.astype(F32)]
    slots = iota((16, LANES), 0)
    for i in range(CH):
        same = (keys_down[:, i : i + 1] == key[i : i + 1, :]) & earlier
        inside = jnp.sum(jnp.where(same, 1.0, 0.0), axis=0, keepdims=True)
        rank = inside + base[i : i + 1, i * LANES : (i + 1) * LANES]
        here = slots == rank.astype(I32)
        for g, v in enumerate(values):
            val_ref[16 * g : 16 * g + 16, i * LANES : (i + 1) * LANES] = jnp.where(
                here, v[i : i + 1, :], 0.0
            ).astype(BF16)
    table = dot(val_ref[...], hot_ref[...], nt)
    tab_ref[0:16, :] = table[0:16] + 128.0 * table[16:32]
    tab_ref[16:64, :] = table[32:80]
    cands = cands_ref[...]
    cand_key = key_of(jnp.right_shift(cands, 11))
    cand_hot = jnp.where(iota((NDEV, 1024), 0) == cand_key, 1.0, 0.0).astype(BF16)
    named = dot(table.astype(BF16), cand_hot, nn)
    cand_off = jnp.bitwise_and(cands, SUP_DEV - 1).astype(F32)
    same_off = named[0:16] + 128.0 * named[16:32] == cand_off
    cand_ref[0:16, :] = jnp.where(same_off, named[32:48], 0.0)
    cand_ref[16:48, :] = named[48:80]


def k2_body(got_ref, tab_ref, cand_ref, out_ref, tmp_ref):
    got = got_ref[pl.ds(0, NCOL, stride=2), :]
    src, lane = iota((NCOL, LANES), 0), iota((NCOL, LANES), 1)
    src = 16 * jnp.bitwise_and(src, 1) + jnp.right_shift(src, 1)
    table = jnp.zeros((NCOL, LANES), I32)
    for j in range(3):
        word = jnp.broadcast_to(got[:, DATES_AT + j : DATES_AT + j + 1], (NCOL, LANES))
        table = jnp.where(lane == 32 * j + src, word, table)
    table = jnp.sum(table, axis=0, keepdims=True)
    bits = jnp.sum(got_ref[pl.ds(1, NCOL, stride=2), :], axis=0, keepdims=True)
    row, at_lane = iota((LANES, LANES), 0), iota((LANES, LANES), 1)
    row = jnp.where(jnp.bitwise_and(at_lane, 15) >= 12, jnp.bitwise_and(row, 7), 7)
    lane8 = iota((8, LANES), 1)
    source = 4 * jnp.right_shift(lane8, 4) + jnp.bitwise_and(lane8, 3)
    bits = [lane_gather(bits, source + 32 * i).astype(F32)[0:1] for i in range(2)]

    def date_ok(where, place):
        return jnp.bitwise_and(jnp.right_shift(lane_gather(table, where.astype(I32)), place.astype(I32)), 1) == 1

    for i in range(8):
        at = slice(i * LANES, (i + 1) * LANES)
        keep = date_ok(cand_ref[16:32, at], cand_ref[32:48, at])
        tmp_ref[i : i + 1, :] = jnp.sum(jnp.where(keep, cand_ref[0:16, at], 0.0), axis=0, keepdims=True)
    part = tmp_ref[...]
    kept = []
    for i in range(4):
        at = slice(i * LANES, (i + 1) * LANES)
        keep = date_ok(tab_ref[32:48, at], tab_ref[48:64, at])
        kept.append(jnp.where(keep, tab_ref[16:32, at], 0.0))
    stack = []
    for i in range(4):
        stack += [tab_ref[0:16, i * LANES : (i + 1) * LANES], kept[i]]
    tiles = jnp.transpose(jnp.concatenate(stack, 0))
    tiles = jnp.where(row == 0, bits[0], jnp.where(row == 1, bits[1], tiles))
    for g in range(NNEAR):
        out_ref[16 * g : 16 * g + 8, :] = tiles[8 * g : 8 * g + 8]
        out_ref[16 * g + 8 : 16 * g + 16, :] = part


def k3_body(got_ref, out_ref, slot_ref):
    lane = iota((8, LANES), 1)
    source = 16 * jnp.right_shift(jnp.bitwise_and(lane, 31), 2) + 12 + jnp.bitwise_and(lane, 3)
    bits = jnp.zeros((8, LANES), F32)
    for j in range(4):
        rows = got_ref[pl.ds(16 * (j // 2) + j % 2, 8, stride=32), :]
        rows = jnp.take_along_axis(rows, source, axis=1, mode="promise_in_bounds")
        bits = jnp.where(jnp.right_shift(lane, 5) == j, rows, bits)
    total = got_ref[8:16, :]
    for g in range(1, NNEAR):
        total = total + got_ref[16 * g + 8 : 16 * g + 16, :]
    total = total * bits
    lane = iota((4, LANES), 1)
    for hi in range(8):
        rows = [got_ref[pl.ds(64 * q + hi, 4, stride=16), :] for q in range(4)]
        for lo in range(4):
            tile = roll(rows[0], -32 * lo)
            for q in range(1, 4):
                tile = jnp.where(jnp.right_shift(lane, 5) == q, roll(rows[q], 32 * (q - lo)), tile)
            to = 4 * hi + lo
            at = sum((to >> b & 1) << p for b, p in ((4, 0), (3, 2), (2, 3), (1, 4), (0, 1)))
            slot_ref[4 * at : 4 * at + 4, :] = tile
            out_ref[LAST * at + 3 : LAST * at + 11, :] = total
    place = jnp.bitwise_and(iota((8, LANES), 1), 15)
    for eight in range(4):
        fourth = slot_ref[pl.ds(32 * eight + 3, 8, stride=4), :]
        for u in range(3):
            rows = slot_ref[pl.ds(32 * eight + u, 8, stride=4), :]
            rows = jnp.where(place < 12, rows, roll(fourth, 12 - 4 * u))
            out_ref[pl.ds(8 * LAST * eight + u, 8, stride=LAST), :] = rows


def k4_body(got_ref, words_ref, owned_ref, cand_ref, total_ref, hi_ref, lo_ref):
    lane = iota((8, LANES), 1)
    first = jnp.bitwise_and(lane, 16) == 0
    high, low = iota((32, LANES), 0), iota((64, LANES), 0)
    high = 2 * jnp.bitwise_and(high, 15) + jnp.right_shift(high, 4)
    place = jnp.bitwise_and(lane, 15)

    def slots(eight):
        sent = [got_ref[pl.ds(8 * LAST * eight + u, 8, stride=LAST), :] for u in range(3)]
        fourth = jnp.zeros((8, LANES), F32)
        for u in range(3):
            fourth = jnp.where(jnp.right_shift(place, 2) == u, roll(sent[u], 4 * u - 12), fourth)
        return [jnp.where(place < 12, x, 0.0) for x in sent] + [fourth]

    tiles = [slots(eight) for eight in range(4)]
    for p in range(8):
        even, odd = tiles[2 * (p // 4)][p % 4], tiles[2 * (p // 4) + 1][p % 4]
        off = jnp.where(first, even, roll(odd, 16)).astype(I32)
        rev = jnp.where(first, roll(even, -16), odd)
        off_hi, off_lo = jnp.right_shift(off, 6), jnp.bitwise_and(off, 63)
        for s in range(8):
            at = slice((8 * p + s) * LANES, (8 * p + s + 1) * LANES)
            hi_ref[:, at] = jnp.where(off_hi[s : s + 1] == high, rev[s : s + 1], 0.0).astype(BF16)
            lo_ref[:, at] = jnp.where(off_lo[s : s + 1] == low, 1.0, 0.0).astype(BF16)
    owned = lax.dot_general(
        hi_ref[...], lo_ref[...], (((1,), (1,)), ((), ())), preferred_element_type=F32
    )
    owned = jnp.concatenate([owned[0:16], owned[16:32]], 1)
    far = lax.axis_index(FAR)
    words = words_ref[pl.ds(4 * jnp.bitwise_and(far, 15) + 2 * jnp.right_shift(far, 4), 1), :]
    place = iota((16, LANES), 0) * LANES + iota((16, LANES), 1)
    slot = div30(place)
    bit = jnp.bitwise_and(jnp.right_shift(lane_gather(words, slot), place - 30 * slot), 1)
    owned_ref[...] = jnp.where(bit == 1, owned, 0.0)
    cand = got_ref[3:11, :]
    for h in range(1, NFAR):
        cand = cand + got_ref[LAST * h + 3 : LAST * h + 11, :]
    cand_ref[...] = cand
    total_ref[...] = jnp.sum(jnp.sum(cand, axis=0, keepdims=True), axis=1, keepdims=True)


SMEM = pl.BlockSpec(memory_space=pltpu.SMEM)
VMEM = pl.BlockSpec(memory_space=pltpu.VMEM)
shape, here = jax.ShapeDtypeStruct, pltpu.VMEM


def near(x):
    return pltpu.with_memory_space_constraint(x, pltpu.VMEM)


def call(body, ins, outs, scratch=(), out_specs=None):
    return pl.pallas_call(
        body,
        out_shape=outs,
        in_specs=ins,
        out_specs=out_specs or (VMEM if not isinstance(outs, (tuple, list)) else [VMEM] * len(outs)),
        scratch_shapes=list(scratch),
        name=body.__name__,
    )


def per_device(fact_block, fact_offset, fact_date, revenue, supplier_words, date_words, candidates):
    cands = candidates.reshape(8, LANES)
    give0 = call(k0_body, [VMEM, VMEM, VMEM], here((2 * NCOL, LANES), I32))(
        supplier_words, date_words, cands
    )
    got0 = lax.all_to_all(give0.reshape(NCOL, 1, 2 * LANES), COL_SENT, 0, 0, tiled=True)
    got0 = near(got0.reshape(2 * NCOL, LANES))
    tab, cand = call(
        k1_body,
        [VMEM] * 5,
        [here((64, NDEV), F32), here((48, 1024), F32)],
        [pltpu.VMEM((NDEV, CH * LANES), BF16), pltpu.VMEM((80, CH * LANES), BF16)],
    )(
        fact_block.reshape(CH, LANES),
        fact_offset.reshape(CH, LANES),
        fact_date.reshape(CH, LANES),
        revenue.reshape(CH, LANES),
        candidates.reshape(1, 1024),
    )
    give1 = call(k2_body, [VMEM] * 3, here((NNEAR * 16, LANES), F32), [pltpu.VMEM((8, LANES), F32)])(
        got0, near(tab), near(cand)
    )
    got1 = lax.all_to_all(give1.reshape(NNEAR, 1, 16 * LANES), NEAR, 0, 0, tiled=True)
    give2 = call(k3_body, [VMEM], here((NFAR * LAST, LANES), F32), [pltpu.VMEM((4 * NFAR, LANES), F32)])(near(got1.reshape(NNEAR * 16, LANES)))
    got2 = lax.all_to_all(give2.reshape(NFAR, 1, LAST * LANES), FAR_SENT, 0, 0, tiled=True)
    got2 = got2.reshape(NFAR * LAST, LANES)
    owned, cand, total = call(
        k4_body,
        [VMEM, VMEM],
        [shape((16, LANES), F32), shape((8, LANES), F32), shape((1, 1), F32)],
        [pltpu.VMEM((32, 64 * LANES), BF16), pltpu.VMEM((64, 64 * LANES), BF16)],
    )(near(got2), got0)
    return owned.reshape(SUP_DEV), cand.reshape(1024), total.reshape(())


def solution(mesh):
    split = Mesh(mesh.devices.reshape((2,) * 9), AXES)
    return jax.shard_map(
        per_device,
        mesh=split,
        in_specs=(P(AXES, None), P(AXES), P(AXES), P(AXES), P(COL), P(COL), P()),
        out_specs=(P(AXES), P(), P()),
        check_vma=False,
    )
```
